32 devices in a mesh: dp: 16 (over z, y, x), tensor: 2 (over core).
Axes of the slice: x: 2, y: 2, z: 4, core: 2. Of those that a mesh axis runs over, the one named last changes fastest.
Arguments:
- tokens: bfloat16 [16384, 1536], P(('dp', 'tensor')), may hold values from -6 to 6
- segment_ids: int32 [16384], P('dp'), may hold values from -1 to 127, as said below
- norm_gain: float32 [1536], replicated, may hold values from 0.5 to 1.5
- in_gate_inner: bfloat16 [1536, 2, 3072], P('dp', None, 'tensor'), may hold values from -0.15625 to 0.15625
- in_state: bfloat16 [1536, 2, 128], P('dp'), may hold values from -0.15625 to 0.15625
- in_step: bfloat16 [1536, 48], P('dp', 'tensor'), may hold values from -0.15625 to 0.15625
- conv_inner: float32 [4, 3072], P(None, 'tensor'), may hold values from -3 to 3
- conv_inner_bias: float32 [3072], P('tensor'), may hold values from -3 to 3
- conv_state: float32 [4, 2, 128], replicated, may hold values from -3 to 3
- conv_state_bias: float32 [2, 128], replicated, may hold values from -3 to 3
- step_bias: float32 [48], P('tensor'), may hold values from -7 to -4
- decay_log: float32 [48], P('tensor'), may hold values from 0 to 2.5
- skip_gain: float32 [48], P('tensor'), may hold values from 0.5 to 1.5
- gate_gain: float32 [3072], P('tensor'), may hold values from 0.5 to 1.5
- out_proj: bfloat16 [3072, 1536], P('tensor', 'dp'), may hold values from -0.109375 to 0.109375
- cotangent: bfloat16 [16384, 1536], P(('dp', 'tensor')), may hold values from -6 to 6
Outputs:
- block_out: bfloat16 [16384, 1536], P(('dp', 'tensor'))
- grad_tokens: float32 [16384, 1536], P(('dp', 'tensor'))
- grad_norm_gain: float32 [1536], replicated
- grad_in_gate_inner: float32 [1536, 2, 3072], P('dp', None, 'tensor')
- grad_in_state: float32 [1536, 2, 128], P('dp')
- grad_in_step: float32 [1536, 48], P('dp', 'tensor')
- grad_conv_inner: float32 [4, 3072], P(None, 'tensor')
- grad_conv_inner_bias: float32 [3072], P('tensor')
- grad_conv_state: float32 [4, 2, 128], replicated
- grad_conv_state_bias: float32 [2, 128], replicated
- grad_step_bias: float32 [48], P('tensor')
- grad_decay_log: float32 [48], P('tensor')
- grad_skip_gain: float32 [48], P('tensor')
- grad_gate_gain: float32 [3072], P('tensor')
- grad_out_proj: float32 [3072, 1536], P('tensor', 'dp')
The draws below stay inside these ranges and needn't reach their ends.
Inputs may be any that keep to these rules, and one draw needn't show every extreme that they name: `segment_ids`: within each block of 1024 slots (one index of dp) the live slots come first and carry sequence numbers counting from 0 in order; every sequence starts at a slot whose place in its block is a multiple of 8 and has at most 1024 slots; the rest carry -1. Every block has at least 512 live slots. One block is fully live and begins with a sequence of exactly 1024 slots, another has exactly 512 live slots, and a third is fully live with sequences of 8 slots each.
All inputs are finite; a program needn't handle non-finite values.
Results may differ from the reference program's by a relative error of at most 0.0079.
Values may be sent and summed in bfloat16 or wider, within the bound.
A program may use at most 256 MiB of HBM per device.

```python
import jax
import jax.numpy as jnp
from jax import lax

D = 1536
INNER = 3072
HEAD_DIM = 64
STATE = 128
HEADS = 48
CONV = 4
TOK_DEV = 1024
SEQ_MAX = 1024
TOKENS = 16384


def draw_segment_ids(key, part):
    groups = TOKENS // TOK_DEV
    length_cap = min(SEQ_MAX, TOK_DEV)
    key_order, key_live, key_start = jax.random.split(key, 3)
    order = jax.random.permutation(key_order, groups)
    full_group = order[0]
    half_group = order[1]
    busy_group = order[2]
    live_count = jax.random.randint(key_live, (groups,), TOK_DEV // 2, TOK_DEV + 1)
    group_index = jnp.arange(groups)
    live_count = jnp.where(group_index == full_group, TOK_DEV, live_count)
    live_count = jnp.where(group_index == half_group, TOK_DEV // 2, live_count)
    live_count = jnp.where(group_index == busy_group, TOK_DEV, live_count)
    places = jnp.arange(TOK_DEV)
    aligned = (places % 8 == 0)[None, :]
    starts = jax.random.randint(key_start, (groups, TOK_DEV), 0, max(length_cap // 8, 1)) < 3
    starts = starts & aligned | (places % length_cap == 0)[None, :]
    quiet_zone = (group_index == full_group)[:, None] & ((places < length_cap) & (places > 0))[None, :]
    starts = starts & jnp.logical_not(quiet_zone)
    starts = jnp.where((group_index == busy_group)[:, None], aligned, starts)
    numbers = jnp.cumsum(starts.astype(jnp.int32), axis=1) - 1
    is_live = places[None, :] < live_count[:, None]
    return jnp.where(is_live, numbers, -1).reshape(TOKENS).astype(jnp.int32)


def steps_of(rng, dims, shards, least, high):
    loudness, own = 1.0, jax.random.fold_in(rng, 6)
    for axis_at, shards_of in shards:
        steps = jnp.exp(jax.random.uniform(jax.random.fold_in(own, axis_at), (shards_of,), jnp.float32, least / len(shards), high / len(shards)))
        loudness = loudness * jnp.repeat(steps, dims[axis_at] // shards_of).reshape([-1 if axis == axis_at else 1 for axis in range(len(dims))])
    return loudness


def gaussian(stream_key, extent, scale, limit, cuts=(), kind=jnp.bfloat16):
    entries = scale * jax.random.normal(stream_key, extent, jnp.float32)
    if cuts:
        entries = entries * steps_of(stream_key, extent, cuts, -0.22, 0.18)
    return jnp.clip(entries, -limit, limit).astype(kind)


def setup_inputs(seed: int = 0) -> dict:
    key_list = jax.random.split(jax.random.key(seed), 17)
    tokens = gaussian(key_list[0], (TOKENS, D), 1.0, 6.0, ((0, 32),))
    segment_ids = draw_segment_ids(jax.random.fold_in(key_list[16], 71), 0)
    norm_gain = jnp.clip(1.0 + 0.1 * jax.random.normal(key_list[2], (D,), jnp.float32), 0.5, 1.5)
    in_gate_inner = gaussian(key_list[3], (D, 2, INNER), D ** -0.5, 0.15625, ((0, 16), (2, 2)))
    in_state = gaussian(key_list[4], (D, 2, STATE), D ** -0.5, 0.15625, ((0, 16),))
    in_step = gaussian(key_list[5], (D, HEADS), D ** -0.5, 0.15625, ((0, 16), (1, 2)))
    conv_inner = gaussian(key_list[6], (CONV, INNER), CONV ** -0.5, 3.0, ((1, 2),), jnp.float32)
    conv_inner_bias = gaussian(key_list[7], (INNER,), 0.5, 3.0, ((0, 2),), jnp.float32)
    conv_state = gaussian(key_list[8], (CONV, 2, STATE), CONV ** -0.5, 3.0, (), jnp.float32)
    conv_state_bias = gaussian(key_list[9], (2, STATE), 0.5, 3.0, (), jnp.float32)
    step_bias = jnp.clip(-7.0 + 3.0 * jax.random.uniform(key_list[10], (HEADS,), jnp.float32) ** steps_of(key_list[10], (HEADS,), ((0, 2),), -0.2, 0.2), -7.0, -4.0)
    decay_log = jnp.clip(2.5 * jax.random.uniform(key_list[11], (HEADS,), jnp.float32) ** steps_of(key_list[11], (HEADS,), ((0, 2),), -0.2, 0.2), 0.0, 2.5)
    skip_gain = jnp.clip(0.5 + 1.0 * jax.random.uniform(key_list[12], (HEADS,), jnp.float32) ** steps_of(key_list[12], (HEADS,), ((0, 2),), -0.2, 0.2), 0.5, 1.5)
    gate_gain = jnp.clip(1.0 + 0.1 * jax.random.normal(key_list[13], (INNER,), jnp.float32), 0.5, 1.5)
    out_proj = gaussian(key_list[14], (INNER, D), INNER ** -0.5, 0.109375, ((0, 2), (1, 16)))
    cotangent = gaussian(key_list[15], (TOKENS, D), 1.0, 6.0, ((0, 32),))
    return dict(tokens=tokens, segment_ids=segment_ids, norm_gain=norm_gain, in_gate_inner=in_gate_inner, in_state=in_state, in_step=in_step, conv_inner=conv_inner, conv_inner_bias=conv_inner_bias, conv_state=conv_state, conv_state_bias=conv_state_bias, step_bias=step_bias, decay_log=decay_log, skip_gain=skip_gain, gate_gain=gate_gain, out_proj=out_proj, cotangent=cotangent)


EPSILON = 1e-05
HIGHEST = lax.Precision.HIGHEST

@jax.custom_vjp
def low(v):
    return lax.optimization_barrier(v.astype(jnp.bfloat16)).astype(jnp.float32)

@jax.custom_vjp
def low_back(v):
    return v

def low_keep(v):
    return (low(v), None)

def low_pass(kept, grad):
    return (grad,)

def back_keep(v):
    return (v, None)

def back_low(kept, grad):
    return (low(grad),)
low.defvjp(low_keep, low_pass)
low_back.defvjp(back_keep, back_low)

def shift_down(values, steps_back, filler):
    leading = jnp.full((steps_back,) + values.shape[1:], filler, values.dtype)
    return jnp.concatenate([leading, values[:values.shape[0] - steps_back]], axis=0)

def causal_conv(values, conv_taps, conv_bias, segment):
    taps_count = conv_taps.shape[0]
    result = conv_bias[None, :] + conv_taps[taps_count - 1][None, :] * values
    for steps_back in range(1, taps_count):
        earlier = shift_down(values, steps_back, 0.0)
        same_seq = (shift_down(segment, steps_back, -2) == segment).astype(values.dtype)
        result = result + conv_taps[taps_count - 1 - steps_back][None, :] * earlier * same_seq[:, None]
    return result

def group_forward(group_rows, segment, params):
    norm_gain, in_gate_inner, in_state, in_step, conv_inner, conv_inner_bias, conv_state, conv_state_bias, step_bias, decay_log, skip_gain, gate_gain, out_proj = params
    length = group_rows.shape[0]
    live_rows = (segment >= 0).astype(group_rows.dtype)
    row_scale = lax.rsqrt(lax.optimization_barrier(jnp.mean(group_rows * group_rows, axis=1, keepdims=True)) + EPSILON)
    normed = low(group_rows * row_scale * norm_gain[None, :])
    first_proj = low_back(jnp.dot(normed, in_gate_inner.reshape(D, 2 * INNER), precision=HIGHEST))
    state_proj = low_back(jnp.dot(normed, in_state.reshape(D, 2 * STATE), precision=HIGHEST))
    step_proj = low_back(jnp.dot(normed, in_step, precision=HIGHEST))
    gate_part = first_proj[:, :INNER]
    inner_act = jax.nn.silu(causal_conv(first_proj[:, INNER:], conv_inner, conv_inner_bias, segment))
    state_act = jax.nn.silu(causal_conv(state_proj, conv_state.reshape(CONV, 2 * STATE), conv_state_bias.reshape(2 * STATE), segment))
    state_in = state_act[:, :STATE]
    state_out = state_act[:, STATE:]
    step_size = jax.nn.softplus(step_proj + step_bias[None, :])
    log_decay = step_size * (-jnp.exp(decay_log))[None, :]
    cumulative = jnp.cumsum(log_decay, axis=0)
    scores = jnp.dot(state_out, state_in.T, precision=HIGHEST)
    places = jnp.arange(length)
    allowed = (places[:, None] >= places[None, :]) & (segment[:, None] == segment[None, :])
    allowed_float = allowed.astype(group_rows.dtype)
    heads_inner = inner_act.reshape(length, HEADS, HEAD_DIM)

    def one_head(head_args):
        head_cum, head_step, head_inner = head_args
        spread = jnp.where(allowed, head_cum[:, None] - head_cum[None, :], 0.0)
        mixing = scores * jnp.exp(spread) * allowed_float * head_step[None, :]
        return jnp.dot(mixing, head_inner, precision=HIGHEST)
    ssd_out = lax.map(jax.checkpoint(one_head), (cumulative.T, step_size.T, heads_inner.transpose(1, 0, 2)))
    mixed_heads = ssd_out.transpose(1, 0, 2) + skip_gain[None, :, None] * heads_inner
    gated_values = mixed_heads.reshape(length, INNER) * jax.nn.silu(gate_part)
    gate_scale = lax.rsqrt(lax.optimization_barrier(jnp.mean(gated_values * gated_values, axis=1, keepdims=True)) + EPSILON)
    normed_inner = low(gated_values * gate_scale * gate_gain[None, :])
    branch = low_back(jnp.dot(normed_inner, out_proj, precision=HIGHEST))
    return group_rows + live_rows[:, None] * branch

def reference(tokens, segment_ids, norm_gain, in_gate_inner, in_state, in_step, conv_inner, conv_inner_bias, conv_state, conv_state_bias, step_bias, decay_log, skip_gain, gate_gain, out_proj, cotangent):
    params = (norm_gain, in_gate_inner.astype(jnp.float32), in_state.astype(jnp.float32), in_step.astype(jnp.float32), conv_inner, conv_inner_bias, conv_state, conv_state_bias, step_bias, decay_log, skip_gain, gate_gain, out_proj.astype(jnp.float32))
    groups = TOKENS // TOK_DEV
    group_segments = segment_ids.reshape(groups, TOK_DEV)

    def whole_block(all_rows, all_params):

        def one_group(group_pair):
            return group_forward(group_pair[0], group_pair[1], all_params)
        outputs = lax.map(jax.checkpoint(one_group), (all_rows.reshape(groups, TOK_DEV, D), group_segments))
        return outputs.reshape(TOKENS, D)
    block_rows, pullback = jax.vjp(whole_block, tokens.astype(jnp.float32), params)
    grad_tokens, weight_grads = pullback(cotangent.astype(jnp.float32))
    grad_norm_gain, grad_in_gate_inner, grad_in_state, grad_in_step, grad_conv_inner, grad_conv_inner_bias, grad_conv_state, grad_conv_state_bias, grad_step_bias, grad_decay_log, grad_skip_gain, grad_gate_gain, grad_out_proj = weight_grads
    return (block_rows.astype(jnp.bfloat16), grad_tokens, grad_norm_gain, grad_in_gate_inner, grad_in_state, grad_in_step, grad_conv_inner, grad_conv_inner_bias, grad_conv_state, grad_conv_state_bias, grad_step_bias, grad_decay_log, grad_skip_gain, grad_gate_gain, grad_out_proj)
```

```python
from functools import partial

import jax
import jax.numpy as jnp
from jax import lax
from jax.sharding import PartitionSpec as P

SPAN = 256


EPSILON = 1e-05
HIGHEST = lax.Precision.HIGHEST


def shift_down(values, steps_back, filler):
    leading = jnp.full((steps_back,) + values.shape[1:], filler, values.dtype)
    return jnp.concatenate([leading, values[: values.shape[0] - steps_back]], axis=0)


def causal_conv(values, conv_taps, conv_bias, segment):
    taps_count = conv_taps.shape[0]
    result = conv_bias[None, :] + conv_taps[taps_count - 1][None, :] * values
    for steps_back in range(1, taps_count):
        earlier = shift_down(values, steps_back, 0.0)
        same_seq = (shift_down(segment, steps_back, -2) == segment).astype(values.dtype)
        result = (
            result + conv_taps[taps_count - 1 - steps_back][None, :] * earlier * same_seq[:, None]
        )
    return result


def span_step(carried_in, block_data):
    state_now, last_segment = carried_in
    inner_blk, state_in, state_out, step_blk, log_blk, seg_blk = block_data
    block_len = seg_blk.shape[0]
    cum_heads = jnp.cumsum(log_blk, axis=0).T
    places = jnp.arange(block_len)
    allowed = (places[:, None] >= places[None, :]) & (seg_blk[:, None] == seg_blk[None, :])
    spread = jnp.where(allowed[None], cum_heads[:, :, None] - cum_heads[:, None, :], 0.0)
    scores = jnp.dot(state_out, state_in.T, precision=HIGHEST)
    mixing = jnp.exp(spread) * (scores * allowed)[None] * step_blk.T[:, None, :]
    within = jnp.einsum("hts,shp->thp", mixing, inner_blk, precision=HIGHEST)
    carried = (seg_blk == last_segment).astype(jnp.float32)
    reach = jnp.exp(cum_heads).T * carried[:, None]
    from_state = (
        jnp.einsum("tn,hnp->thp", state_out, state_now, precision=HIGHEST) * reach[:, :, None]
    )
    end_segment = seg_blk[block_len - 1]
    keep_end = (seg_blk == end_segment).astype(jnp.float32)
    to_end = (
        jnp.exp(cum_heads[:, block_len - 1][:, None] - cum_heads).T * keep_end[:, None] * step_blk
    )
    fresh = jnp.einsum("sn,shp->hnp", state_in, inner_blk * to_end[:, :, None], precision=HIGHEST)
    kept_share = jnp.exp(cum_heads[:, block_len - 1]) * (end_segment == last_segment).astype(
        jnp.float32
    )
    new_state = fresh + state_now * kept_share[:, None, None]
    return ((new_state, end_segment), within + from_state)


def mixer(
    gate_inner,
    state_act,
    step_proj,
    conv_inner,
    conv_inner_bias,
    step_bias,
    decay_log,
    skip_gain,
    segment,
):
    length = gate_inner.shape[0]
    inner_dev = gate_inner.shape[1] // 2
    heads_dev = step_proj.shape[1]
    head_size = inner_dev // heads_dev
    state_dim = state_act.shape[1] // 2
    blocks = length // SPAN
    inner_act = jax.nn.silu(
        causal_conv(gate_inner[:, inner_dev:], conv_inner, conv_inner_bias, segment)
    )
    step_size = jax.nn.softplus(step_proj + step_bias[None, :])
    log_decay = step_size * (-jnp.exp(decay_log))[None, :]
    heads_inner = inner_act.reshape(length, heads_dev, head_size)
    initial = (jnp.zeros((heads_dev, state_dim, head_size), jnp.float32), jnp.int32(-2))
    scanned = (
        heads_inner.reshape(blocks, SPAN, heads_dev, head_size),
        state_act[:, :state_dim].reshape(blocks, SPAN, state_dim),
        state_act[:, state_dim:].reshape(blocks, SPAN, state_dim),
        step_size.reshape(blocks, SPAN, heads_dev),
        log_decay.reshape(blocks, SPAN, heads_dev),
        segment.reshape(blocks, SPAN),
    )
    unused, ssd_out = lax.scan(jax.checkpoint(span_step), initial, scanned)
    mixed_heads = (
        ssd_out.reshape(length, heads_dev, head_size) + skip_gain[None, :, None] * heads_inner
    )
    return mixed_heads.reshape(length, inner_dev) * jax.nn.silu(gate_inner[:, :inner_dev])


def shards(
    tokens,
    segment_ids,
    norm_gain,
    in_gate_inner,
    in_state,
    in_step,
    conv_inner,
    conv_inner_bias,
    conv_state,
    conv_state_bias,
    step_bias,
    decay_log,
    skip_gain,
    gate_gain,
    out_proj,
    cotangent,
):
    half_rows = tokens.shape[0]
    model_width = tokens.shape[1]
    tensor_place = lax.axis_index("tensor")
    own_segment = lax.dynamic_slice_in_dim(segment_ids, tensor_place * half_rows, half_rows)
    own_live = (own_segment >= 0).astype(jnp.float32)[:, None]
    own_rows = tokens.astype(jnp.float32)
    row_scale = lax.rsqrt(jnp.mean(own_rows * own_rows, axis=1, keepdims=True) + EPSILON)
    normed_own = (own_rows * row_scale * norm_gain[None, :]).astype(jnp.bfloat16)
    packed_in = jnp.concatenate(
        [
            in_gate_inner.reshape(in_gate_inner.shape[0], -1),
            in_state.reshape(in_state.shape[0], -1),
            in_step,
            jnp.zeros((in_step.shape[0], -in_step.shape[1] % 128), jnp.bfloat16),
        ],
        axis=1,
    )
    packed_weights = lax.all_gather(packed_in, "dp", axis=0, tiled=True)
    out_weights_t = lax.all_gather(out_proj.T, "dp", axis=0, tiled=True)
    inner_dev = in_gate_inner.shape[2]
    state_end = 2 * inner_dev + 2 * in_state.shape[2]
    gate_weights = packed_weights[:, : 2 * inner_dev]
    state_weights = packed_weights[:, 2 * inner_dev : state_end]
    step_weights = packed_weights[:, state_end : state_end + in_step.shape[1]]
    normed = lax.all_gather(normed_own, "tensor", axis=0, tiled=True)
    gate_inner = jnp.dot(
        normed, gate_weights, preferred_element_type=jnp.float32
    )
    state_proj = jnp.dot(
        normed, state_weights, preferred_element_type=jnp.float32
    )
    step_proj = jnp.dot(normed, step_weights, preferred_element_type=jnp.float32)

    def state_piece(state_values, conv_taps, conv_bias):
        return jax.nn.silu(
            causal_conv(
                state_values,
                conv_taps.reshape(conv_taps.shape[0], -1),
                conv_bias.reshape(-1),
                segment_ids,
            )
        )

    state_act, state_back = jax.vjp(state_piece, state_proj, conv_state, conv_state_bias)
    gated_values, mixer_back = jax.vjp(
        partial(mixer, segment=segment_ids),
        gate_inner,
        state_act,
        step_proj,
        conv_inner,
        conv_inner_bias,
        step_bias,
        decay_log,
        skip_gain,
    )
    full_inner = inner_dev * lax.axis_size("tensor")
    squares = lax.psum(jnp.sum(gated_values * gated_values, axis=1), "tensor")
    gate_scale = lax.rsqrt(squares / full_inner + EPSILON)[:, None]
    normed_inner = (gated_values * gate_scale * gate_gain[None, :]).astype(jnp.bfloat16)
    partial_out = jnp.einsum(
        "tc,dc->td", normed_inner, out_weights_t, preferred_element_type=jnp.float32
    )
    branch_own = lax.psum_scatter(partial_out, "tensor", scatter_dimension=0, tiled=True)
    block_out = (own_rows + own_live * branch_own).astype(jnp.bfloat16)
    cot_rows = cotangent.astype(jnp.float32)
    branch_grad_own = (own_live * cot_rows).astype(jnp.bfloat16)
    branch_grad = lax.all_gather(branch_grad_own, "tensor", axis=0, tiled=True)
    grad_out_proj_t = jnp.einsum(
        "td,tc->dc", branch_grad, normed_inner, preferred_element_type=jnp.float32
    )
    grad_normed_inner = jnp.einsum(
        "td,dc->tc", branch_grad, out_weights_t, preferred_element_type=jnp.float32
    )
    grad_gate_gain = jnp.sum(grad_normed_inner * gated_values * gate_scale, axis=0)
    scaled_grad = grad_normed_inner * gate_gain[None, :]
    products = lax.psum(jnp.sum(scaled_grad * gated_values, axis=1), "tensor")
    grad_gated = (
        gate_scale * scaled_grad - gated_values * gate_scale**3 * (products / full_inner)[:, None]
    )
    (
        grad_gate_inner,
        grad_state_part,
        grad_step_proj,
        grad_conv_inner,
        grad_conv_inner_bias,
        grad_step_bias,
        grad_decay_log,
        grad_skip_gain,
    ) = mixer_back(grad_gated)
    grad_state_act = lax.psum(grad_state_part, "tensor")
    grad_state_proj, grad_conv_state, grad_conv_state_bias = state_back(grad_state_act)
    low_gate_inner = grad_gate_inner.astype(jnp.bfloat16)
    low_state = grad_state_proj.astype(jnp.bfloat16)
    low_step = grad_step_proj.astype(jnp.bfloat16)
    grad_gate_half = jnp.einsum(
        "td,tc->dc", normed, low_gate_inner[:, :inner_dev], preferred_element_type=jnp.float32
    )
    early_part = lax.psum_scatter(
        jnp.concatenate([grad_out_proj_t, grad_gate_half], axis=1).astype(jnp.bfloat16),
        "dp",
        scatter_dimension=0,
        tiled=True,
    ).astype(jnp.float32)
    low_late = jnp.concatenate(
        [
            low_gate_inner[:, inner_dev:],
            low_state,
            low_step,
            jnp.zeros((low_step.shape[0], -low_step.shape[1] % 128), jnp.bfloat16),
        ],
        axis=1,
    )
    grad_late = jnp.einsum("td,tc->dc", normed, low_late, preferred_element_type=jnp.float32)
    late_part = lax.psum_scatter(
        grad_late.astype(jnp.bfloat16), "dp", scatter_dimension=0, tiled=True
    ).astype(jnp.float32)
    grad_out_proj = early_part[:, :inner_dev].T
    grad_in_gate_inner = jnp.stack([early_part[:, inner_dev:], late_part[:, :inner_dev]], axis=1)
    late_state = inner_dev + low_state.shape[1]
    grad_in_state = late_part[:, inner_dev:late_state].reshape(in_state.shape)
    grad_in_step = late_part[:, late_state : late_state + low_step.shape[1]]
    head_grads = jnp.einsum(
        "tc,dc->td",
        low_gate_inner,
        gate_weights,
        preferred_element_type=jnp.float32,
    )
    head_grads = head_grads + jnp.einsum(
        "th,dh->td", low_step, step_weights, preferred_element_type=jnp.float32
    )
    normed_grad_own = lax.psum_scatter(head_grads, "tensor", scatter_dimension=0, tiled=True)
    own_state_grad = lax.dynamic_slice_in_dim(low_state, tensor_place * half_rows, half_rows)
    normed_grad_own = normed_grad_own + jnp.einsum(
        "tc,dc->td",
        own_state_grad,
        state_weights,
        preferred_element_type=jnp.float32,
    )
    grad_norm_part = jnp.sum(normed_grad_own * own_rows * row_scale, axis=0)
    scaled_rows = normed_grad_own * norm_gain[None, :]
    row_products = jnp.sum(scaled_rows * own_rows, axis=1, keepdims=True)
    grad_tokens = (
        cot_rows + row_scale * scaled_rows - own_rows * row_scale**3 * row_products / model_width
    )
    split_parts = (
        grad_conv_inner,
        grad_conv_inner_bias,
        grad_step_bias,
        grad_decay_log,
        grad_skip_gain,
        grad_gate_gain,
    )
    half_state = 1.0 / lax.axis_size("tensor")
    whole_parts = (grad_norm_part, grad_conv_state * half_state, grad_conv_state_bias * half_state)
    split_row = jnp.concatenate([part.reshape(-1) for part in split_parts])
    split_rows = jnp.zeros((lax.axis_size("tensor"), split_row.shape[0]), jnp.float32)
    split_rows = lax.dynamic_update_slice(split_rows, split_row[None], (tensor_place, 0))
    whole_row = jnp.concatenate([part.reshape(-1) for part in whole_parts])
    summed = lax.psum(jnp.concatenate([split_rows.reshape(-1), whole_row]), ("dp", "tensor"))
    split_sum = lax.dynamic_slice_in_dim(
        summed, tensor_place * split_row.shape[0], split_row.shape[0]
    )
    whole_sum = summed[split_rows.size :]

    def unpack(row, parts):
        pieces, start = [], 0
        for part in parts:
            pieces.append(row[start : start + part.size].reshape(part.shape))
            start += part.size
        return pieces

    split_out = unpack(split_sum, split_parts)
    whole_out = unpack(whole_sum, whole_parts)
    return (
        block_out,
        grad_tokens,
        whole_out[0],
        grad_in_gate_inner,
        grad_in_state,
        grad_in_step,
        split_out[0],
        split_out[1],
        whole_out[1],
        whole_out[2],
        split_out[2],
        split_out[3],
        split_out[4],
        split_out[5],
        grad_out_proj,
    )


def solution(mesh):
    in_specs = (
        P(("dp", "tensor"), None),
        P("dp"),
        P(),
        P("dp", None, "tensor"),
        P("dp", None, None),
        P("dp", "tensor"),
        P(None, "tensor"),
        P("tensor"),
        P(),
        P(),
        P("tensor"),
        P("tensor"),
        P("tensor"),
        P("tensor"),
        P("tensor", "dp"),
        P(("dp", "tensor"), None),
    )
    out_specs = (
        P(("dp", "tensor"), None),
        P(("dp", "tensor"), None),
        P(),
        P("dp", None, "tensor"),
        P("dp", None, None),
        P("dp", "tensor"),
        P(None, "tensor"),
        P("tensor"),
        P(),
        P(),
        P("tensor"),
        P("tensor"),
        P("tensor"),
        P("tensor"),
        P("tensor", "dp"),
    )
    return jax.shard_map(shards, mesh=mesh, in_specs=in_specs, out_specs=out_specs, check_vma=False)
```

```python
from functools import partial

import jax
import jax.numpy as jnp
from jax import lax
from jax.experimental import pallas as pl
from jax.experimental.pallas import tpu as pltpu
from jax.sharding import PartitionSpec as P

EPSILON = 1e-05
HIGHEST = lax.Precision.HIGHEST
CHUNK = 128
HEADS_STEP = 8
F32 = jnp.float32
BF16 = jnp.bfloat16


def shift_down(values, steps_back, filler):
    leading = jnp.full((steps_back,) + values.shape[1:], filler, values.dtype)
    return jnp.concatenate([leading, values[: values.shape[0] - steps_back]], axis=0)


def causal_conv(values, conv_taps, conv_bias, segment):
    taps_count = conv_taps.shape[0]
    result = conv_bias[None, :] + conv_taps[taps_count - 1][None, :] * values
    for steps_back in range(1, taps_count):
        earlier = shift_down(values, steps_back, 0.0)
        same_seq = (shift_down(segment, steps_back, -2) == segment).astype(values.dtype)
        result = (
            result + conv_taps[taps_count - 1 - steps_back][None, :] * earlier * same_seq[:, None]
        )
    return result


def dot(a, b):
    return jnp.dot(a, b, preferred_element_type=F32)


def dot_nt(a, b):
    return lax.dot_general(a, b, (((1,), (1,)), ((), ())), preferred_element_type=F32)


def spread_heads(columns, pair, head_size):
    lane = lax.broadcasted_iota(jnp.int32, (columns.shape[0], 2 * head_size), 1)
    first = columns[:, 2 * pair : 2 * pair + 1]
    second = columns[:, 2 * pair + 1 : 2 * pair + 2]
    return jnp.where(lane < head_size, first, second)


def conv_pair(xr, taps, bias, masks, rows, before, lanes):
    current = xr[rows, lanes]
    joined = jnp.concatenate([xr[before, lanes], current], axis=0)
    count = taps.shape[0]
    value = bias[0:1, lanes] + taps[count - 1 : count, lanes] * current
    shifted = []
    for back in range(1, count):
        piece = pltpu.roll(joined, back, 0)[8:] * masks[back - 1, rows, :]
        shifted.append(piece)
        value = value + taps[count - 1 - back : count - back, lanes] * piece
    return current, shifted, value


def ssd_forward_kernel(
    xr, taps, bias, skip, masks, score, cs, bst, dt, cumc, reach, toend, cumr, kept,
    y_out, states_out, state,
):
    width = xr.shape[1]
    head_size = width // dt.shape[2]
    pair_width = 2 * head_size
    chunks = xr.shape[0] // CHUNK
    state[...] = jnp.zeros_like(state)

    def chunk_body(place, unused):
        start = pl.multiple_of(place * CHUNK, CHUNK)
        rows = pl.ds(start, CHUNK)
        before = pl.ds(pl.multiple_of(jnp.maximum(start - 8, 0), 8), 8)
        dt_cols, cum_cols = dt[0, rows, :], cumc[0, rows, :]
        reach_cols, end_cols = reach[0, rows, :], toend[0, rows, :]
        score_now, cs_now, bst_now = score[rows, :], cs[rows, :], bst[:, rows]
        lane = lax.broadcasted_iota(jnp.int32, (CHUNK, pair_width), 1)
        row_of = pl.ds(pl.multiple_of(place * 8, 8), 8)
        for pair in range(width // pair_width):
            lanes = slice(pair * pair_width, (pair + 1) * pair_width)
            unused_cur, unused_shift, value = conv_pair(
                xr, taps, bias, masks, rows, before, lanes
            )
            x = value * jax.nn.sigmoid(value)
            xdt = x * spread_heads(dt_cols, pair, head_size)
            xb = xdt.astype(BF16)
            held = state[:, lanes]
            held_low = held.astype(BF16)
            states_out[rows, lanes] = held_low
            halves = []
            for head in (2 * pair, 2 * pair + 1):
                spread = cum_cols[:, head : head + 1] - cumr[0, head : head + 1, rows]
                mixing = score_now * jnp.exp(jnp.minimum(spread, 0.0))
                halves.append(dot(mixing.astype(BF16), xb))
            y = jnp.where(lane < head_size, halves[0], halves[1])
            y = y + spread_heads(reach_cols, pair, head_size) * dot(cs_now, held_low)
            y_out[rows, lanes] = y + skip[0:1, lanes] * x
            fresh = dot(bst_now, (xdt * spread_heads(end_cols, pair, head_size)).astype(BF16))
            state[:, lanes] = fresh + kept[0, row_of, lanes][0:1] * held
        return unused

    lax.fori_loop(0, chunks, chunk_body, 0)


def ssd_backward_kernel(
    xr, taps, bias, skip, masks, score_t, cs, bs, cst, pick, dt, cumc, reach, toend, cumr, kept,
    states, dy,
    dxr_out, dscore_out, dbs_out, dcs_out, cols_out, rows_out, span_out, sums_out,
    dstate, dvalue_next,
):
    width = xr.shape[1]
    head_size = width // dt.shape[2]
    pair_width = 2 * head_size
    length = xr.shape[0]
    chunks = length // CHUNK
    count = taps.shape[0]
    dstate[...] = jnp.zeros_like(dstate)
    dvalue_next[...] = jnp.zeros_like(dvalue_next)
    sums_out[...] = jnp.zeros_like(sums_out)

    @pl.when(pl.program_id(0) == 0)
    def clear():
        dscore_out[...] = jnp.zeros_like(dscore_out)
        dbs_out[...] = jnp.zeros_like(dbs_out)
        dcs_out[...] = jnp.zeros_like(dcs_out)

    def chunk_body(step, unused):
        place = chunks - 1 - step
        start = pl.multiple_of(place * CHUNK, CHUNK)
        rows = pl.ds(start, CHUNK)
        before = pl.ds(pl.multiple_of(jnp.maximum(start - 8, 0), 8), 8)
        after = pl.ds(pl.multiple_of(jnp.minimum(start + CHUNK, length - 8), 8), 8)
        dt_cols, cum_cols = dt[0, rows, :], cumc[0, rows, :]
        reach_cols, end_cols = reach[0, rows, :], toend[0, rows, :]
        score_now, cs_now, bs_now, cst_now = score_t[rows, :], cs[rows, :], bs[rows, :], cst[:, rows]
        lane = lax.broadcasted_iota(jnp.int32, (CHUNK, pair_width), 1)
        row_of = pl.ds(pl.multiple_of(place * 8, 8), 8)
        dscore = jnp.zeros((CHUNK, CHUNK), F32)
        dbs = jnp.zeros((CHUNK, bs_now.shape[1]), F32)
        dcs = jnp.zeros((CHUNK, bs_now.shape[1]), F32)
        columns = jnp.zeros((CHUNK, cols_out.shape[2]), F32)
        column_lane = lax.broadcasted_iota(jnp.int32, columns.shape, 1)
        for pair in range(width // pair_width):
            lanes = slice(pair * pair_width, (pair + 1) * pair_width)
            current, shifted, value = conv_pair(xr, taps, bias, masks, rows, before, lanes)
            gate = jax.nn.sigmoid(value)
            x = value * gate
            dt_now = spread_heads(dt_cols, pair, head_size)
            end_now = spread_heads(end_cols, pair, head_size)
            xdt = x * dt_now
            xb = xdt.astype(BF16)
            dy_now = dy[rows, lanes]
            dyb = dy_now.astype(BF16)
            held_low = states[rows, lanes]
            dheld = dstate[:, lanes]
            dheld_low = dheld.astype(BF16)
            dyr = dy_now * spread_heads(reach_cols, pair, head_size)
            dyr_low = dyr.astype(BF16)
            from_state = dyr * dot(cs_now, held_low)
            dcs = dcs + dot_nt(dyr_low, held_low)
            dxdt_end = end_now * dot(bs_now, dheld_low)
            dbs = dbs + dot_nt((xdt * end_now).astype(BF16), dheld_low)
            halves = []
            for side in (0, 1):
                head = 2 * pair + side
                spread = cumr[0, head : head + 1, rows] - cum_cols[:, head : head + 1]
                decay = jnp.exp(jnp.minimum(spread, 0.0))
                weight = score_now * decay
                own = (lane < head_size) if side == 0 else (lane >= head_size)
                pairs = dot_nt(jnp.where(own, xdt, 0.0).astype(BF16), dyb)
                dscore = dscore + pairs * decay
                share = pairs * weight
                columns = columns - jnp.where(
                    column_lane == head, jnp.sum(share, axis=1, keepdims=True), 0.0
                )
                rows_out[0, head : head + 1, rows] = jnp.sum(share, axis=0, keepdims=True)
                halves.append(dot(weight.astype(BF16), dyb))
            dxdt = jnp.where(lane < head_size, halves[0], halves[1]) + dxdt_end
            picked = jnp.concatenate(
                [
                    from_state.astype(BF16),
                    (xdt * dxdt_end).astype(BF16),
                    (x * dxdt).astype(BF16),
                ],
                axis=1,
            )
            columns = columns + dot(picked, pick[pair])
            dx = skip[0:1, lanes] * dy_now + dt_now * dxdt
            kept_row = kept[0, row_of, lanes][0:1]
            span_row = kept_row * jnp.sum(dheld * held_low.astype(F32), axis=0, keepdims=True)
            span_out[0, row_of, lanes] = jnp.broadcast_to(span_row, (8, pair_width))
            dstate[:, lanes] = kept_row * dheld + dot(cst_now, dyr_low)
            dvalue = dx * (gate * (1.0 + value * (1.0 - gate)))
            dxr = taps[count - 1 : count, lanes] * dvalue
            next_rows = dvalue_next[:, lanes]
            sums = [jnp.sum(dvalue * current, axis=0, keepdims=True)]
            for back in range(1, count):
                masked = dvalue * masks[back - 1, rows, :]
                joined = jnp.concatenate(
                    [masked, next_rows * masks[back - 1, after, :]], axis=0
                )
                lifted = pltpu.roll(joined, CHUNK + 8 - back, 0)[:CHUNK]
                dxr = dxr + taps[count - 1 - back : count - back, lanes] * lifted
                sums.append(jnp.sum(dvalue * shifted[back - 1], axis=0, keepdims=True))
            dvalue_next[:, lanes] = dvalue[:8]
            sums.append(jnp.sum(dvalue, axis=0, keepdims=True))
            sums.append(jnp.sum(dy_now * x, axis=0, keepdims=True))
            for slot, row in enumerate(sums):
                sums_out[slot : slot + 1, lanes] += row
            dxr_out[rows, lanes] = dxr.astype(dxr_out.dtype)
        dscore_out[rows, :] += dscore
        dbs_out[rows, :] += dbs
        dcs_out[rows, :] += dcs
        cols_out[0, rows, :] = columns
        return unused

    lax.fori_loop(0, chunks, chunk_body, 0)


def chunk_terms(step_size, log_decay, segment, head_size):
    length, heads = step_size.shape
    chunks, groups = length // CHUNK, heads // HEADS_STEP
    parted = segment.reshape(chunks, CHUNK)
    places = jnp.arange(CHUNK)
    lower = (places[:, None] >= places[None, :]).astype(F32)
    allowed = (
        (parted[:, :, None] == parted[:, None, :]) & (places[:, None] >= places[None, :])[None]
    ).astype(F32)
    cumulative = jnp.einsum(
        "ts,csh->cth", lower, log_decay.reshape(chunks, CHUNK, heads), precision=HIGHEST
    )
    last = jnp.concatenate([jnp.full((1,), -2, segment.dtype), parted[:-1, CHUNK - 1]])
    carried = (parted == last[:, None]).astype(F32)
    final = parted[:, CHUNK - 1]
    at_end = (parted == final[:, None]).astype(F32)
    total = cumulative[:, CHUNK - 1]
    reach = jnp.exp(cumulative) * carried[:, :, None]
    to_end = jnp.exp(total[:, None, :] - cumulative) * at_end[:, :, None]
    kept = jnp.exp(total) * (final == last).astype(F32)[:, None]

    def by_group(array):
        return array.reshape(length, groups, HEADS_STEP).transpose(1, 0, 2)

    columns = tuple(by_group(a.reshape(length, heads)) for a in (step_size, cumulative, reach, to_end))
    cum_rows = cumulative.reshape(length, heads).T.reshape(groups, HEADS_STEP, length)
    kept_rows = jnp.repeat(kept, head_size, axis=1).reshape(chunks, groups, -1).transpose(1, 0, 2)
    kept_rows = jnp.repeat(kept_rows, 8, axis=1)
    masks = jnp.stack(
        [
            jnp.broadcast_to(
                (shift_down(segment, back, -2) == segment).astype(F32)[:, None],
                (length, 2 * head_size),
            )
            for back in (1, 2, 3)
        ]
    )
    return allowed, columns, cum_rows, kept_rows, masks


def whole_spec(array):
    zeros = (0,) * array.ndim
    return pl.BlockSpec(array.shape, lambda g: zeros)


def group_spec(array):
    rest = (0,) * (array.ndim - 1)
    return pl.BlockSpec((1,) + array.shape[1:], lambda g: (g,) + rest)


def lanes_spec(array, width):
    return pl.BlockSpec((array.shape[0], width), lambda g: (0, g))


def ssd_forward(xr, taps, bias, skip_row, terms, bs_low, cs_low):
    allowed, columns, cum_rows, kept_rows, masks = terms
    length, inner = xr.shape
    groups = cum_rows.shape[0]
    width = inner // groups
    state_dim = bs_low.shape[1]
    chunks = length // CHUNK
    score = (
        jnp.einsum(
            "ctn,csn->cts",
            cs_low.reshape(chunks, CHUNK, state_dim),
            bs_low.reshape(chunks, CHUNK, state_dim),
            preferred_element_type=F32,
        )
        * allowed
    )
    shared = (masks, score.reshape(length, CHUNK), cs_low, bs_low.T)
    grouped = (*columns, cum_rows, kept_rows)
    y, states = pl.pallas_call(
        ssd_forward_kernel,
        grid=(groups,),
        in_specs=[lanes_spec(a, width) for a in (xr, taps, bias, skip_row)]
        + [whole_spec(a) for a in shared]
        + [group_spec(a) for a in grouped],
        out_specs=[
            pl.BlockSpec((length, width), lambda g: (0, g)),
            pl.BlockSpec((chunks * state_dim, width), lambda g: (0, g)),
        ],
        out_shape=[
            jax.ShapeDtypeStruct((length, inner), F32),
            jax.ShapeDtypeStruct((chunks * state_dim, inner), BF16),
        ],
        scratch_shapes=[pltpu.VMEM((state_dim, width), F32)],
        cost_estimate=pl.CostEstimate(
            flops=8 * length * inner * CHUNK, bytes_accessed=12 * length * inner, transcendentals=0
        ),
        name="ssd_forward",
    )(xr, taps, bias, skip_row, *shared, *grouped)
    return y, states, score


def ssd_backward(xr, taps, bias, skip_row, terms, score, bs_low, cs_low, states, dy):
    allowed, columns, cum_rows, kept_rows, masks = terms
    length, inner = xr.shape
    groups, heads_step = cum_rows.shape[:2]
    width = inner // groups
    head_size = width // heads_step
    state_dim = bs_low.shape[1]
    chunks = length // CHUNK
    lane = jnp.arange(2 * head_size) // head_size
    pick = jnp.stack(
        [
            jnp.concatenate(
                [
                    (
                        (2 * pair + lane + slot * heads_step)[:, None] == jnp.arange(CHUNK)[None, :]
                    ).astype(BF16)
                    for slot in range(3)
                ]
            )
            for pair in range(heads_step // 2)
        ]
    )
    score_t = score.transpose(0, 2, 1).reshape(length, CHUNK)
    shared = (masks, score_t, cs_low, bs_low, cs_low.T, pick)
    grouped = (*columns, cum_rows, kept_rows)
    fixed = pl.BlockSpec((length, CHUNK), lambda g: (0, 0))
    out = pl.pallas_call(
        ssd_backward_kernel,
        grid=(groups,),
        in_specs=[lanes_spec(a, width) for a in (xr, taps, bias, skip_row)]
        + [whole_spec(a) for a in shared]
        + [group_spec(a) for a in grouped]
        + [lanes_spec(a, width) for a in (states, dy)],
        out_specs=[
            pl.BlockSpec((length, width), lambda g: (0, g)),
            fixed,
            pl.BlockSpec((length, state_dim), lambda g: (0, 0)),
            pl.BlockSpec((length, state_dim), lambda g: (0, 0)),
            pl.BlockSpec((1, length, CHUNK), lambda g: (g, 0, 0)),
            pl.BlockSpec((1, heads_step, length), lambda g: (g, 0, 0)),
            pl.BlockSpec((1, 8 * chunks, width), lambda g: (g, 0, 0)),
            pl.BlockSpec((8, width), lambda g: (0, g)),
        ],
        out_shape=[
            jax.ShapeDtypeStruct((length, inner), BF16),
            jax.ShapeDtypeStruct((length, CHUNK), F32),
            jax.ShapeDtypeStruct((length, state_dim), F32),
            jax.ShapeDtypeStruct((length, state_dim), F32),
            jax.ShapeDtypeStruct((groups, length, CHUNK), F32),
            jax.ShapeDtypeStruct((groups, heads_step, length), F32),
            jax.ShapeDtypeStruct((groups, 8 * chunks, width), F32),
            jax.ShapeDtypeStruct((8, inner), F32),
        ],
        scratch_shapes=[pltpu.VMEM((state_dim, width), F32), pltpu.VMEM((8, width), F32)],
        cost_estimate=pl.CostEstimate(
            flops=24 * length * inner * CHUNK, bytes_accessed=16 * length * inner, transcendentals=0
        ),
        name="ssd_backward",
    )(xr, taps, bias, skip_row, *shared, *grouped, states, dy)
    dxr, dscore_t, dbs, dcs, cols, rows, span, sums = out
    dscore_t = (dscore_t.reshape(chunks, CHUNK, CHUNK) * allowed.transpose(0, 2, 1)).astype(BF16)
    parted_c = cs_low.reshape(chunks, CHUNK, state_dim)
    parted_b = bs_low.reshape(chunks, CHUNK, state_dim)
    dbs = dbs + jnp.einsum(
        "cst,ctn->csn", dscore_t, parted_c, preferred_element_type=F32
    ).reshape(length, state_dim)
    dcs = dcs + jnp.einsum(
        "cst,csn->ctn", dscore_t, parted_b, preferred_element_type=F32
    ).reshape(length, state_dim)
    heads = groups * heads_step

    def from_columns(slot):
        part = cols[:, :, slot * heads_step : (slot + 1) * heads_step]
        return part.transpose(1, 0, 2).reshape(length, heads)

    upward = from_columns(0) + rows.reshape(heads, length).T
    onward = from_columns(1)
    dstep = from_columns(2)
    spans = jnp.sum(span[:, ::8].reshape(groups, chunks, heads_step, head_size), axis=3)
    spans = spans.transpose(1, 0, 2).reshape(chunks, 1, heads)
    places = jnp.arange(CHUNK)
    at_or_after = (places[None, :] >= places[:, None]).astype(F32)
    ahead = (places[None, :] < places[:, None]).astype(F32)
    dlog = (
        jnp.einsum(
            "rt,cth->crh", at_or_after, upward.reshape(chunks, CHUNK, heads), precision=HIGHEST
        )
        + jnp.einsum("rs,csh->crh", ahead, onward.reshape(chunks, CHUNK, heads), precision=HIGHEST)
        + spans
    ).reshape(length, heads)
    return dxr, dbs, dcs, dstep, dlog, sums


def swap_pair(values):
    return lax.ppermute(values, "tensor", [(0, 1), (1, 0)])


def gather_pair(own, place):
    joined = jnp.concatenate([own, swap_pair(own), own], axis=0)
    return lax.dynamic_slice_in_dim(joined, place * own.shape[0], 2 * own.shape[0])


def scatter_pair(values, place):
    half = values.shape[0] // 2
    sent = lax.dynamic_slice_in_dim(values, (1 - place) * half, half)
    kept = lax.dynamic_slice_in_dim(values, place * half, half)
    return kept + swap_pair(sent)


def stage_orders(size):
    bits = size.bit_length() - 1
    if bits == 4:
        return ((0, 1, 2, 3), (1, 2, 3, 0), (2, 0, 1, 3))
    return tuple(tuple((bit + turn) % bits for bit in range(bits)) for turn in range(3))


def partner(values, bit):
    size = lax.axis_size("dp")
    return lax.ppermute(values, "dp", [(i, i ^ (1 << bit)) for i in range(size)])


def place_kernel(table, *refs):
    out = refs[-1]
    start = 0
    for ref in refs[:-1]:
        width = ref.shape[2]
        out[:, start : start + width] = ref[0]
        start += width


def gather_rows(shard):
    size, index = lax.axis_size("dp"), lax.axis_index("dp")
    orders = stage_orders(size)
    rows, width = shard.shape[0], shard.shape[1] // len(orders)
    targets = jnp.arange(size, dtype=jnp.int32) ^ index.astype(jnp.int32)
    pieces = [shard[None, :, turn * width : (turn + 1) * width] for turn in range(len(orders))]
    tables = []
    for order in orders:
        stages = order[::-1]
        tables.append(sum(((targets >> bit) & 1) << stage for stage, bit in enumerate(stages)))
    for stage in range(size.bit_length() - 1):
        pieces = [
            jnp.concatenate([piece, partner(piece, order[::-1][stage])], axis=0)
            for piece, order in zip(pieces, orders)
        ]

    def piece_spec(turn):
        return pl.BlockSpec((1, rows, width), lambda d, table: (table[turn, d], 0, 0))

    return pl.pallas_call(
        place_kernel,
        grid_spec=pltpu.PrefetchScalarGridSpec(
            num_scalar_prefetch=1,
            grid=(size,),
            in_specs=[piece_spec(turn) for turn in range(len(orders))],
            out_specs=pl.BlockSpec((rows, shard.shape[1]), lambda d, table: (d, 0)),
        ),
        out_shape=jax.ShapeDtypeStruct((size * rows, shard.shape[1]), shard.dtype),
        cost_estimate=pl.CostEstimate(
            flops=0, bytes_accessed=4 * size * shard.size, transcendentals=0
        ),
        name="place_rows",
    )(jnp.stack(tables), *pieces)


def scatter_rows(values):
    size, index = lax.axis_size("dp"), lax.axis_index("dp")
    bits = size.bit_length() - 1
    orders = stage_orders(size)
    width = values.shape[1] // len(orders)
    rows = values.shape[0] // size
    held, left = [], []
    for turn in range(len(orders)):
        piece = values[:, turn * width : (turn + 1) * width]
        held.append(piece.reshape((2,) * bits + (rows, width)))
        left.append(list(range(bits - 1, -1, -1)))
    for stage in range(bits):
        for turn, order in enumerate(orders):
            bit = order[stage]
            axis = left[turn].index(bit)
            mine = (index >> bit) & 1
            sent = lax.dynamic_index_in_dim(held[turn], 1 - mine, axis, keepdims=False)
            kept = lax.dynamic_index_in_dim(held[turn], mine, axis, keepdims=False)
            got = partner(sent.astype(BF16), bit)
            held[turn] = kept.astype(F32) + got.astype(F32)
            left[turn].pop(axis)
    return jnp.concatenate(held, axis=1)


def sum_small(values):
    for bit in range(lax.axis_size("dp").bit_length() - 1):
        values = values + partner(values, bit)
    return values


def shards(
    tokens,
    segment_ids,
    norm_gain,
    in_gate_inner,
    in_state,
    in_step,
    conv_inner,
    conv_inner_bias,
    conv_state,
    conv_state_bias,
    step_bias,
    decay_log,
    skip_gain,
    gate_gain,
    out_proj,
    cotangent,
):
    half_rows = tokens.shape[0]
    model_width = tokens.shape[1]
    tensor_place = lax.axis_index("tensor")
    own_segment = lax.dynamic_slice_in_dim(segment_ids, tensor_place * half_rows, half_rows)
    own_live = (own_segment >= 0).astype(F32)[:, None]
    own_rows = tokens.astype(F32)
    row_scale = lax.rsqrt(jnp.mean(own_rows * own_rows, axis=1, keepdims=True) + EPSILON)
    normed_own = (own_rows * row_scale * norm_gain[None, :]).astype(BF16)
    width, _, inner_dev = in_gate_inner.shape
    state_dim = in_state.shape[2]
    heads_dev = in_step.shape[1]
    head_size = inner_dev // heads_dev
    step_pad = -heads_dev % 128
    first_shard = jnp.concatenate(
        [
            in_gate_inner[:, 1],
            in_state.reshape(width, -1),
            in_step,
            jnp.zeros((width, step_pad), BF16),
        ],
        axis=1,
    )
    first_weights = gather_rows(first_shard)
    later_shard = jnp.concatenate([in_gate_inner[:, 0], out_proj.T], axis=1)
    later_weights = gather_rows(later_shard)
    normed = gather_pair(normed_own, tensor_place)
    first_proj = dot(normed, first_weights)
    state_end = inner_dev + 2 * state_dim
    inner_proj = first_proj[:, :inner_dev]
    state_proj = first_proj[:, inner_dev:state_end]
    step_proj = first_proj[:, state_end : state_end + heads_dev]

    def state_piece(state_values, conv_taps, conv_bias):
        return jax.nn.silu(
            causal_conv(
                state_values,
                conv_taps.reshape(conv_taps.shape[0], -1),
                conv_bias.reshape(-1),
                segment_ids,
            )
        )

    state_act, state_back = jax.vjp(state_piece, state_proj, conv_state, conv_state_bias)
    bs_low = state_act[:, :state_dim].astype(BF16)
    cs_low = state_act[:, state_dim:].astype(BF16)
    step_size = jax.nn.softplus(step_proj + step_bias[None, :])
    decay_rate = -jnp.exp(decay_log)
    log_decay = step_size * decay_rate[None, :]
    terms = chunk_terms(step_size, log_decay, segment_ids, head_size)
    skip_row = jnp.repeat(skip_gain, head_size)[None]
    bias_row = conv_inner_bias[None]
    mixed, states, score = ssd_forward(
        inner_proj, conv_inner, bias_row, skip_row, terms, bs_low, cs_low
    )
    gate_weights = later_weights[:, :inner_dev]
    out_weights_t = later_weights[:, inner_dev:]
    gate_proj = dot(normed, gate_weights)
    gate_sigmoid = jax.nn.sigmoid(gate_proj)
    gated_values = mixed * (gate_proj * gate_sigmoid)
    full_inner = inner_dev * lax.axis_size("tensor")
    squares = lax.psum(jnp.sum(gated_values * gated_values, axis=1), "tensor")
    gate_scale = lax.rsqrt(squares / full_inner + EPSILON)[:, None]
    normed_inner = (gated_values * gate_scale * gate_gain[None, :]).astype(BF16)
    partial_out = jnp.einsum(
        "tc,dc->td", normed_inner, out_weights_t, preferred_element_type=F32
    )
    branch_own = scatter_pair(partial_out, tensor_place)
    block_out = (own_rows + own_live * branch_own).astype(BF16)
    cot_rows = cotangent.astype(F32)
    branch_grad_own = (own_live * cot_rows).astype(BF16)
    branch_grad = gather_pair(branch_grad_own, tensor_place)
    grad_out_proj_t = jnp.einsum(
        "td,tc->dc", branch_grad, normed_inner, preferred_element_type=F32
    )
    grad_normed_inner = jnp.einsum(
        "td,dc->tc", branch_grad, out_weights_t, preferred_element_type=F32
    )
    grad_gate_gain = jnp.sum(grad_normed_inner * gated_values * gate_scale, axis=0)
    scaled_grad = grad_normed_inner * gate_gain[None, :]
    products = lax.psum(jnp.sum(scaled_grad * gated_values, axis=1), "tensor")
    grad_gated = (
        gate_scale * scaled_grad - gated_values * gate_scale**3 * (products / full_inner)[:, None]
    )
    low_gate = (
        grad_gated * mixed * (gate_sigmoid * (1.0 + gate_proj * (1.0 - gate_sigmoid)))
    ).astype(BF16)
    grad_mixed = grad_gated * (gate_proj * gate_sigmoid)
    grad_gate_half = jnp.einsum(
        "td,tc->dc", normed, low_gate, preferred_element_type=F32
    ).astype(BF16)
    grad_out_low = grad_out_proj_t.astype(BF16)
    grad_mixed, grad_gate_half, grad_out_low = lax.optimization_barrier(
        (grad_mixed, grad_gate_half, grad_out_low)
    )
    gate_part = scatter_rows(grad_gate_half)
    out_part = scatter_rows(grad_out_low)
    low_inner, grad_bs, grad_cs, grad_step_size, grad_log, inner_sums = ssd_backward(
        inner_proj, conv_inner, bias_row, skip_row, terms, score, bs_low, cs_low, states, grad_mixed
    )
    taps_count = conv_inner.shape[0]
    grad_conv_inner = inner_sums[:taps_count][::-1]
    grad_conv_inner_bias = inner_sums[taps_count]
    grad_skip_gain = jnp.sum(inner_sums[taps_count + 1].reshape(heads_dev, head_size), axis=1)
    grad_decay_log = jnp.sum(grad_log * log_decay, axis=0)
    grad_step_proj = (grad_step_size + grad_log * decay_rate[None, :]) * jax.nn.sigmoid(
        step_proj + step_bias[None, :]
    )
    grad_step_bias = jnp.sum(grad_step_proj, axis=0)
    grad_state_part = jnp.concatenate([grad_bs, grad_cs], axis=1)
    grad_state_act = grad_state_part + swap_pair(grad_state_part)
    grad_state_proj, grad_conv_state, grad_conv_state_bias = state_back(grad_state_act)
    low_state = grad_state_proj.astype(BF16)
    low_step = grad_step_proj.astype(BF16)
    own_state = low_state * (tensor_place == 0).astype(BF16)
    low_pad = jnp.zeros((low_step.shape[0], step_pad), BF16)
    low_first = jnp.concatenate([low_inner, low_state, low_step, low_pad], axis=1)
    grad_first = jnp.einsum(
        "td,tc->dc", normed, low_first, preferred_element_type=F32
    ).astype(BF16)
    first_part = scatter_rows(grad_first)
    grad_out_proj = out_part.T
    grad_in_gate_inner = jnp.stack([gate_part, first_part[:, :inner_dev]], axis=1)
    grad_in_state = first_part[:, inner_dev:state_end].reshape(in_state.shape)
    grad_in_step = first_part[:, state_end : state_end + heads_dev]
    low_heads = jnp.concatenate([low_inner, own_state, low_step, low_pad], axis=1)
    head_grads = dot_nt(low_gate, gate_weights) + dot_nt(low_heads, first_weights)
    normed_grad_own = scatter_pair(head_grads, tensor_place)
    grad_norm_part = jnp.sum(normed_grad_own * own_rows * row_scale, axis=0)
    scaled_rows = normed_grad_own * norm_gain[None, :]
    row_products = jnp.sum(scaled_rows * own_rows, axis=1, keepdims=True)
    grad_tokens = (
        cot_rows + row_scale * scaled_rows - own_rows * row_scale**3 * row_products / model_width
    )
    small_parts = (
        grad_norm_part + swap_pair(grad_norm_part),
        grad_conv_inner,
        grad_conv_inner_bias,
        grad_conv_state,
        grad_conv_state_bias,
        grad_step_bias,
        grad_decay_log,
        grad_skip_gain,
        grad_gate_gain,
    )
    summed = sum_small(jnp.concatenate([part.reshape(-1) for part in small_parts]))
    small, start = [], 0
    for part in small_parts:
        small.append(summed[start : start + part.size].reshape(part.shape))
        start += part.size
    return (
        block_out,
        grad_tokens,
        small[0],
        grad_in_gate_inner,
        grad_in_state,
        grad_in_step,
        *small[1:],
        grad_out_proj,
    )


def solution(mesh):
    in_specs = (
        P(("dp", "tensor"), None),
        P("dp"),
        P(),
        P("dp", None, "tensor"),
        P("dp", None, None),
        P("dp", "tensor"),
        P(None, "tensor"),
        P("tensor"),
        P(),
        P(),
        P("tensor"),
        P("tensor"),
        P("tensor"),
        P("tensor"),
        P("tensor", "dp"),
        P(("dp", "tensor"), None),
    )
    out_specs = (
        P(("dp", "tensor"), None),
        P(("dp", "tensor"), None),
        P(),
        P("dp", None, "tensor"),
        P("dp", None, None),
        P("dp", "tensor"),
        P(None, "tensor"),
        P("tensor"),
        P(),
        P(),
        P("tensor"),
        P("tensor"),
        P("tensor"),
        P("tensor"),
        P("tensor", "dp"),
    )
    return jax.shard_map(shards, mesh=mesh, in_specs=in_specs, out_specs=out_specs, check_vma=False)
```

```python
import jax
import jax.numpy as jnp
from jax import lax
from jax.experimental import pallas as pl
from jax.experimental.pallas import tpu as pltpu
from jax.sharding import PartitionSpec as P


EPSILON = 1e-05
HIGHEST = lax.Precision.HIGHEST
CHUNK = 128
HEADS_STEP = 8
F32 = jnp.float32
BF16 = jnp.bfloat16


def shift_down(values, steps_back, filler):
    leading = jnp.full((steps_back,) + values.shape[1:], filler, values.dtype)
    return jnp.concatenate([leading, values[: values.shape[0] - steps_back]], axis=0)


def causal_conv(values, conv_taps, conv_bias, segment):
    taps_count = conv_taps.shape[0]
    result = conv_bias[None, :] + conv_taps[taps_count - 1][None, :] * values
    for steps_back in range(1, taps_count):
        earlier = shift_down(values, steps_back, 0.0)
        same_seq = (shift_down(segment, steps_back, -2) == segment).astype(values.dtype)
        result = (
            result + conv_taps[taps_count - 1 - steps_back][None, :] * earlier * same_seq[:, None]
        )
    return result


def dot(a, b):
    return jnp.dot(a, b, preferred_element_type=F32)


def dot_nt(a, b):
    return lax.dot_general(a, b, (((1,), (1,)), ((), ())), preferred_element_type=F32)


def spread_heads(columns, pair, head_size):
    lane = lax.broadcasted_iota(jnp.int32, (columns.shape[0], 2 * head_size), 1)
    first = columns[:, 2 * pair : 2 * pair + 1]
    second = columns[:, 2 * pair + 1 : 2 * pair + 2]
    return jnp.where(lane < head_size, first, second)


def conv_pair(xr, taps, bias, masks, rows, before, lanes):
    current = xr[rows, lanes]
    joined = jnp.concatenate([xr[before, lanes], current], axis=0)
    count = taps.shape[0]
    value = bias[0:1, lanes] + taps[count - 1 : count, lanes] * current
    shifted = []
    for back in range(1, count):
        piece = pltpu.roll(joined, back, 0)[8:] * masks[back - 1, rows, :]
        shifted.append(piece)
        value = value + taps[count - 1 - back : count - back, lanes] * piece
    return current, shifted, value


def ssd_forward_kernel(
    xr, taps, bias, skip, masks, score, cs, bst, dt, cumc, reach, toend, cumr, kept,
    y_out, states_out, state,
):
    width = xr.shape[1]
    head_size = width // dt.shape[2]
    pair_width = 2 * head_size
    chunks = xr.shape[0] // CHUNK
    state[...] = jnp.zeros_like(state)

    def chunk_body(place, unused):
        start = pl.multiple_of(place * CHUNK, CHUNK)
        rows = pl.ds(start, CHUNK)
        before = pl.ds(pl.multiple_of(jnp.maximum(start - 8, 0), 8), 8)
        dt_cols, cum_cols = dt[0, rows, :], cumc[0, rows, :]
        reach_cols, end_cols = reach[0, rows, :], toend[0, rows, :]
        score_now, cs_now, bst_now = score[rows, :], cs[rows, :], bst[:, rows]
        lane = lax.broadcasted_iota(jnp.int32, (CHUNK, pair_width), 1)
        row_of = pl.ds(pl.multiple_of(place * 8, 8), 8)
        for pair in range(width // pair_width):
            lanes = slice(pair * pair_width, (pair + 1) * pair_width)
            _, _, value = conv_pair(
                xr, taps, bias, masks, rows, before, lanes
            )
            x = value * jax.nn.sigmoid(value)
            xdt = x * spread_heads(dt_cols, pair, head_size)
            xb = xdt.astype(BF16)
            held = state[:, lanes]
            held_low = held.astype(BF16)
            states_out[rows, lanes] = held_low
            halves = []
            for head in (2 * pair, 2 * pair + 1):
                spread = cum_cols[:, head : head + 1] - cumr[0, head : head + 1, rows]
                mixing = score_now * jnp.exp(jnp.minimum(spread, 0.0))
                halves.append(dot(mixing.astype(BF16), xb))
            y = jnp.where(lane < head_size, halves[0], halves[1])
            y = y + spread_heads(reach_cols, pair, head_size) * dot(cs_now, held_low)
            y_out[rows, lanes] = y + skip[0:1, lanes] * x
            fresh = dot(bst_now, (xdt * spread_heads(end_cols, pair, head_size)).astype(BF16))
            state[:, lanes] = fresh + kept[0, row_of, lanes][0:1] * held
        return unused

    lax.fori_loop(0, chunks, chunk_body, 0)


def ssd_backward_kernel(
    xr, taps, bias, skip, masks, score_t, cs, bs, cst, pick, dt, cumc, reach, toend, cumr, kept,
    states, dy,
    dxr_out, dscore_out, dbs_out, dcs_out, cols_out, rows_out, span_out, sums_out,
    dstate, dvalue_next,
):
    width = xr.shape[1]
    head_size = width // dt.shape[2]
    pair_width = 2 * head_size
    length = xr.shape[0]
    chunks = length // CHUNK
    count = taps.shape[0]
    dstate[...] = jnp.zeros_like(dstate)
    dvalue_next[...] = jnp.zeros_like(dvalue_next)
    sums_out[...] = jnp.zeros_like(sums_out)

    @pl.when(pl.program_id(0) == 0)
    def clear():
        dscore_out[...] = jnp.zeros_like(dscore_out)
        dbs_out[...] = jnp.zeros_like(dbs_out)
        dcs_out[...] = jnp.zeros_like(dcs_out)

    def chunk_body(step, unused):
        place = chunks - 1 - step
        start = pl.multiple_of(place * CHUNK, CHUNK)
        rows = pl.ds(start, CHUNK)
        before = pl.ds(pl.multiple_of(jnp.maximum(start - 8, 0), 8), 8)
        after = pl.ds(pl.multiple_of(jnp.minimum(start + CHUNK, length - 8), 8), 8)
        dt_cols, cum_cols = dt[0, rows, :], cumc[0, rows, :]
        reach_cols, end_cols = reach[0, rows, :], toend[0, rows, :]
        score_now, cs_now, bs_now, cst_now = score_t[rows, :], cs[rows, :], bs[rows, :], cst[:, rows]
        lane = lax.broadcasted_iota(jnp.int32, (CHUNK, pair_width), 1)
        row_of = pl.ds(pl.multiple_of(place * 8, 8), 8)
        dscore = jnp.zeros((CHUNK, CHUNK), F32)
        dbs = jnp.zeros((CHUNK, bs_now.shape[1]), F32)
        dcs = jnp.zeros((CHUNK, bs_now.shape[1]), F32)
        columns = jnp.zeros((CHUNK, cols_out.shape[2]), F32)
        column_lane = lax.broadcasted_iota(jnp.int32, columns.shape, 1)
        for pair in range(width // pair_width):
            lanes = slice(pair * pair_width, (pair + 1) * pair_width)
            current, shifted, value = conv_pair(xr, taps, bias, masks, rows, before, lanes)
            gate = jax.nn.sigmoid(value)
            x = value * gate
            dt_now = spread_heads(dt_cols, pair, head_size)
            end_now = spread_heads(end_cols, pair, head_size)
            xdt = x * dt_now
            xb = xdt.astype(BF16)
            dy_now = dy[rows, lanes]
            dyb = dy_now.astype(BF16)
            held_low = states[rows, lanes]
            dheld = dstate[:, lanes]
            dheld_low = dheld.astype(BF16)
            dyr = dy_now * spread_heads(reach_cols, pair, head_size)
            dyr_low = dyr.astype(BF16)
            from_state = dyr * dot(cs_now, held_low)
            dcs = dcs + dot_nt(dyr_low, held_low)
            dxdt_end = end_now * dot(bs_now, dheld_low)
            dbs = dbs + dot_nt((xdt * end_now).astype(BF16), dheld_low)
            halves = []
            for side in (0, 1):
                head = 2 * pair + side
                spread = cumr[0, head : head + 1, rows] - cum_cols[:, head : head + 1]
                decay = jnp.exp(jnp.minimum(spread, 0.0))
                weight = score_now * decay
                own = (lane < head_size) if side == 0 else (lane >= head_size)
                pairs = dot_nt(jnp.where(own, xdt, 0.0).astype(BF16), dyb)
                dscore = dscore + pairs * decay
                share = pairs * weight
                columns = columns - jnp.where(
                    column_lane == head, jnp.sum(share, axis=1, keepdims=True), 0.0
                )
                rows_out[0, head : head + 1, rows] = jnp.sum(share, axis=0, keepdims=True)
                halves.append(dot(weight.astype(BF16), dyb))
            dxdt = jnp.where(lane < head_size, halves[0], halves[1]) + dxdt_end
            picked = jnp.concatenate(
                [
                    from_state.astype(BF16),
                    (xdt * dxdt_end).astype(BF16),
                    (x * dxdt).astype(BF16),
                ],
                axis=1,
            )
            columns = columns + dot(picked, pick[pair])
            dx = skip[0:1, lanes] * dy_now + dt_now * dxdt
            kept_row = kept[0, row_of, lanes][0:1]
            span_row = kept_row * jnp.sum(dheld * held_low.astype(F32), axis=0, keepdims=True)
            span_out[0, row_of, lanes] = jnp.broadcast_to(span_row, (8, pair_width))
            dstate[:, lanes] = kept_row * dheld + dot(cst_now, dyr_low)
            dvalue = dx * (gate * (1.0 + value * (1.0 - gate)))
            dxr = taps[count - 1 : count, lanes] * dvalue
            next_rows = dvalue_next[:, lanes]
            sums = [jnp.sum(dvalue * current, axis=0, keepdims=True)]
            for back in range(1, count):
                masked = dvalue * masks[back - 1, rows, :]
                joined = jnp.concatenate(
                    [masked, next_rows * masks[back - 1, after, :]], axis=0
                )
                lifted = pltpu.roll(joined, CHUNK + 8 - back, 0)[:CHUNK]
                dxr = dxr + taps[count - 1 - back : count - back, lanes] * lifted
                sums.append(jnp.sum(dvalue * shifted[back - 1], axis=0, keepdims=True))
            dvalue_next[:, lanes] = dvalue[:8]
            sums.append(jnp.sum(dvalue, axis=0, keepdims=True))
            sums.append(jnp.sum(dy_now * x, axis=0, keepdims=True))
            for slot, row in enumerate(sums):
                sums_out[slot : slot + 1, lanes] += row
            dxr_out[rows, lanes] = dxr.astype(dxr_out.dtype)
        dscore_out[rows, :] += dscore
        dbs_out[rows, :] += dbs
        dcs_out[rows, :] += dcs
        cols_out[0, rows, :] = columns
        return unused

    lax.fori_loop(0, chunks, chunk_body, 0)


def chunk_terms(step_size, log_decay, segment, head_size):
    length, heads = step_size.shape
    chunks, groups = length // CHUNK, heads // HEADS_STEP
    parted = segment.reshape(chunks, CHUNK)
    places = jnp.arange(CHUNK)
    lower = (places[:, None] >= places[None, :]).astype(F32)
    allowed = (
        (parted[:, :, None] == parted[:, None, :]) & (places[:, None] >= places[None, :])[None]
    ).astype(F32)
    cumulative = jnp.einsum(
        "ts,csh->cth", lower, log_decay.reshape(chunks, CHUNK, heads), precision=HIGHEST
    )
    last = jnp.concatenate([jnp.full((1,), -2, segment.dtype), parted[:-1, CHUNK - 1]])
    carried = (parted == last[:, None]).astype(F32)
    final = parted[:, CHUNK - 1]
    at_end = (parted == final[:, None]).astype(F32)
    total = cumulative[:, CHUNK - 1]
    reach = jnp.exp(cumulative) * carried[:, :, None]
    to_end = jnp.exp(total[:, None, :] - cumulative) * at_end[:, :, None]
    kept = jnp.exp(total) * (final == last).astype(F32)[:, None]

    def by_group(array):
        return array.reshape(length, groups, HEADS_STEP).transpose(1, 0, 2)

    columns = tuple(by_group(a.reshape(length, heads)) for a in (step_size, cumulative, reach, to_end))
    cum_rows = cumulative.reshape(length, heads).T.reshape(groups, HEADS_STEP, length)
    kept_rows = jnp.repeat(kept, head_size, axis=1).reshape(chunks, groups, -1).transpose(1, 0, 2)
    kept_rows = jnp.repeat(kept_rows, 8, axis=1)
    masks = jnp.stack(
        [
            jnp.broadcast_to(
                (shift_down(segment, back, -2) == segment).astype(F32)[:, None],
                (length, 2 * head_size),
            )
            for back in (1, 2, 3)
        ]
    )
    return allowed, columns, cum_rows, kept_rows, masks


def whole_spec(array):
    zeros = (0,) * array.ndim
    return pl.BlockSpec(array.shape, lambda g: zeros)


def group_spec(array):
    rest = (0,) * (array.ndim - 1)
    return pl.BlockSpec((1,) + array.shape[1:], lambda g: (g,) + rest)


def lanes_spec(array, width):
    return pl.BlockSpec((array.shape[0], width), lambda g: (0, g))


def ssd_forward(xr, taps, bias, skip_row, terms, bs_low, cs_low):
    allowed, columns, cum_rows, kept_rows, masks = terms
    length, inner = xr.shape
    groups = cum_rows.shape[0]
    width = inner // groups
    state_dim = bs_low.shape[1]
    chunks = length // CHUNK
    score = (
        jnp.einsum(
            "ctn,csn->cts",
            cs_low.reshape(chunks, CHUNK, state_dim),
            bs_low.reshape(chunks, CHUNK, state_dim),
            preferred_element_type=F32,
        )
        * allowed
    )
    shared = (masks, score.reshape(length, CHUNK), cs_low, bs_low.T)
    grouped = (*columns, cum_rows, kept_rows)
    y, states = pl.pallas_call(
        ssd_forward_kernel,
        grid=(groups,),
        in_specs=[lanes_spec(a, width) for a in (xr, taps, bias, skip_row)]
        + [whole_spec(a) for a in shared]
        + [group_spec(a) for a in grouped],
        out_specs=[
            pl.BlockSpec((length, width), lambda g: (0, g)),
            pl.BlockSpec((chunks * state_dim, width), lambda g: (0, g)),
        ],
        out_shape=[
            jax.ShapeDtypeStruct((length, inner), F32),
            jax.ShapeDtypeStruct((chunks * state_dim, inner), BF16),
        ],
        scratch_shapes=[pltpu.VMEM((state_dim, width), F32)],
        cost_estimate=pl.CostEstimate(
            flops=130 * length * inner * CHUNK, bytes_accessed=12 * length * inner, transcendentals=0
        ),
        name="ssd_forward",
    )(xr, taps, bias, skip_row, *shared, *grouped)
    return y, states, score


def ssd_backward(xr, taps, bias, skip_row, terms, score, bs_low, cs_low, states, dy):
    allowed, columns, cum_rows, kept_rows, masks = terms
    length, inner = xr.shape
    groups, heads_step = cum_rows.shape[:2]
    width = inner // groups
    head_size = width // heads_step
    state_dim = bs_low.shape[1]
    chunks = length // CHUNK
    lane = jnp.arange(2 * head_size) // head_size
    pick = jnp.stack(
        [
            jnp.concatenate(
                [
                    (
                        (2 * pair + lane + slot * heads_step)[:, None] == jnp.arange(CHUNK)[None, :]
                    ).astype(BF16)
                    for slot in range(3)
                ]
            )
            for pair in range(heads_step // 2)
        ]
    )
    score_t = score.transpose(0, 2, 1).reshape(length, CHUNK)
    shared = (masks, score_t, cs_low, bs_low, cs_low.T, pick)
    grouped = (*columns, cum_rows, kept_rows)
    fixed = pl.BlockSpec((length, CHUNK), lambda g: (0, 0))
    out = pl.pallas_call(
        ssd_backward_kernel,
        grid=(groups,),
        in_specs=[lanes_spec(a, width) for a in (xr, taps, bias, skip_row)]
        + [whole_spec(a) for a in shared]
        + [group_spec(a) for a in grouped]
        + [lanes_spec(a, width) for a in (states, dy)],
        out_specs=[
            pl.BlockSpec((length, width), lambda g: (0, g)),
            fixed,
            pl.BlockSpec((length, state_dim), lambda g: (0, 0)),
            pl.BlockSpec((length, state_dim), lambda g: (0, 0)),
            pl.BlockSpec((1, length, CHUNK), lambda g: (g, 0, 0)),
            pl.BlockSpec((1, heads_step, length), lambda g: (g, 0, 0)),
            pl.BlockSpec((1, 8 * chunks, width), lambda g: (g, 0, 0)),
            pl.BlockSpec((8, width), lambda g: (0, g)),
        ],
        out_shape=[
            jax.ShapeDtypeStruct((length, inner), BF16),
            jax.ShapeDtypeStruct((length, CHUNK), F32),
            jax.ShapeDtypeStruct((length, state_dim), F32),
            jax.ShapeDtypeStruct((length, state_dim), F32),
            jax.ShapeDtypeStruct((groups, length, CHUNK), F32),
            jax.ShapeDtypeStruct((groups, heads_step, length), F32),
            jax.ShapeDtypeStruct((groups, 8 * chunks, width), F32),
            jax.ShapeDtypeStruct((8, inner), F32),
        ],
        scratch_shapes=[pltpu.VMEM((state_dim, width), F32), pltpu.VMEM((8, width), F32)],
        cost_estimate=pl.CostEstimate(
            flops=290 * length * inner * CHUNK, bytes_accessed=16 * length * inner, transcendentals=0
        ),
        name="ssd_backward",
    )(xr, taps, bias, skip_row, *shared, *grouped, states, dy)
    dxr, dscore_t, dbs, dcs, cols, rows, span, sums = out
    dscore_t = (dscore_t.reshape(chunks, CHUNK, CHUNK) * allowed.transpose(0, 2, 1)).astype(BF16)
    parted_c = cs_low.reshape(chunks, CHUNK, state_dim)
    parted_b = bs_low.reshape(chunks, CHUNK, state_dim)
    from_score_b = jnp.einsum("cst,ctn->csn", dscore_t, parted_c, preferred_element_type=F32)
    from_score_c = jnp.einsum("cst,csn->ctn", dscore_t, parted_b, preferred_element_type=F32)
    dbs = dbs + from_score_b.reshape(length, state_dim)
    dcs = dcs + from_score_c.reshape(length, state_dim)
    heads = groups * heads_step

    def from_columns(slot):
        part = cols[:, :, slot * heads_step : (slot + 1) * heads_step]
        return part.transpose(1, 0, 2).reshape(length, heads)

    upward = from_columns(0) + rows.reshape(heads, length).T
    onward = from_columns(1)
    dstep = from_columns(2)
    spans = jnp.sum(span[:, ::8].reshape(groups, chunks, heads_step, head_size), axis=3)
    spans = spans.transpose(1, 0, 2).reshape(chunks, 1, heads)
    places = jnp.arange(CHUNK)
    at_or_after = (places[None, :] >= places[:, None]).astype(F32)
    ahead = (places[None, :] < places[:, None]).astype(F32)
    dlog = (
        jnp.einsum(
            "rt,cth->crh", at_or_after, upward.reshape(chunks, CHUNK, heads), precision=HIGHEST
        )
        + jnp.einsum("rs,csh->crh", ahead, onward.reshape(chunks, CHUNK, heads), precision=HIGHEST)
        + spans
    ).reshape(length, heads)
    return dxr, dbs, dcs, dstep, dlog, sums


def swap_pair(values):
    return lax.ppermute(values, "tensor", [(0, 1), (1, 0)])


def gather_pair(own, place):
    joined = jnp.concatenate([own, swap_pair(own), own], axis=0)
    return lax.dynamic_slice_in_dim(joined, place * own.shape[0], 2 * own.shape[0])


def scatter_pair(values, place):
    half = values.shape[0] // 2
    sent = lax.dynamic_slice_in_dim(values, (1 - place) * half, half)
    kept = lax.dynamic_slice_in_dim(values, place * half, half)
    return kept + swap_pair(sent)


def stage_orders(size):
    bits = size.bit_length() - 1
    if bits == 4:
        return ((0, 1, 2, 3), (1, 2, 3, 0), (2, 0, 1, 3))
    return tuple(tuple((bit + turn) % bits for bit in range(bits)) for turn in range(3))


def partner(values, bit):
    size = lax.axis_size("dp")
    return lax.ppermute(values, "dp", [(i, i ^ (1 << bit)) for i in range(size)])


def place_kernel(table, *refs):
    sources, (out, buffer, arrived, left) = refs[:-4], refs[-4:]
    turns, size = len(sources) // 2, out.shape[0]
    half = size // 2
    width = sources[0].shape[2]

    def arrival(turn, source, block, target):
        lanes = pl.ds(turn * width, width)
        return pltpu.make_async_copy(
            source.at[block], buffer.at[target, :, lanes], arrived.at[turn, target]
        )

    def start_in(target, unused):
        for turn in range(turns):
            block = table[turn, target]

            @pl.when(block < half)
            def from_own():
                arrival(turn, sources[2 * turn], block, target).start()

            @pl.when(block >= half)
            def from_other():
                arrival(turn, sources[2 * turn + 1], block - half, target).start()

        return unused

    def start_out(target, unused):
        for turn in range(turns):
            arrival(turn, sources[2 * turn], 0, target).wait()
        pltpu.make_async_copy(buffer.at[target], out.at[target], left.at[target]).start()
        return unused

    def finish(target, unused):
        pltpu.make_async_copy(buffer.at[target], out.at[target], left.at[target]).wait()
        return unused

    lax.fori_loop(0, size, start_in, 0)
    lax.fori_loop(0, size, start_out, 0)
    lax.fori_loop(0, size, finish, 0)


def gather_stages(pieces, first_stage, last_stage):
    orders = stage_orders(lax.axis_size("dp"))
    for stage in range(first_stage, last_stage):
        joined = []
        for piece, order in zip(pieces, orders):
            other = partner(piece, order[::-1][stage])
            if stage == len(order) - 1:
                joined.append((piece, other))
            else:
                joined.append(jnp.concatenate([piece, other], axis=0))
        pieces = joined
    return pieces


def split_shard(shard):
    turns = len(stage_orders(lax.axis_size("dp")))
    width = shard.shape[1] // turns
    return [shard[None, :, turn * width : (turn + 1) * width] for turn in range(turns)]


def place_rows(pieces):
    size, index = lax.axis_size("dp"), lax.axis_index("dp")
    orders = stage_orders(size)
    targets = jnp.arange(size, dtype=jnp.int32) ^ index.astype(jnp.int32)
    tables = [
        sum(((targets >> bit) & 1) << stage for stage, bit in enumerate(order[::-1]))
        for order in orders
    ]
    _, rows, width = pieces[0][0].shape
    sources = [part for pair in pieces for part in pair]
    shape = (size, rows, width * len(orders))
    placed = pl.pallas_call(
        place_kernel,
        in_specs=[pl.BlockSpec(memory_space=pltpu.SMEM)]
        + [pl.BlockSpec(memory_space=pl.ANY)] * len(sources),
        out_specs=pl.BlockSpec(memory_space=pl.ANY),
        out_shape=jax.ShapeDtypeStruct(shape, BF16),
        scratch_shapes=[
            pltpu.VMEM(shape, BF16),
            pltpu.SemaphoreType.DMA((len(orders), size)),
            pltpu.SemaphoreType.DMA((size,)),
        ],
        cost_estimate=pl.CostEstimate(
            flops=0, bytes_accessed=4 * size * rows * shape[2], transcendentals=0
        ),
        name="place_rows",
    )(jnp.stack(tables), *sources)
    return placed.reshape(size * rows, shape[2])


def scatter_rows(pieces):
    size, index = lax.axis_size("dp"), lax.axis_index("dp")
    bits = size.bit_length() - 1
    orders = stage_orders(size)
    held, left = [], []
    for piece in pieces:
        held.append(piece.reshape((2,) * bits + (piece.shape[0] // size, piece.shape[1])))
        left.append(list(range(bits - 1, -1, -1)))
    for stage in range(bits):
        for turn, order in enumerate(orders):
            bit = order[stage]
            axis = left[turn].index(bit)
            mine = (index >> bit) & 1
            sent = lax.dynamic_index_in_dim(held[turn], 1 - mine, axis, keepdims=False)
            kept = lax.dynamic_index_in_dim(held[turn], mine, axis, keepdims=False)
            got = partner(sent.astype(BF16), bit)
            held[turn] = kept.astype(F32) + got.astype(F32)
            left[turn].pop(axis)
    return held


def column_thirds(values):
    width = values.shape[1] // 3
    return [values[:, turn * width : (turn + 1) * width] for turn in range(3)]


def sum_small(values):
    for bit in range(lax.axis_size("dp").bit_length() - 1):
        values = values + partner(values, bit)
    return values


def shards(
    tokens,
    segment_ids,
    norm_gain,
    in_gate_inner,
    in_state,
    in_step,
    conv_inner,
    conv_inner_bias,
    conv_state,
    conv_state_bias,
    step_bias,
    decay_log,
    skip_gain,
    gate_gain,
    out_proj,
    cotangent,
):
    half_rows = tokens.shape[0]
    model_width = tokens.shape[1]
    tensor_place = lax.axis_index("tensor")
    own_segment = lax.dynamic_slice_in_dim(segment_ids, tensor_place * half_rows, half_rows)
    own_live = (own_segment >= 0).astype(F32)[:, None]
    own_rows = tokens.astype(F32)
    row_scale = lax.rsqrt(jnp.mean(own_rows * own_rows, axis=1, keepdims=True) + EPSILON)
    normed_own = (own_rows * row_scale * norm_gain[None, :]).astype(BF16)
    width, _, inner_dev = in_gate_inner.shape
    state_dim = in_state.shape[2]
    heads_dev = in_step.shape[1]
    head_size = inner_dev // heads_dev
    step_pad = -heads_dev % 128
    first_shard = jnp.concatenate(
        [
            in_gate_inner[:, 1],
            in_state.reshape(width, -1),
            in_step,
            jnp.zeros((width, step_pad), BF16),
        ],
        axis=1,
    )
    bits = lax.axis_size("dp").bit_length() - 1
    first_pieces = gather_stages(split_shard(first_shard), 0, bits)
    later_shard = jnp.concatenate([in_gate_inner[:, 0], out_proj.T], axis=1)
    later_pieces = gather_stages(split_shard(later_shard), 0, 2)
    first_pieces, later_pieces = lax.optimization_barrier((first_pieces, later_pieces))
    later_pieces = gather_stages(later_pieces, 2, bits)
    first_weights = place_rows(first_pieces)
    normed = gather_pair(normed_own, tensor_place)
    first_proj = dot(normed, first_weights)
    state_end = inner_dev + 2 * state_dim
    inner_proj = first_proj[:, :inner_dev]
    state_proj = first_proj[:, inner_dev:state_end]
    step_proj = first_proj[:, state_end : state_end + heads_dev]

    def state_piece(state_values, conv_taps, conv_bias):
        return jax.nn.silu(
            causal_conv(
                state_values,
                conv_taps.reshape(conv_taps.shape[0], -1),
                conv_bias.reshape(-1),
                segment_ids,
            )
        )

    state_act, state_back = jax.vjp(state_piece, state_proj, conv_state, conv_state_bias)
    bs_low = state_act[:, :state_dim].astype(BF16)
    cs_low = state_act[:, state_dim:].astype(BF16)
    step_size = jax.nn.softplus(step_proj + step_bias[None, :])
    decay_rate = -jnp.exp(decay_log)
    log_decay = step_size * decay_rate[None, :]
    terms = chunk_terms(step_size, log_decay, segment_ids, head_size)
    skip_row = jnp.repeat(skip_gain, head_size)[None]
    bias_row = conv_inner_bias[None]
    mixed, states, score = ssd_forward(
        inner_proj, conv_inner, bias_row, skip_row, terms, bs_low, cs_low
    )
    later_weights = place_rows(later_pieces)
    gate_weights = later_weights[:, :inner_dev]
    out_weights_t = later_weights[:, inner_dev:]
    gate_proj = dot(normed, gate_weights)
    gate_sigmoid = jax.nn.sigmoid(gate_proj)
    gated_values = mixed * (gate_proj * gate_sigmoid)
    full_inner = inner_dev * lax.axis_size("tensor")
    squares = lax.psum(jnp.sum(gated_values * gated_values, axis=1), "tensor")
    gate_scale = lax.rsqrt(squares / full_inner + EPSILON)[:, None]
    normed_inner = (gated_values * gate_scale * gate_gain[None, :]).astype(BF16)
    partial_out = jnp.einsum(
        "tc,dc->td", normed_inner, out_weights_t, preferred_element_type=F32
    )
    branch_own = scatter_pair(partial_out, tensor_place)
    block_out = (own_rows + own_live * branch_own).astype(BF16)
    cot_rows = cotangent.astype(F32)
    branch_grad_own = (own_live * cot_rows).astype(BF16)
    branch_grad = gather_pair(branch_grad_own, tensor_place)
    grad_out_proj_t = jnp.einsum(
        "td,tc->dc", branch_grad, normed_inner, preferred_element_type=F32
    )
    grad_normed_inner = jnp.einsum(
        "td,dc->tc", branch_grad, out_weights_t, preferred_element_type=F32
    )
    grad_gate_gain = jnp.sum(grad_normed_inner * gated_values * gate_scale, axis=0)
    scaled_grad = grad_normed_inner * gate_gain[None, :]
    products = lax.psum(jnp.sum(scaled_grad * gated_values, axis=1), "tensor")
    grad_gated = (
        gate_scale * scaled_grad - gated_values * gate_scale**3 * (products / full_inner)[:, None]
    )
    low_gate = (
        grad_gated * mixed * (gate_sigmoid * (1.0 + gate_proj * (1.0 - gate_sigmoid)))
    ).astype(BF16)
    grad_mixed = grad_gated * (gate_proj * gate_sigmoid)
    grad_gate_half = jnp.einsum(
        "td,tc->dc", normed, low_gate, preferred_element_type=F32
    ).astype(BF16)
    grad_out_low = grad_out_proj_t.astype(BF16)
    grad_mixed, grad_gate_half, grad_out_low = lax.optimization_barrier(
        (grad_mixed, grad_gate_half, grad_out_low)
    )
    cut = 2 * inner_dev // 3
    early_parts = scatter_rows(
        [
            grad_gate_half[:, :cut],
            jnp.concatenate([grad_gate_half[:, cut:], grad_out_low[:, : 2 * cut - inner_dev]], axis=1),
            grad_out_low[:, 2 * cut - inner_dev :],
        ],
    )
    early_part = jnp.concatenate(early_parts, axis=1)
    gate_part, out_part = early_part[:, :inner_dev], early_part[:, inner_dev:]
    scan_back = ssd_backward(
        inner_proj,
        conv_inner,
        bias_row,
        skip_row,
        terms,
        score,
        bs_low,
        cs_low,
        states,
        grad_mixed,
    )
    low_inner, grad_bs, grad_cs, grad_step_size, grad_log, inner_sums = scan_back
    taps_count = conv_inner.shape[0]
    grad_conv_inner = inner_sums[:taps_count][::-1]
    grad_conv_inner_bias = inner_sums[taps_count]
    grad_skip_gain = jnp.sum(inner_sums[taps_count + 1].reshape(heads_dev, head_size), axis=1)
    grad_decay_log = jnp.sum(grad_log * log_decay, axis=0)
    grad_step_proj = (grad_step_size + grad_log * decay_rate[None, :]) * jax.nn.sigmoid(
        step_proj + step_bias[None, :]
    )
    grad_step_bias = jnp.sum(grad_step_proj, axis=0)
    grad_state_part = jnp.concatenate([grad_bs, grad_cs], axis=1)
    grad_state_act = grad_state_part + swap_pair(grad_state_part)
    grad_state_proj, grad_conv_state, grad_conv_state_bias = state_back(grad_state_act)
    low_state = grad_state_proj.astype(BF16)
    low_step = grad_step_proj.astype(BF16)
    own_state = low_state * (tensor_place == 0).astype(BF16)
    low_pad = jnp.zeros((low_step.shape[0], step_pad), BF16)
    low_first = jnp.concatenate([low_inner, low_state, low_step, low_pad], axis=1)
    grad_first = jnp.einsum("td,tc->dc", normed, low_first, preferred_element_type=F32).astype(BF16)
    grad_first, low_inner, low_gate = lax.optimization_barrier((grad_first, low_inner, low_gate))
    first_part = jnp.concatenate(scatter_rows(column_thirds(grad_first)), axis=1)
    grad_out_proj = out_part.T
    grad_in_gate_inner = jnp.stack([gate_part, first_part[:, :inner_dev]], axis=1)
    grad_in_state = first_part[:, inner_dev:state_end].reshape(in_state.shape)
    grad_in_step = first_part[:, state_end : state_end + heads_dev]
    low_heads = jnp.concatenate([low_inner, own_state, low_step, low_pad], axis=1)
    head_grads = dot_nt(low_gate, gate_weights) + dot_nt(low_heads, first_weights)
    normed_grad_own = scatter_pair(head_grads, tensor_place)
    grad_norm_part = jnp.sum(normed_grad_own * own_rows * row_scale, axis=0)
    scaled_rows = normed_grad_own * norm_gain[None, :]
    row_products = jnp.sum(scaled_rows * own_rows, axis=1, keepdims=True)
    grad_tokens = (
        cot_rows + row_scale * scaled_rows - own_rows * row_scale**3 * row_products / model_width
    )
    small_parts = (
        grad_norm_part + swap_pair(grad_norm_part),
        grad_conv_inner,
        grad_conv_inner_bias,
        grad_conv_state,
        grad_conv_state_bias,
        grad_step_bias,
        grad_decay_log,
        grad_skip_gain,
        grad_gate_gain,
    )
    summed = sum_small(jnp.concatenate([part.reshape(-1) for part in small_parts]))
    small, start = [], 0
    for part in small_parts:
        small.append(summed[start : start + part.size].reshape(part.shape))
        start += part.size
    return (
        block_out,
        grad_tokens,
        small[0],
        grad_in_gate_inner,
        grad_in_state,
        grad_in_step,
        *small[1:],
        grad_out_proj,
    )


def solution(mesh):
    in_specs = (
        P(("dp", "tensor"), None),
        P("dp"),
        P(),
        P("dp", None, "tensor"),
        P("dp", None, None),
        P("dp", "tensor"),
        P(None, "tensor"),
        P("tensor"),
        P(),
        P(),
        P("tensor"),
        P("tensor"),
        P("tensor"),
        P("tensor"),
        P("tensor", "dp"),
        P(("dp", "tensor"), None),
    )
    out_specs = (
        P(("dp", "tensor"), None),
        P(("dp", "tensor"), None),
        P(),
        P("dp", None, "tensor"),
        P("dp", None, None),
        P("dp", "tensor"),
        P(None, "tensor"),
        P("tensor"),
        P(),
        P(),
        P("tensor"),
        P("tensor"),
        P("tensor"),
        P("tensor"),
        P("tensor", "dp"),
    )

    return jax.shard_map(shards, mesh=mesh, in_specs=in_specs, out_specs=out_specs, check_vma=False)
```

```python
import jax
import jax.numpy as jnp
from jax import lax
from jax.experimental import pallas as pl
from jax.experimental.pallas import tpu as pltpu
from jax.sharding import PartitionSpec as P


EPSILON = 1e-05
HIGHEST = lax.Precision.HIGHEST
CHUNK = 128
HEADS_STEP = 8
F32 = jnp.float32
BF16 = jnp.bfloat16


def shift_down(values, steps_back, filler):
    leading = jnp.full((steps_back,) + values.shape[1:], filler, values.dtype)
    return jnp.concatenate([leading, values[: values.shape[0] - steps_back]], axis=0)


def causal_conv(values, conv_taps, conv_bias, segment):
    taps_count = conv_taps.shape[0]
    result = conv_bias[None, :] + conv_taps[taps_count - 1][None, :] * values
    for steps_back in range(1, taps_count):
        earlier = shift_down(values, steps_back, 0.0)
        same_seq = (shift_down(segment, steps_back, -2) == segment).astype(values.dtype)
        result = (
            result + conv_taps[taps_count - 1 - steps_back][None, :] * earlier * same_seq[:, None]
        )
    return result


def dot(a, b):
    return jnp.dot(a, b, preferred_element_type=F32)


def dot_nt(a, b):
    return lax.dot_general(a, b, (((1,), (1,)), ((), ())), preferred_element_type=F32)


def spread_heads(columns, pair, head_size):
    lane = lax.broadcasted_iota(jnp.int32, (columns.shape[0], 2 * head_size), 1)
    first = columns[:, 2 * pair : 2 * pair + 1]
    second = columns[:, 2 * pair + 1 : 2 * pair + 2]
    return jnp.where(lane < head_size, first, second)


def conv_pair(xr, taps, bias, masks, rows, before, lanes):
    current = xr[rows, lanes]
    joined = jnp.concatenate([xr[before, lanes], current], axis=0)
    count = taps.shape[0]
    value = bias[0:1, lanes] + taps[count - 1 : count, lanes] * current
    shifted = []
    for back in range(1, count):
        piece = pltpu.roll(joined, back, 0)[8:] * masks[back - 1, rows, :]
        shifted.append(piece)
        value = value + taps[count - 1 - back : count - back, lanes] * piece
    return current, shifted, value


def ssd_forward_kernel(
    xr, taps, bias, skip, masks, score, cs, bst, dt, cumc, reach, toend, cumr, kept,
    y_out, states_out, state,
):
    width = xr.shape[1]
    head_size = width // HEADS_STEP
    pair_width = 2 * head_size
    chunks = xr.shape[0] // CHUNK
    lane_count = dt.shape[1]
    to_front = lax.rem(lane_count - pl.program_id(0) * HEADS_STEP, lane_count)
    state[...] = jnp.zeros_like(state)

    def chunk_body(place, unused):
        start = pl.multiple_of(place * CHUNK, CHUNK)
        rows = pl.ds(start, CHUNK)
        before = pl.ds(pl.multiple_of(jnp.maximum(start - 8, 0), 8), 8)
        dt_cols, cum_cols, reach_cols, end_cols = (
            pltpu.roll(ref[rows, :], to_front, 1) for ref in (dt, cumc, reach, toend)
        )
        score_now, cs_now, bst_now = score[rows, :], cs[rows, :], bst[:, rows]
        lane = lax.broadcasted_iota(jnp.int32, (CHUNK, pair_width), 1)
        row_of = pl.ds(pl.multiple_of(place * 8, 8), 8)
        for pair in range(width // pair_width):
            lanes = slice(pair * pair_width, (pair + 1) * pair_width)
            _, _, value = conv_pair(
                xr, taps, bias, masks, rows, before, lanes
            )
            x = value * jax.nn.sigmoid(value)
            xdt = x * spread_heads(dt_cols, pair, head_size)
            xb = xdt.astype(BF16)
            held = state[:, lanes]
            held_low = held.astype(BF16)
            states_out[rows, lanes] = held_low
            halves = []
            for head in (2 * pair, 2 * pair + 1):
                spread = cum_cols[:, head : head + 1] - cumr[head : head + 1, rows]
                mixing = score_now * jnp.exp(jnp.minimum(spread, 0.0))
                halves.append(dot(mixing.astype(BF16), xb))
            y = jnp.where(lane < head_size, halves[0], halves[1])
            y = y + spread_heads(reach_cols, pair, head_size) * dot(cs_now, held_low)
            y_out[rows, lanes] = y + skip[0:1, lanes] * x
            fresh = dot(bst_now, (xdt * spread_heads(end_cols, pair, head_size)).astype(BF16))
            state[:, lanes] = fresh + kept[row_of, lanes][0:1] * held
        return unused

    lax.fori_loop(0, chunks, chunk_body, 0)


def ssd_backward_kernel(
    xr, taps, bias, skip, masks, score_t, cs, bs, cst, pick, dt, cumc, reach, toend, cumr, kept,
    states, dy,
    dxr_out, dscore_out, dbs_out, dcs_out, up_out, on_out, step_out, rows_out, span_out, sums_out,
    dstate, dvalue_next,
):
    width = xr.shape[1]
    head_size = width // HEADS_STEP
    pair_width = 2 * head_size
    length = xr.shape[0]
    chunks = length // CHUNK
    count = taps.shape[0]
    lane_count = dt.shape[1]
    first_head = pl.program_id(0) * HEADS_STEP
    to_front = lax.rem(lane_count - first_head, lane_count)
    dstate[...] = jnp.zeros_like(dstate)
    dvalue_next[...] = jnp.zeros_like(dvalue_next)
    sums_out[...] = jnp.zeros_like(sums_out)

    @pl.when(pl.program_id(0) == 0)
    def clear():
        dscore_out[...] = jnp.zeros_like(dscore_out)
        dbs_out[...] = jnp.zeros_like(dbs_out)
        dcs_out[...] = jnp.zeros_like(dcs_out)
        up_out[...] = jnp.zeros_like(up_out)
        on_out[...] = jnp.zeros_like(on_out)
        step_out[...] = jnp.zeros_like(step_out)

    def chunk_body(step, unused):
        place = chunks - 1 - step
        start = pl.multiple_of(place * CHUNK, CHUNK)
        rows = pl.ds(start, CHUNK)
        before = pl.ds(pl.multiple_of(jnp.maximum(start - 8, 0), 8), 8)
        after = pl.ds(pl.multiple_of(jnp.minimum(start + CHUNK, length - 8), 8), 8)
        dt_cols, cum_cols, reach_cols, end_cols = (
            pltpu.roll(ref[rows, :], to_front, 1) for ref in (dt, cumc, reach, toend)
        )
        score_now, cs_now, bs_now, cst_now = score_t[rows, :], cs[rows, :], bs[rows, :], cst[:, rows]
        lane = lax.broadcasted_iota(jnp.int32, (CHUNK, pair_width), 1)
        row_of = pl.ds(pl.multiple_of(place * 8, 8), 8)
        dscore = jnp.zeros((CHUNK, CHUNK), F32)
        dbs = jnp.zeros((CHUNK, bs_now.shape[1]), F32)
        dcs = jnp.zeros((CHUNK, bs_now.shape[1]), F32)
        columns = jnp.zeros((CHUNK, lane_count), F32)
        column_lane = lax.broadcasted_iota(jnp.int32, columns.shape, 1)
        for pair in range(width // pair_width):
            lanes = slice(pair * pair_width, (pair + 1) * pair_width)
            current, shifted, value = conv_pair(xr, taps, bias, masks, rows, before, lanes)
            gate = jax.nn.sigmoid(value)
            x = value * gate
            dt_now = spread_heads(dt_cols, pair, head_size)
            end_now = spread_heads(end_cols, pair, head_size)
            xdt = x * dt_now
            xb = xdt.astype(BF16)
            dy_now = dy[rows, lanes]
            dyb = dy_now.astype(BF16)
            held_low = states[rows, lanes]
            dheld = dstate[:, lanes]
            dheld_low = dheld.astype(BF16)
            dyr = dy_now * spread_heads(reach_cols, pair, head_size)
            dyr_low = dyr.astype(BF16)
            from_state = dyr * dot(cs_now, held_low)
            dcs = dcs + dot_nt(dyr_low, held_low)
            dxdt_end = end_now * dot(bs_now, dheld_low)
            dbs = dbs + dot_nt((xdt * end_now).astype(BF16), dheld_low)
            halves = []
            for side in (0, 1):
                head = 2 * pair + side
                spread = cumr[head : head + 1, rows] - cum_cols[:, head : head + 1]
                decay = jnp.exp(jnp.minimum(spread, 0.0))
                weight = score_now * decay
                own = (lane < head_size) if side == 0 else (lane >= head_size)
                pairs = dot_nt(jnp.where(own, xdt, 0.0).astype(BF16), dyb)
                dscore = dscore + pairs * decay
                share = pairs * weight
                columns = columns - jnp.where(
                    column_lane == head, jnp.sum(share, axis=1, keepdims=True), 0.0
                )
                rows_out[head : head + 1, rows] = jnp.sum(share, axis=0, keepdims=True)
                halves.append(dot(weight.astype(BF16), dyb))
            dxdt = jnp.where(lane < head_size, halves[0], halves[1]) + dxdt_end
            picked = jnp.concatenate(
                [
                    from_state.astype(BF16),
                    (xdt * dxdt_end).astype(BF16),
                    (x * dxdt).astype(BF16),
                ],
                axis=1,
            )
            columns = columns + dot(picked, pick[pair])
            dx = skip[0:1, lanes] * dy_now + dt_now * dxdt
            kept_row = kept[row_of, lanes][0:1]
            span_row = kept_row * jnp.sum(dheld * held_low.astype(F32), axis=0, keepdims=True)
            span_out[row_of, lanes] = jnp.broadcast_to(span_row, (8, pair_width))
            dstate[:, lanes] = kept_row * dheld + dot(cst_now, dyr_low)
            dvalue = dx * (gate * (1.0 + value * (1.0 - gate)))
            dxr = taps[count - 1 : count, lanes] * dvalue
            next_rows = dvalue_next[:, lanes]
            sums = [jnp.sum(dvalue * current, axis=0, keepdims=True)]
            for back in range(1, count):
                masked = dvalue * masks[back - 1, rows, :]
                joined = jnp.concatenate(
                    [masked, next_rows * masks[back - 1, after, :]], axis=0
                )
                lifted = pltpu.roll(joined, CHUNK + 8 - back, 0)[:CHUNK]
                dxr = dxr + taps[count - 1 - back : count - back, lanes] * lifted
                sums.append(jnp.sum(dvalue * shifted[back - 1], axis=0, keepdims=True))
            dvalue_next[:, lanes] = dvalue[:8]
            sums.append(jnp.sum(dvalue, axis=0, keepdims=True))
            sums.append(jnp.sum(dy_now * x, axis=0, keepdims=True))
            for slot, row in enumerate(sums):
                sums_out[slot : slot + 1, lanes] += row
            dxr_out[rows, lanes] = dxr.astype(dxr_out.dtype)
        dscore_out[rows, :] += dscore
        dbs_out[rows, :] += dbs
        dcs_out[rows, :] += dcs
        held_lane = (column_lane >= first_head) & (column_lane < first_head + HEADS_STEP)
        for slot, out in enumerate((up_out, on_out, step_out)):
            turn = lax.rem(first_head + lane_count - slot * HEADS_STEP, lane_count)
            out[rows, :] += jnp.where(held_lane, pltpu.roll(columns, turn, 1), 0.0)
        return unused

    lax.fori_loop(0, chunks, chunk_body, 0)


def chunk_terms(step_size, log_decay, segment, real_heads, head_size):
    length, heads = step_size.shape
    chunks = length // CHUNK
    parted = segment.reshape(chunks, CHUNK)
    places = jnp.arange(CHUNK)
    lower = (places[:, None] >= places[None, :]).astype(F32)
    allowed = (
        (parted[:, :, None] == parted[:, None, :]) & (places[:, None] >= places[None, :])[None]
    ).astype(F32)
    cumulative = jnp.einsum(
        "ts,csh->cth", lower, log_decay.reshape(chunks, CHUNK, heads), precision=HIGHEST
    )
    last = jnp.concatenate([jnp.full((1,), -2, segment.dtype), parted[:-1, CHUNK - 1]])
    carried = (parted == last[:, None]).astype(F32)
    final = parted[:, CHUNK - 1]
    at_end = (parted == final[:, None]).astype(F32)
    total = cumulative[:, CHUNK - 1]
    reach = jnp.exp(cumulative) * carried[:, :, None]
    to_end = jnp.exp(total[:, None, :] - cumulative) * at_end[:, :, None]
    kept = jnp.exp(total) * (final == last).astype(F32)[:, None]

    columns = (step_size, *(a.reshape(length, heads) for a in (cumulative, reach, to_end)))
    cum_rows = columns[1].T
    kept_rows = jnp.repeat(jnp.repeat(kept[:, :real_heads], head_size, axis=1), 8, axis=0)
    masks = jnp.stack(
        [
            jnp.broadcast_to(
                (shift_down(segment, back, -2) == segment).astype(F32)[:, None],
                (length, 2 * head_size),
            )
            for back in (1, 2, 3)
        ]
    )
    return allowed, columns, cum_rows, kept_rows, masks


def whole_spec(array):
    zeros = (0,) * array.ndim
    return pl.BlockSpec(array.shape, lambda g: zeros)


def lanes_spec(array, width):
    return pl.BlockSpec((array.shape[0], width), lambda g: (0, g))


def ssd_forward(xr, taps, bias, skip_row, terms, bs_low, cs_low, head_size):
    allowed, columns, cum_rows, kept_rows, masks = terms
    length, inner = xr.shape[0], taps.shape[1]
    width = HEADS_STEP * head_size
    groups = inner // width
    state_dim = bs_low.shape[1]
    chunks = length // CHUNK
    score = (
        jnp.einsum(
            "ctn,csn->cts",
            cs_low.reshape(chunks, CHUNK, state_dim),
            bs_low.reshape(chunks, CHUNK, state_dim),
            preferred_element_type=F32,
        )
        * allowed
    )
    shared = (masks, score.reshape(length, CHUNK), cs_low, bs_low.T, *columns)
    rows_spec = pl.BlockSpec((HEADS_STEP, length), lambda g: (g, 0))
    y, states = pl.pallas_call(
        ssd_forward_kernel,
        grid=(groups,),
        in_specs=[lanes_spec(a, width) for a in (xr, taps, bias, skip_row)]
        + [whole_spec(a) for a in shared]
        + [rows_spec, lanes_spec(kept_rows, width)],
        out_specs=[
            pl.BlockSpec((length, width), lambda g: (0, g)),
            pl.BlockSpec((chunks * state_dim, width), lambda g: (0, g)),
        ],
        out_shape=[
            jax.ShapeDtypeStruct((length, inner), F32),
            jax.ShapeDtypeStruct((chunks * state_dim, inner), BF16),
        ],
        scratch_shapes=[pltpu.VMEM((state_dim, width), F32)],
        cost_estimate=pl.CostEstimate(
            flops=130 * length * inner * CHUNK, bytes_accessed=12 * length * inner, transcendentals=0
        ),
        name="ssd_forward",
    )(xr, taps, bias, skip_row, *shared, cum_rows, kept_rows)
    return y, states, score


def ssd_backward(
    xr, taps, bias, skip_row, terms, score, bs_low, cs_low, states, dy, head_size
):
    allowed, columns, cum_rows, kept_rows, masks = terms
    length, inner = xr.shape[0], taps.shape[1]
    heads_step, heads = HEADS_STEP, columns[0].shape[1]
    width = heads_step * head_size
    groups = inner // width
    state_dim = bs_low.shape[1]
    chunks = length // CHUNK
    lane = jnp.arange(2 * head_size) // head_size
    pick = jnp.stack(
        [
            jnp.concatenate(
                [
                    (
                        (2 * pair + lane + slot * heads_step)[:, None] == jnp.arange(CHUNK)[None, :]
                    ).astype(BF16)
                    for slot in range(3)
                ]
            )
            for pair in range(heads_step // 2)
        ]
    )
    score_t = score.transpose(0, 2, 1).reshape(length, CHUNK)
    shared = (masks, score_t, cs_low, bs_low, cs_low.T, pick, *columns)
    rows_spec = pl.BlockSpec((heads_step, length), lambda g: (g, 0))
    fixed = pl.BlockSpec((length, CHUNK), lambda g: (0, 0))
    out = pl.pallas_call(
        ssd_backward_kernel,
        grid=(groups,),
        in_specs=[lanes_spec(a, width) for a in (xr, taps, bias, skip_row)]
        + [whole_spec(a) for a in shared]
        + [rows_spec, lanes_spec(kept_rows, width)]
        + [lanes_spec(a, width) for a in (states, dy)],
        out_specs=[
            pl.BlockSpec((length, width), lambda g: (0, g)),
            fixed,
            pl.BlockSpec((length, state_dim), lambda g: (0, 0)),
            pl.BlockSpec((length, state_dim), lambda g: (0, 0)),
            *[pl.BlockSpec((length, heads), lambda g: (0, 0))] * 3,
            rows_spec,
            pl.BlockSpec((8 * chunks, width), lambda g: (0, g)),
            pl.BlockSpec((8, width), lambda g: (0, g)),
        ],
        out_shape=[
            jax.ShapeDtypeStruct((length, inner), BF16),
            jax.ShapeDtypeStruct((length, CHUNK), F32),
            jax.ShapeDtypeStruct((length, state_dim), F32),
            jax.ShapeDtypeStruct((length, state_dim), F32),
            *[jax.ShapeDtypeStruct((length, heads), F32)] * 3,
            jax.ShapeDtypeStruct((groups * heads_step, length), F32),
            jax.ShapeDtypeStruct((8 * chunks, inner), F32),
            jax.ShapeDtypeStruct((8, inner), F32),
        ],
        scratch_shapes=[pltpu.VMEM((state_dim, width), F32), pltpu.VMEM((8, width), F32)],
        cost_estimate=pl.CostEstimate(
            flops=290 * length * inner * CHUNK, bytes_accessed=16 * length * inner, transcendentals=0
        ),
        name="ssd_backward",
    )(xr, taps, bias, skip_row, *shared, cum_rows, kept_rows, states, dy)
    dxr, dscore_t, dbs, dcs, upward, onward, dstep, rows, span, sums = out
    dscore_t = (dscore_t.reshape(chunks, CHUNK, CHUNK) * allowed.transpose(0, 2, 1)).astype(BF16)
    parted_c = cs_low.reshape(chunks, CHUNK, state_dim)
    parted_b = bs_low.reshape(chunks, CHUNK, state_dim)
    from_score_b = jnp.einsum("cst,ctn->csn", dscore_t, parted_c, preferred_element_type=F32)
    from_score_c = jnp.einsum("cst,csn->ctn", dscore_t, parted_b, preferred_element_type=F32)
    dbs = dbs + from_score_b.reshape(length, state_dim)
    dcs = dcs + from_score_c.reshape(length, state_dim)
    real_heads = groups * heads_step
    spare = heads - real_heads
    upward = upward + jnp.pad(rows.T, ((0, 0), (0, spare)))
    spans = jnp.sum(span[::8].reshape(chunks, real_heads, head_size), axis=2)
    spans = jnp.pad(spans, ((0, 0), (0, spare))).reshape(chunks, 1, heads)
    places = jnp.arange(CHUNK)
    at_or_after = (places[None, :] >= places[:, None]).astype(F32)
    ahead = (places[None, :] < places[:, None]).astype(F32)
    dlog = jnp.einsum(
        "rt,cth->crh", at_or_after, upward.reshape(chunks, CHUNK, heads), precision=HIGHEST
    )
    dlog = dlog + jnp.einsum(
        "rs,csh->crh", ahead, onward.reshape(chunks, CHUNK, heads), precision=HIGHEST
    )
    dlog = (dlog + spans).reshape(length, heads)
    return dxr, dbs, dcs, dstep, dlog, sums


def swap_pair(values):
    return lax.ppermute(values, "tensor", [(0, 1), (1, 0)])


def gather_pair(own, place):
    other = swap_pair(own)
    lower = jnp.where(place == 0, own, other)
    upper = jnp.where(place == 0, other, own)
    return jnp.concatenate([lower, upper], axis=0)


def scatter_pair(values, place):
    half = values.shape[0] // 2
    sent = lax.dynamic_slice_in_dim(values, (1 - place) * half, half)
    kept = lax.dynamic_slice_in_dim(values, place * half, half)
    return kept + swap_pair(sent)


def stage_orders(size):
    bits = size.bit_length() - 1
    if bits == 4:
        return ((0, 1, 2, 3), (1, 2, 3, 0), (2, 0, 1, 3))
    return tuple(tuple((bit + turn) % bits for bit in range(bits)) for turn in range(3))


def partner(values, bit):
    size = lax.axis_size("dp")
    return lax.ppermute(values, "dp", [(i, i ^ (1 << bit)) for i in range(size)])


def place_kernel(table, *refs):
    sources, (out, buffer, arrived, left) = refs[:-4], refs[-4:]
    turns, size = len(sources) // 2, out.shape[0]
    half = size // 2
    width = sources[0].shape[2]

    def arrival(turn, source, block, target):
        lanes = pl.ds(turn * width, width)
        return pltpu.make_async_copy(
            source.at[block], buffer.at[target, :, lanes], arrived.at[turn, target]
        )

    def start_in(target, unused):
        for turn in range(turns):
            block = table[turn, target]

            @pl.when(block < half)
            def from_own():
                arrival(turn, sources[2 * turn], block, target).start()

            @pl.when(block >= half)
            def from_other():
                arrival(turn, sources[2 * turn + 1], block - half, target).start()

        return unused

    def start_out(target, unused):
        for turn in range(turns):
            arrival(turn, sources[2 * turn], 0, target).wait()
        pltpu.make_async_copy(buffer.at[target], out.at[target], left.at[target]).start()
        return unused

    def finish(target, unused):
        pltpu.make_async_copy(buffer.at[target], out.at[target], left.at[target]).wait()
        return unused

    lax.fori_loop(0, size, start_in, 0)
    lax.fori_loop(0, size, start_out, 0)
    lax.fori_loop(0, size, finish, 0)


def gather_stages(pieces, first_stage, last_stage):
    orders = stage_orders(lax.axis_size("dp"))
    for stage in range(first_stage, last_stage):
        joined = []
        for piece, order in zip(pieces, orders):
            other = partner(piece, order[::-1][stage])
            if stage == len(order) - 1:
                joined.append((piece, other))
            else:
                joined.append(jnp.concatenate([piece, other], axis=0))
        pieces = joined
    return pieces


def split_shard(shard):
    turns = len(stage_orders(lax.axis_size("dp")))
    width = shard.shape[1] // turns
    return [shard[None, :, turn * width : (turn + 1) * width] for turn in range(turns)]


def place_rows(pieces):
    size, index = lax.axis_size("dp"), lax.axis_index("dp")
    orders = stage_orders(size)
    targets = jnp.arange(size, dtype=jnp.int32) ^ index.astype(jnp.int32)
    tables = [
        sum(((targets >> bit) & 1) << stage for stage, bit in enumerate(order[::-1]))
        for order in orders
    ]
    _, rows, width = pieces[0][0].shape
    sources = [part for pair in pieces for part in pair]
    shape = (size, rows, width * len(orders))
    placed = pl.pallas_call(
        place_kernel,
        in_specs=[pl.BlockSpec(memory_space=pltpu.SMEM)]
        + [pl.BlockSpec(memory_space=pl.ANY)] * len(sources),
        out_specs=pl.BlockSpec(memory_space=pl.ANY),
        out_shape=jax.ShapeDtypeStruct(shape, BF16),
        scratch_shapes=[
            pltpu.VMEM(shape, BF16),
            pltpu.SemaphoreType.DMA((len(orders), size)),
            pltpu.SemaphoreType.DMA((size,)),
        ],
        cost_estimate=pl.CostEstimate(
            flops=0, bytes_accessed=4 * size * rows * shape[2], transcendentals=0
        ),
        name="place_rows",
    )(jnp.stack(tables), *sources)
    return placed.reshape(size * rows, shape[2])


def scatter_rows(pieces):
    size, index = lax.axis_size("dp"), lax.axis_index("dp")
    bits = size.bit_length() - 1
    orders = stage_orders(size)
    held, left = [], []
    for piece in pieces:
        held.append(piece.reshape((2,) * bits + (piece.shape[0] // size, piece.shape[1])))
        left.append(list(range(bits - 1, -1, -1)))
    for stage in range(bits):
        for turn, order in enumerate(orders[: len(pieces)]):
            bit = order[stage]
            axis = left[turn].index(bit)
            mine = (index >> bit) & 1
            sent = lax.dynamic_index_in_dim(held[turn], 1 - mine, axis, keepdims=False)
            kept = lax.dynamic_index_in_dim(held[turn], mine, axis, keepdims=False)
            got = partner(sent.astype(BF16), bit)
            held[turn] = kept.astype(F32) + got.astype(F32)
            left[turn].pop(axis)
    return held


def sum_small(values):
    for bit in range(lax.axis_size("dp").bit_length() - 1):
        values = values + partner(values, bit)
    return values


def shards(
    tokens,
    segment_ids,
    norm_gain,
    in_gate_inner,
    in_state,
    in_step,
    conv_inner,
    conv_inner_bias,
    conv_state,
    conv_state_bias,
    step_bias,
    decay_log,
    skip_gain,
    gate_gain,
    out_proj,
    cotangent,
):
    half_rows = tokens.shape[0]
    model_width = tokens.shape[1]
    tensor_place = lax.axis_index("tensor")
    own_segment = lax.dynamic_slice_in_dim(segment_ids, tensor_place * half_rows, half_rows)
    own_live = (own_segment >= 0).astype(F32)[:, None]
    own_rows = tokens.astype(F32)
    row_scale = lax.rsqrt(jnp.mean(own_rows * own_rows, axis=1, keepdims=True) + EPSILON)
    normed_own = (own_rows * row_scale * norm_gain[None, :]).astype(BF16)
    width, _, inner_dev = in_gate_inner.shape
    state_dim = in_state.shape[2]
    heads_dev = in_step.shape[1]
    head_size = inner_dev // heads_dev
    step_pad = -heads_dev % 128
    first_shard = jnp.concatenate(
        [
            in_gate_inner[:, 1],
            in_state.reshape(width, -1),
            in_step,
            jnp.zeros((width, step_pad), BF16),
        ],
        axis=1,
    )
    bits = lax.axis_size("dp").bit_length() - 1
    first_pieces = gather_stages(split_shard(first_shard), 0, bits - 1)
    later_shard = jnp.concatenate([in_gate_inner[:, 0], out_proj.T], axis=1)
    first_pieces, later_pieces = lax.optimization_barrier((first_pieces, split_shard(later_shard)))
    first_pieces = gather_stages(first_pieces, bits - 1, bits)
    later_pieces = gather_stages(later_pieces, 0, bits)
    first_weights = place_rows(first_pieces)
    normed = gather_pair(normed_own, tensor_place)
    first_proj = dot(normed, first_weights)
    state_end = inner_dev + 2 * state_dim
    inner_proj = first_proj
    state_proj = first_proj[:, inner_dev:state_end]
    step_proj = first_proj[:, state_end:]
    step_bias_row = jnp.pad(step_bias, (0, step_pad))[None]

    def state_piece(state_values, conv_taps, conv_bias):
        return jax.nn.silu(
            causal_conv(
                state_values,
                conv_taps.reshape(conv_taps.shape[0], -1),
                conv_bias.reshape(-1),
                segment_ids,
            )
        )

    state_act, state_back = jax.vjp(state_piece, state_proj, conv_state, conv_state_bias)
    bs_low = state_act[:, :state_dim].astype(BF16)
    cs_low = state_act[:, state_dim:].astype(BF16)
    step_size = jax.nn.softplus(step_proj + step_bias_row)
    decay_rate = -jnp.exp(jnp.pad(decay_log, (0, step_pad)))
    log_decay = step_size * decay_rate[None, :]
    terms = chunk_terms(step_size, log_decay, segment_ids, heads_dev, head_size)
    skip_row = jnp.repeat(skip_gain, head_size)[None]
    bias_row = conv_inner_bias[None]
    mixed, states, score = ssd_forward(
        inner_proj, conv_inner, bias_row, skip_row, terms, bs_low, cs_low, head_size
    )
    later_weights = place_rows(later_pieces)
    gate_weights = later_weights[:, :inner_dev]
    out_weights_t = later_weights[:, inner_dev:]
    gate_proj = dot(normed, gate_weights)
    gate_sigmoid = jax.nn.sigmoid(gate_proj)
    gated_values = mixed * (gate_proj * gate_sigmoid)
    full_inner = inner_dev * lax.axis_size("tensor")
    squares = lax.psum(jnp.sum(gated_values * gated_values, axis=1), "tensor")
    gate_scale = lax.rsqrt(squares / full_inner + EPSILON)[:, None]
    normed_inner = (gated_values * gate_scale * gate_gain[None, :]).astype(BF16)
    partial_out = jnp.einsum(
        "tc,dc->td", normed_inner, out_weights_t, preferred_element_type=F32
    )
    branch_own = scatter_pair(partial_out, tensor_place)
    block_out = (own_rows + own_live * branch_own).astype(BF16)
    cot_rows = cotangent.astype(F32)
    branch_grad_own = (own_live * cot_rows).astype(BF16)
    branch_grad = gather_pair(branch_grad_own, tensor_place)
    grad_out_proj_t = jnp.einsum(
        "td,tc->dc", branch_grad, normed_inner, preferred_element_type=F32
    )
    grad_normed_inner = jnp.einsum(
        "td,dc->tc", branch_grad, out_weights_t, preferred_element_type=F32
    )
    grad_gate_gain = jnp.sum(grad_normed_inner * gated_values * gate_scale, axis=0)
    scaled_grad = grad_normed_inner * gate_gain[None, :]
    products = lax.psum(jnp.sum(scaled_grad * gated_values, axis=1), "tensor")
    grad_gated = (
        gate_scale * scaled_grad - gated_values * gate_scale**3 * (products / full_inner)[:, None]
    )
    low_gate = (
        grad_gated * mixed * (gate_sigmoid * (1.0 + gate_proj * (1.0 - gate_sigmoid)))
    ).astype(BF16)
    grad_mixed = grad_gated * (gate_proj * gate_sigmoid)
    grad_gate_half = jnp.einsum(
        "td,tc->dc", normed, low_gate, preferred_element_type=F32
    ).astype(BF16)
    grad_out_low = grad_out_proj_t.astype(BF16)
    grad_mixed, grad_gate_half, grad_out_low = lax.optimization_barrier(
        (grad_mixed, grad_gate_half, grad_out_low)
    )
    cut = 2 * inner_dev // 3
    early_parts = scatter_rows(
        [
            grad_gate_half[:, :cut],
            jnp.concatenate([grad_gate_half[:, cut:], grad_out_low[:, : 2 * cut - inner_dev]], axis=1),
            grad_out_low[:, 2 * cut - inner_dev :],
        ],
    )
    early_part = jnp.concatenate(early_parts, axis=1)
    gate_part, out_part = early_part[:, :inner_dev], early_part[:, inner_dev:]
    scan_back = ssd_backward(
        inner_proj,
        conv_inner,
        bias_row,
        skip_row,
        terms,
        score,
        bs_low,
        cs_low,
        states,
        grad_mixed,
        head_size,
    )
    low_inner, grad_bs, grad_cs, grad_step_size, grad_log, inner_sums = scan_back
    taps_count = conv_inner.shape[0]
    grad_conv_inner = inner_sums[:taps_count][::-1]
    grad_conv_inner_bias = inner_sums[taps_count]
    grad_skip_gain = jnp.sum(inner_sums[taps_count + 1].reshape(heads_dev, head_size), axis=1)
    grad_decay_log = jnp.sum(grad_log * log_decay, axis=0)[:heads_dev]
    grad_step_proj = (grad_step_size + grad_log * decay_rate[None, :]) * jax.nn.sigmoid(
        step_proj + step_bias_row
    )
    grad_step_bias = jnp.sum(grad_step_proj, axis=0)[:heads_dev]
    grad_inner = jnp.einsum("td,tc->dc", normed, low_inner, preferred_element_type=F32).astype(BF16)
    grad_state_part = jnp.concatenate([grad_bs, grad_cs], axis=1)
    grad_state_act = grad_state_part + swap_pair(grad_state_part)
    grad_state_proj, grad_conv_state, grad_conv_state_bias = state_back(grad_state_act)
    low_state = grad_state_proj.astype(BF16)
    low_step = grad_step_proj.astype(BF16)
    own_state = low_state * (tensor_place == 0).astype(BF16)
    low_rest = jnp.concatenate([low_state, low_step], axis=1)
    low_rest_own = jnp.concatenate([own_state, low_step], axis=1)
    grad_rest = jnp.einsum("td,tc->dc", normed, low_rest, preferred_element_type=F32).astype(BF16)
    third = inner_dev // 3
    late_parts = scatter_rows(
        [grad_inner[:, turn * third : (turn + 1) * third] for turn in range(3)]
    )
    first_part = jnp.concatenate(late_parts + scatter_rows([grad_rest]), axis=1)
    grad_out_proj = out_part.T
    grad_in_gate_inner = jnp.stack([gate_part, first_part[:, :inner_dev]], axis=1)
    grad_in_state = first_part[:, inner_dev:state_end].reshape(in_state.shape)
    grad_in_step = first_part[:, state_end : state_end + heads_dev]
    head_grads = (
        dot_nt(low_gate, gate_weights)
        + dot_nt(low_inner, first_weights[:, :inner_dev])
        + dot_nt(low_rest_own, first_weights[:, inner_dev:])
    )
    normed_grad_own = scatter_pair(head_grads, tensor_place)
    grad_norm_part = jnp.sum(normed_grad_own * own_rows * row_scale, axis=0)
    scaled_rows = normed_grad_own * norm_gain[None, :]
    row_products = jnp.sum(scaled_rows * own_rows, axis=1, keepdims=True)
    grad_tokens = (
        cot_rows + row_scale * scaled_rows - own_rows * row_scale**3 * row_products / model_width
    )
    small_parts = (
        grad_norm_part + swap_pair(grad_norm_part),
        grad_conv_inner,
        grad_conv_inner_bias,
        grad_conv_state,
        grad_conv_state_bias,
        grad_step_bias,
        grad_decay_log,
        grad_skip_gain,
        grad_gate_gain,
    )
    summed = sum_small(jnp.concatenate([part.reshape(-1) for part in small_parts]))
    small, start = [], 0
    for part in small_parts:
        small.append(summed[start : start + part.size].reshape(part.shape))
        start += part.size
    return (
        block_out,
        grad_tokens,
        small[0],
        grad_in_gate_inner,
        grad_in_state,
        grad_in_step,
        *small[1:],
        grad_out_proj,
    )


def solution(mesh):
    in_specs = (
        P(("dp", "tensor"), None),
        P("dp"),
        P(),
        P("dp", None, "tensor"),
        P("dp", None, None),
        P("dp", "tensor"),
        P(None, "tensor"),
        P("tensor"),
        P(),
        P(),
        P("tensor"),
        P("tensor"),
        P("tensor"),
        P("tensor"),
        P("tensor", "dp"),
        P(("dp", "tensor"), None),
    )
    out_specs = (
        P(("dp", "tensor"), None),
        P(("dp", "tensor"), None),
        P(),
        P("dp", None, "tensor"),
        P("dp", None, None),
        P("dp", "tensor"),
        P(None, "tensor"),
        P("tensor"),
        P(),
        P(),
        P("tensor"),
        P("tensor"),
        P("tensor"),
        P("tensor"),
        P("tensor", "dp"),
    )

    return jax.shard_map(shards, mesh=mesh, in_specs=in_specs, out_specs=out_specs, check_vma=False)
```

```python
import jax
import jax.numpy as jnp
from jax import lax
from jax.experimental import pallas as pl
from jax.experimental.pallas import tpu as pltpu
from jax.sharding import PartitionSpec as P


EPSILON = 1e-05
HIGHEST = lax.Precision.HIGHEST
CHUNK = 128
HEADS_STEP = 8
F32 = jnp.float32
BF16 = jnp.bfloat16


def shift_down(values, steps_back, filler):
    leading = jnp.full((steps_back,) + values.shape[1:], filler, values.dtype)
    return jnp.concatenate([leading, values[: values.shape[0] - steps_back]], axis=0)


def causal_conv(values, conv_taps, conv_bias, segment):
    taps_count = conv_taps.shape[0]
    result = conv_bias[None, :] + conv_taps[taps_count - 1][None, :] * values
    for steps_back in range(1, taps_count):
        earlier = shift_down(values, steps_back, 0.0)
        same_seq = (shift_down(segment, steps_back, -2) == segment).astype(values.dtype)
        result = (
            result + conv_taps[taps_count - 1 - steps_back][None, :] * earlier * same_seq[:, None]
        )
    return result


def dot(a, b):
    return jnp.dot(a, b, preferred_element_type=F32)


def dot_nt(a, b):
    return lax.dot_general(a, b, (((1,), (1,)), ((), ())), preferred_element_type=F32)


def spread_heads(columns, pair, head_size):
    lane = lax.broadcasted_iota(jnp.int32, (columns.shape[0], 2 * head_size), 1)
    first = columns[:, 2 * pair : 2 * pair + 1]
    second = columns[:, 2 * pair + 1 : 2 * pair + 2]
    return jnp.where(lane < head_size, first, second)


def conv_pair(xr, taps, bias, masks, rows, before, lanes):
    current = xr[rows, lanes]
    joined = jnp.concatenate([xr[before, lanes], current], axis=0)
    count = taps.shape[0]
    value = bias[0:1, lanes] + taps[count - 1 : count, lanes] * current
    shifted = []
    for back in range(1, count):
        piece = pltpu.roll(joined, back, 0)[8:] * masks[back - 1, rows, :]
        shifted.append(piece)
        value = value + taps[count - 1 - back : count - back, lanes] * piece
    return current, shifted, value


def ssd_forward_kernel(
    xr, taps, bias, skip, masks, score, cs, bst, dt, cumc, reach, toend, cumr, kept,
    y_out, states_out, state,
):
    width = xr.shape[1]
    head_size = width // HEADS_STEP
    pair_width = 2 * head_size
    chunks = xr.shape[0] // CHUNK
    lane_count = dt.shape[1]
    to_front = lax.rem(lane_count - pl.program_id(0) * HEADS_STEP, lane_count)
    state[...] = jnp.zeros_like(state)

    def chunk_body(place, unused):
        start = pl.multiple_of(place * CHUNK, CHUNK)
        rows = pl.ds(start, CHUNK)
        before = pl.ds(pl.multiple_of(jnp.maximum(start - 8, 0), 8), 8)
        dt_cols, cum_cols, reach_cols, end_cols = (
            pltpu.roll(ref[rows, :], to_front, 1) for ref in (dt, cumc, reach, toend)
        )
        score_now, cs_now, bst_now = score[rows, :], cs[rows, :], bst[:, rows]
        lane = lax.broadcasted_iota(jnp.int32, (CHUNK, pair_width), 1)
        row_of = pl.ds(pl.multiple_of(place * 8, 8), 8)
        for pair in range(width // pair_width):
            lanes = slice(pair * pair_width, (pair + 1) * pair_width)
            _, _, value = conv_pair(
                xr, taps, bias, masks, rows, before, lanes
            )
            x = value * jax.nn.sigmoid(value)
            xdt = x * spread_heads(dt_cols, pair, head_size)
            xb = xdt.astype(BF16)
            held = state[:, lanes]
            held_low = held.astype(BF16)
            states_out[rows, lanes] = held_low
            halves = []
            for head in (2 * pair, 2 * pair + 1):
                spread = cum_cols[:, head : head + 1] - cumr[head : head + 1, rows]
                mixing = score_now * jnp.exp(jnp.minimum(spread, 0.0))
                halves.append(dot(mixing.astype(BF16), xb))
            y = jnp.where(lane < head_size, halves[0], halves[1])
            y = y + spread_heads(reach_cols, pair, head_size) * dot(cs_now, held_low)
            y_out[rows, lanes] = y + skip[0:1, lanes] * x
            fresh = dot(bst_now, (xdt * spread_heads(end_cols, pair, head_size)).astype(BF16))
            state[:, lanes] = fresh + kept[row_of, lanes][0:1] * held
        return unused

    lax.fori_loop(0, chunks, chunk_body, 0)


def ssd_backward_kernel(
    xr, taps, bias, skip, masks, score_t, cs, bs, cst, pick, dt, cumc, reach, toend, cumr, kept,
    states, dy,
    dxr_out, dscore_out, dbs_out, dcs_out, up_out, on_out, step_out, rows_out, span_out, sums_out,
    dstate, dvalue_next,
):
    width = xr.shape[1]
    head_size = width // HEADS_STEP
    pair_width = 2 * head_size
    length = xr.shape[0]
    chunks = length // CHUNK
    count = taps.shape[0]
    lane_count = dt.shape[1]
    first_head = pl.program_id(0) * HEADS_STEP
    to_front = lax.rem(lane_count - first_head, lane_count)
    dstate[...] = jnp.zeros_like(dstate)
    dvalue_next[...] = jnp.zeros_like(dvalue_next)
    sums_out[...] = jnp.zeros_like(sums_out)

    @pl.when(pl.program_id(0) == 0)
    def clear():
        dscore_out[...] = jnp.zeros_like(dscore_out)
        dbs_out[...] = jnp.zeros_like(dbs_out)
        dcs_out[...] = jnp.zeros_like(dcs_out)
        up_out[...] = jnp.zeros_like(up_out)
        on_out[...] = jnp.zeros_like(on_out)
        step_out[...] = jnp.zeros_like(step_out)

    def chunk_body(step, unused):
        place = chunks - 1 - step
        start = pl.multiple_of(place * CHUNK, CHUNK)
        rows = pl.ds(start, CHUNK)
        before = pl.ds(pl.multiple_of(jnp.maximum(start - 8, 0), 8), 8)
        after = pl.ds(pl.multiple_of(jnp.minimum(start + CHUNK, length - 8), 8), 8)
        dt_cols, cum_cols, reach_cols, end_cols = (
            pltpu.roll(ref[rows, :], to_front, 1) for ref in (dt, cumc, reach, toend)
        )
        score_now, cs_now, bs_now, cst_now = score_t[rows, :], cs[rows, :], bs[rows, :], cst[:, rows]
        lane = lax.broadcasted_iota(jnp.int32, (CHUNK, pair_width), 1)
        row_of = pl.ds(pl.multiple_of(place * 8, 8), 8)
        dscore = jnp.zeros((CHUNK, CHUNK), F32)
        dbs = jnp.zeros((CHUNK, bs_now.shape[1]), F32)
        dcs = jnp.zeros((CHUNK, bs_now.shape[1]), F32)
        columns = jnp.zeros((CHUNK, lane_count), F32)
        column_lane = lax.broadcasted_iota(jnp.int32, columns.shape, 1)
        for pair in range(width // pair_width):
            lanes = slice(pair * pair_width, (pair + 1) * pair_width)
            current, shifted, value = conv_pair(xr, taps, bias, masks, rows, before, lanes)
            gate = jax.nn.sigmoid(value)
            x = value * gate
            dt_now = spread_heads(dt_cols, pair, head_size)
            end_now = spread_heads(end_cols, pair, head_size)
            xdt = x * dt_now
            xb = xdt.astype(BF16)
            dy_now = dy[rows, lanes]
            dyb = dy_now.astype(BF16)
            held_low = states[rows, lanes]
            dheld = dstate[:, lanes]
            dheld_low = dheld.astype(BF16)
            dyr = dy_now * spread_heads(reach_cols, pair, head_size)
            dyr_low = dyr.astype(BF16)
            from_state = dyr * dot(cs_now, held_low)
            dcs = dcs + dot_nt(dyr_low, held_low)
            dxdt_end = end_now * dot(bs_now, dheld_low)
            dbs = dbs + dot_nt((xdt * end_now).astype(BF16), dheld_low)
            halves = []
            for side in (0, 1):
                head = 2 * pair + side
                spread = cumr[head : head + 1, rows] - cum_cols[:, head : head + 1]
                decay = jnp.exp(jnp.minimum(spread, 0.0))
                weight = score_now * decay
                own = (lane < head_size) if side == 0 else (lane >= head_size)
                pairs = dot_nt(jnp.where(own, xdt, 0.0).astype(BF16), dyb)
                dscore = dscore + pairs * decay
                share = pairs * weight
                columns = columns - jnp.where(
                    column_lane == head, jnp.sum(share, axis=1, keepdims=True), 0.0
                )
                rows_out[head : head + 1, rows] = jnp.sum(share, axis=0, keepdims=True)
                halves.append(dot(weight.astype(BF16), dyb))
            dxdt = jnp.where(lane < head_size, halves[0], halves[1]) + dxdt_end
            picked = jnp.concatenate(
                [
                    from_state.astype(BF16),
                    (xdt * dxdt_end).astype(BF16),
                    (x * dxdt).astype(BF16),
                ],
                axis=1,
            )
            columns = columns + dot(picked, pick[pair])
            dx = skip[0:1, lanes] * dy_now + dt_now * dxdt
            kept_row = kept[row_of, lanes][0:1]
            span_row = kept_row * jnp.sum(dheld * held_low.astype(F32), axis=0, keepdims=True)
            span_out[row_of, lanes] = jnp.broadcast_to(span_row, (8, pair_width))
            dstate[:, lanes] = kept_row * dheld + dot(cst_now, dyr_low)
            dvalue = dx * (gate * (1.0 + value * (1.0 - gate)))
            dxr = taps[count - 1 : count, lanes] * dvalue
            next_rows = dvalue_next[:, lanes]
            sums = [jnp.sum(dvalue * current, axis=0, keepdims=True)]
            for back in range(1, count):
                masked = dvalue * masks[back - 1, rows, :]
                joined = jnp.concatenate(
                    [masked, next_rows * masks[back - 1, after, :]], axis=0
                )
                lifted = pltpu.roll(joined, CHUNK + 8 - back, 0)[:CHUNK]
                dxr = dxr + taps[count - 1 - back : count - back, lanes] * lifted
                sums.append(jnp.sum(dvalue * shifted[back - 1], axis=0, keepdims=True))
            dvalue_next[:, lanes] = dvalue[:8]
            sums.append(jnp.sum(dvalue, axis=0, keepdims=True))
            sums.append(jnp.sum(dy_now * x, axis=0, keepdims=True))
            for slot, row in enumerate(sums):
                sums_out[slot : slot + 1, lanes] += row
            dxr_out[rows, lanes] = dxr.astype(dxr_out.dtype)
        dscore_out[rows, :] += dscore
        dbs_out[rows, :] += dbs
        dcs_out[rows, :] += dcs
        held_lane = (column_lane >= first_head) & (column_lane < first_head + HEADS_STEP)
        for slot, out in enumerate((up_out, on_out, step_out)):
            turn = lax.rem(first_head + lane_count - slot * HEADS_STEP, lane_count)
            out[rows, :] += jnp.where(held_lane, pltpu.roll(columns, turn, 1), 0.0)
        return unused

    lax.fori_loop(0, chunks, chunk_body, 0)


def chunk_terms(step_size, log_decay, segment, real_heads, head_size):
    length, heads = step_size.shape
    chunks = length // CHUNK
    parted = segment.reshape(chunks, CHUNK)
    places = jnp.arange(CHUNK)
    lower = (places[:, None] >= places[None, :]).astype(F32)
    allowed = (
        (parted[:, :, None] == parted[:, None, :]) & (places[:, None] >= places[None, :])[None]
    ).astype(F32)
    cumulative = jnp.einsum(
        "ts,csh->cth", lower, log_decay.reshape(chunks, CHUNK, heads), precision=HIGHEST
    )
    last = jnp.concatenate([jnp.full((1,), -2, segment.dtype), parted[:-1, CHUNK - 1]])
    carried = (parted == last[:, None]).astype(F32)
    final = parted[:, CHUNK - 1]
    at_end = (parted == final[:, None]).astype(F32)
    total = cumulative[:, CHUNK - 1]
    reach = jnp.exp(cumulative) * carried[:, :, None]
    to_end = jnp.exp(total[:, None, :] - cumulative) * at_end[:, :, None]
    kept = jnp.exp(total) * (final == last).astype(F32)[:, None]

    columns = (step_size, *(a.reshape(length, heads) for a in (cumulative, reach, to_end)))
    cum_rows = columns[1].T
    kept_rows = jnp.repeat(jnp.repeat(kept[:, :real_heads], head_size, axis=1), 8, axis=0)
    masks = jnp.stack(
        [
            jnp.broadcast_to(
                (shift_down(segment, back, -2) == segment).astype(F32)[:, None],
                (length, 2 * head_size),
            )
            for back in (1, 2, 3)
        ]
    )
    return allowed, columns, cum_rows, kept_rows, masks


def whole_spec(array):
    zeros = (0,) * array.ndim
    return pl.BlockSpec(array.shape, lambda g: zeros)


def lanes_spec(array, width):
    return pl.BlockSpec((array.shape[0], width), lambda g: (0, g))


def ssd_forward(xr, taps, bias, skip_row, terms, bs_low, cs_low, head_size):
    allowed, columns, cum_rows, kept_rows, masks = terms
    length, inner = xr.shape[0], taps.shape[1]
    width = HEADS_STEP * head_size
    groups = inner // width
    state_dim = bs_low.shape[1]
    chunks = length // CHUNK
    score = (
        jnp.einsum(
            "ctn,csn->cts",
            cs_low.reshape(chunks, CHUNK, state_dim),
            bs_low.reshape(chunks, CHUNK, state_dim),
            preferred_element_type=F32,
        )
        * allowed
    )
    shared = (masks, score.reshape(length, CHUNK), cs_low, bs_low.T, *columns)
    rows_spec = pl.BlockSpec((HEADS_STEP, length), lambda g: (g, 0))
    y, states = pl.pallas_call(
        ssd_forward_kernel,
        grid=(groups,),
        in_specs=[lanes_spec(a, width) for a in (xr, taps, bias, skip_row)]
        + [whole_spec(a) for a in shared]
        + [rows_spec, lanes_spec(kept_rows, width)],
        out_specs=[
            pl.BlockSpec((length, width), lambda g: (0, g)),
            pl.BlockSpec((chunks * state_dim, width), lambda g: (0, g)),
        ],
        out_shape=[
            jax.ShapeDtypeStruct((length, inner), F32),
            jax.ShapeDtypeStruct((chunks * state_dim, inner), BF16),
        ],
        scratch_shapes=[pltpu.VMEM((state_dim, width), F32)],
        cost_estimate=pl.CostEstimate(
            flops=130 * length * inner * CHUNK, bytes_accessed=12 * length * inner, transcendentals=0
        ),
        name="ssd_forward",
    )(xr, taps, bias, skip_row, *shared, cum_rows, kept_rows)
    return y, states, score


def ssd_backward(
    xr, taps, bias, skip_row, terms, score, bs_low, cs_low, states, dy, head_size
):
    allowed, columns, cum_rows, kept_rows, masks = terms
    length, inner = xr.shape[0], taps.shape[1]
    heads_step, heads = HEADS_STEP, columns[0].shape[1]
    width = heads_step * head_size
    groups = inner // width
    state_dim = bs_low.shape[1]
    chunks = length // CHUNK
    lane = jnp.arange(2 * head_size) // head_size
    pick = jnp.stack(
        [
            jnp.concatenate(
                [
                    (
                        (2 * pair + lane + slot * heads_step)[:, None] == jnp.arange(CHUNK)[None, :]
                    ).astype(BF16)
                    for slot in range(3)
                ]
            )
            for pair in range(heads_step // 2)
        ]
    )
    score_t = score.transpose(0, 2, 1).reshape(length, CHUNK)
    shared = (masks, score_t, cs_low, bs_low, cs_low.T, pick, *columns)
    rows_spec = pl.BlockSpec((heads_step, length), lambda g: (g, 0))
    fixed = pl.BlockSpec((length, CHUNK), lambda g: (0, 0))
    out = pl.pallas_call(
        ssd_backward_kernel,
        grid=(groups,),
        in_specs=[lanes_spec(a, width) for a in (xr, taps, bias, skip_row)]
        + [whole_spec(a) for a in shared]
        + [rows_spec, lanes_spec(kept_rows, width)]
        + [lanes_spec(a, width) for a in (states, dy)],
        out_specs=[
            pl.BlockSpec((length, width), lambda g: (0, g)),
            fixed,
            pl.BlockSpec((length, state_dim), lambda g: (0, 0)),
            pl.BlockSpec((length, state_dim), lambda g: (0, 0)),
            *[pl.BlockSpec((length, heads), lambda g: (0, 0))] * 3,
            rows_spec,
            pl.BlockSpec((8 * chunks, width), lambda g: (0, g)),
            pl.BlockSpec((8, width), lambda g: (0, g)),
        ],
        out_shape=[
            jax.ShapeDtypeStruct((length, inner), BF16),
            jax.ShapeDtypeStruct((length, CHUNK), F32),
            jax.ShapeDtypeStruct((length, state_dim), F32),
            jax.ShapeDtypeStruct((length, state_dim), F32),
            *[jax.ShapeDtypeStruct((length, heads), F32)] * 3,
            jax.ShapeDtypeStruct((groups * heads_step, length), F32),
            jax.ShapeDtypeStruct((8 * chunks, inner), F32),
            jax.ShapeDtypeStruct((8, inner), F32),
        ],
        scratch_shapes=[pltpu.VMEM((state_dim, width), F32), pltpu.VMEM((8, width), F32)],
        cost_estimate=pl.CostEstimate(
            flops=290 * length * inner * CHUNK, bytes_accessed=16 * length * inner, transcendentals=0
        ),
        name="ssd_backward",
    )(xr, taps, bias, skip_row, *shared, cum_rows, kept_rows, states, dy)
    dxr, dscore_t, dbs, dcs, upward, onward, dstep, rows, span, sums = out
    dscore_t = (dscore_t.reshape(chunks, CHUNK, CHUNK) * allowed.transpose(0, 2, 1)).astype(BF16)
    parted_c = cs_low.reshape(chunks, CHUNK, state_dim)
    parted_b = bs_low.reshape(chunks, CHUNK, state_dim)
    from_score_b = jnp.einsum("cst,ctn->csn", dscore_t, parted_c, preferred_element_type=F32)
    from_score_c = jnp.einsum("cst,csn->ctn", dscore_t, parted_b, preferred_element_type=F32)
    dbs = dbs + from_score_b.reshape(length, state_dim)
    dcs = dcs + from_score_c.reshape(length, state_dim)
    real_heads = groups * heads_step
    spare = heads - real_heads
    upward = upward + jnp.pad(rows.T, ((0, 0), (0, spare)))
    spans = jnp.sum(span[::8].reshape(chunks, real_heads, head_size), axis=2)
    spans = jnp.pad(spans, ((0, 0), (0, spare))).reshape(chunks, 1, heads)
    places = jnp.arange(CHUNK)
    at_or_after = (places[None, :] >= places[:, None]).astype(F32)
    ahead = (places[None, :] < places[:, None]).astype(F32)
    dlog = jnp.einsum(
        "rt,cth->crh", at_or_after, upward.reshape(chunks, CHUNK, heads), precision=HIGHEST
    )
    dlog = dlog + jnp.einsum(
        "rs,csh->crh", ahead, onward.reshape(chunks, CHUNK, heads), precision=HIGHEST
    )
    dlog = (dlog + spans).reshape(length, heads)
    return dxr, dbs, dcs, dstep, dlog, sums


def swap_pair(values):
    return lax.ppermute(values, "tensor", [(0, 1), (1, 0)])


def gather_pair(own, place):
    other = swap_pair(own)
    lower = jnp.where(place == 0, own, other)
    upper = jnp.where(place == 0, other, own)
    return jnp.concatenate([lower, upper], axis=0)


def scatter_pair(values, place):
    half = values.shape[0] // 2
    sent = lax.dynamic_slice_in_dim(values, (1 - place) * half, half)
    kept = lax.dynamic_slice_in_dim(values, place * half, half)
    return kept + swap_pair(sent)


def stage_orders(size):
    bits = size.bit_length() - 1
    if bits == 4:
        return ((0, 1, 2, 3), (1, 2, 3, 0), (2, 0, 1, 3))
    return tuple(tuple((bit + turn) % bits for bit in range(bits)) for turn in range(3))


def partner(values, bit):
    size = lax.axis_size("dp")
    return lax.ppermute(values, "dp", [(i, i ^ (1 << bit)) for i in range(size)])


def place_kernel(table, *refs):
    sources, (out, buffer, arrived, left) = refs[:-4], refs[-4:]
    turns, size = len(sources) // 4, out.shape[0]
    part = size // 4
    width = sources[0].shape[2]

    def arrival(turn, source, block, target):
        lanes = pl.ds(turn * width, width)
        return pltpu.make_async_copy(
            source.at[block], buffer.at[target, :, lanes], arrived.at[turn, target]
        )

    def start_in(target, unused):
        for turn in range(turns):
            block = table[turn, target]

            for place in range(4):

                @pl.when((block >= place * part) & (block < (place + 1) * part))
                def from_part():
                    source = sources[4 * turn + place]
                    arrival(turn, source, block - place * part, target).start()

        return unused

    def start_out(target, unused):
        for turn in range(turns):
            arrival(turn, sources[4 * turn], 0, target).wait()
        pltpu.make_async_copy(buffer.at[target], out.at[target], left.at[target]).start()
        return unused

    def finish(target, unused):
        pltpu.make_async_copy(buffer.at[target], out.at[target], left.at[target]).wait()
        return unused

    lax.fori_loop(0, size, start_in, 0)
    lax.fori_loop(0, size, start_out, 0)
    lax.fori_loop(0, size, finish, 0)


def gather_stages(pieces, first_stage, last_stage):
    size = lax.axis_size("dp")
    bits = size.bit_length() - 1
    for stage in range(first_stage, last_stage):
        joined = []
        for parts, order in zip(pieces, stage_orders(size)):
            others = [partner(part, order[::-1][stage]) for part in parts]
            if stage < bits - 2:
                joined.append([jnp.concatenate(parts + others, axis=0)])
            else:
                joined.append(parts + others)
        pieces = joined
    return pieces


def split_shard(shard):
    turns = len(stage_orders(lax.axis_size("dp")))
    width = shard.shape[1] // turns
    return [[shard[None, :, turn * width : (turn + 1) * width]] for turn in range(turns)]


def place_rows(pieces):
    size, index = lax.axis_size("dp"), lax.axis_index("dp")
    orders = stage_orders(size)
    targets = jnp.arange(size, dtype=jnp.int32) ^ index.astype(jnp.int32)
    tables = [
        sum(((targets >> bit) & 1) << stage for stage, bit in enumerate(order[::-1]))
        for order in orders
    ]
    _, rows, width = pieces[0][0].shape
    sources = [part for pair in pieces for part in pair]
    shape = (size, rows, width * len(orders))
    placed = pl.pallas_call(
        place_kernel,
        in_specs=[pl.BlockSpec(memory_space=pltpu.SMEM)]
        + [pl.BlockSpec(memory_space=pl.ANY)] * len(sources),
        out_specs=pl.BlockSpec(memory_space=pl.ANY),
        out_shape=jax.ShapeDtypeStruct(shape, BF16),
        scratch_shapes=[
            pltpu.VMEM(shape, BF16),
            pltpu.SemaphoreType.DMA((len(orders), size)),
            pltpu.SemaphoreType.DMA((size,)),
        ],
        cost_estimate=pl.CostEstimate(
            flops=0, bytes_accessed=4 * size * rows * shape[2], transcendentals=0
        ),
        name="place_rows",
    )(jnp.stack(tables), *sources)
    return placed.reshape(size * rows, shape[2])


def scatter_rows(pieces):
    size, index = lax.axis_size("dp"), lax.axis_index("dp")
    bits = size.bit_length() - 1
    orders = stage_orders(size)
    held, left = [], []
    for piece in pieces:
        held.append(piece.reshape((2,) * bits + (piece.shape[0] // size, piece.shape[1])))
        left.append(list(range(bits - 1, -1, -1)))
    for stage in range(bits):
        for turn, order in enumerate(orders[: len(pieces)]):
            bit = order[stage]
            axis = left[turn].index(bit)
            mine = (index >> bit) & 1
            sent = lax.dynamic_index_in_dim(held[turn], 1 - mine, axis, keepdims=False)
            kept = lax.dynamic_index_in_dim(held[turn], mine, axis, keepdims=False)
            got = partner(sent.astype(BF16), bit)
            held[turn] = kept.astype(F32) + got.astype(F32)
            left[turn].pop(axis)
    return held


def sum_small(values):
    for bit in range(lax.axis_size("dp").bit_length() - 1):
        values = values + partner(values, bit)
    return values


def shards(
    tokens,
    segment_ids,
    norm_gain,
    in_gate_inner,
    in_state,
    in_step,
    conv_inner,
    conv_inner_bias,
    conv_state,
    conv_state_bias,
    step_bias,
    decay_log,
    skip_gain,
    gate_gain,
    out_proj,
    cotangent,
):
    width, _, inner_dev = in_gate_inner.shape
    state_dim = in_state.shape[2]
    heads_dev = in_step.shape[1]
    head_size = inner_dev // heads_dev
    step_pad = -heads_dev % 128
    first_shard = jnp.concatenate(
        [
            in_gate_inner[:, 1],
            in_state.reshape(width, -1),
            in_step,
            jnp.zeros((width, step_pad), BF16),
        ],
        axis=1,
    )
    bits = lax.axis_size("dp").bit_length() - 1
    first_pieces = gather_stages(split_shard(first_shard), 0, bits - 1)
    held_back = (
        in_gate_inner,
        out_proj,
        tokens,
        cotangent,
        segment_ids,
        norm_gain,
        conv_inner,
        conv_inner_bias,
        conv_state,
        conv_state_bias,
        step_bias,
        decay_log,
        skip_gain,
        gate_gain,
    )
    first_pieces, held_back = lax.optimization_barrier((first_pieces, held_back))
    (
        in_gate_inner,
        out_proj,
        tokens,
        cotangent,
        segment_ids,
        norm_gain,
        conv_inner,
        conv_inner_bias,
        conv_state,
        conv_state_bias,
        step_bias,
        decay_log,
        skip_gain,
        gate_gain,
    ) = held_back
    later_shard = jnp.concatenate([in_gate_inner[:, 0], out_proj.T], axis=1)
    later_pieces = split_shard(later_shard)
    first_pieces = gather_stages(first_pieces, bits - 1, bits)
    later_pieces = gather_stages(later_pieces, 0, bits)
    half_rows = tokens.shape[0]
    model_width = tokens.shape[1]
    tensor_place = lax.axis_index("tensor")
    own_segment = lax.dynamic_slice_in_dim(segment_ids, tensor_place * half_rows, half_rows)
    own_live = (own_segment >= 0).astype(F32)[:, None]
    own_rows = tokens.astype(F32)
    row_scale = lax.rsqrt(jnp.mean(own_rows * own_rows, axis=1, keepdims=True) + EPSILON)
    normed_own = (own_rows * row_scale * norm_gain[None, :]).astype(BF16)
    first_weights = place_rows(first_pieces)
    normed = gather_pair(normed_own, tensor_place)
    first_proj = dot(normed, first_weights)
    state_end = inner_dev + 2 * state_dim
    inner_proj = first_proj
    state_proj = first_proj[:, inner_dev:state_end]
    step_proj = first_proj[:, state_end:]
    step_bias_row = jnp.pad(step_bias, (0, step_pad))[None]

    def state_piece(state_values, conv_taps, conv_bias):
        return jax.nn.silu(
            causal_conv(
                state_values,
                conv_taps.reshape(conv_taps.shape[0], -1),
                conv_bias.reshape(-1),
                segment_ids,
            )
        )

    state_act, state_back = jax.vjp(state_piece, state_proj, conv_state, conv_state_bias)
    bs_low = state_act[:, :state_dim].astype(BF16)
    cs_low = state_act[:, state_dim:].astype(BF16)
    step_size = jax.nn.softplus(step_proj + step_bias_row)
    decay_rate = -jnp.exp(jnp.pad(decay_log, (0, step_pad)))
    log_decay = step_size * decay_rate[None, :]
    terms = chunk_terms(step_size, log_decay, segment_ids, heads_dev, head_size)
    skip_row = jnp.repeat(skip_gain, head_size)[None]
    bias_row = conv_inner_bias[None]
    mixed, states, score = ssd_forward(
        inner_proj, conv_inner, bias_row, skip_row, terms, bs_low, cs_low, head_size
    )
    later_weights = place_rows(later_pieces)
    gate_weights = later_weights[:, :inner_dev]
    out_weights_t = later_weights[:, inner_dev:]
    gate_proj = dot(normed, gate_weights)
    gate_sigmoid = jax.nn.sigmoid(gate_proj)
    gated_values = mixed * (gate_proj * gate_sigmoid)
    full_inner = inner_dev * lax.axis_size("tensor")
    squares = lax.psum(jnp.sum(gated_values * gated_values, axis=1), "tensor")
    gate_scale = lax.rsqrt(squares / full_inner + EPSILON)[:, None]
    normed_inner = (gated_values * gate_scale * gate_gain[None, :]).astype(BF16)
    partial_out = jnp.einsum(
        "tc,dc->td", normed_inner, out_weights_t, preferred_element_type=F32
    )
    branch_own = scatter_pair(partial_out, tensor_place)
    block_out = (own_rows + own_live * branch_own).astype(BF16)
    cot_rows = cotangent.astype(F32)
    branch_grad_own = (own_live * cot_rows).astype(BF16)
    branch_grad = gather_pair(branch_grad_own, tensor_place)
    grad_out_proj_t = jnp.einsum(
        "td,tc->dc", branch_grad, normed_inner, preferred_element_type=F32
    )
    grad_normed_inner = jnp.einsum(
        "td,dc->tc", branch_grad, out_weights_t, preferred_element_type=F32
    )
    grad_gate_gain = jnp.sum(grad_normed_inner * gated_values * gate_scale, axis=0)
    scaled_grad = grad_normed_inner * gate_gain[None, :]
    products = lax.psum(jnp.sum(scaled_grad * gated_values, axis=1), "tensor")
    grad_gated = (
        gate_scale * scaled_grad - gated_values * gate_scale**3 * (products / full_inner)[:, None]
    )
    low_gate = (
        grad_gated * mixed * (gate_sigmoid * (1.0 + gate_proj * (1.0 - gate_sigmoid)))
    ).astype(BF16)
    grad_mixed = grad_gated * (gate_proj * gate_sigmoid)
    grad_gate_half = jnp.einsum(
        "td,tc->dc", normed, low_gate, preferred_element_type=F32
    ).astype(BF16)
    grad_out_low = grad_out_proj_t.astype(BF16)
    grad_mixed, grad_gate_half, grad_out_low = lax.optimization_barrier(
        (grad_mixed, grad_gate_half, grad_out_low)
    )
    cut = 2 * inner_dev // 3
    early_parts = scatter_rows(
        [
            grad_gate_half[:, :cut],
            jnp.concatenate([grad_gate_half[:, cut:], grad_out_low[:, : 2 * cut - inner_dev]], axis=1),
            grad_out_low[:, 2 * cut - inner_dev :],
        ],
    )
    early_part = jnp.concatenate(early_parts, axis=1)
    gate_part, out_part = early_part[:, :inner_dev], early_part[:, inner_dev:]
    scan_back = ssd_backward(
        inner_proj,
        conv_inner,
        bias_row,
        skip_row,
        terms,
        score,
        bs_low,
        cs_low,
        states,
        grad_mixed,
        head_size,
    )
    low_inner, grad_bs, grad_cs, grad_step_size, grad_log, inner_sums = scan_back
    taps_count = conv_inner.shape[0]
    grad_conv_inner = inner_sums[:taps_count][::-1]
    grad_conv_inner_bias = inner_sums[taps_count]
    grad_skip_gain = jnp.sum(inner_sums[taps_count + 1].reshape(heads_dev, head_size), axis=1)
    grad_decay_log = jnp.sum(grad_log * log_decay, axis=0)[:heads_dev]
    grad_step_proj = (grad_step_size + grad_log * decay_rate[None, :]) * jax.nn.sigmoid(
        step_proj + step_bias_row
    )
    grad_step_bias = jnp.sum(grad_step_proj, axis=0)[:heads_dev]
    grad_inner = jnp.einsum("td,tc->dc", normed, low_inner, preferred_element_type=F32).astype(BF16)
    grad_state_part = jnp.concatenate([grad_bs, grad_cs], axis=1)
    grad_state_act = grad_state_part + swap_pair(grad_state_part)
    grad_state_proj, grad_conv_state, grad_conv_state_bias = state_back(grad_state_act)
    low_state = grad_state_proj.astype(BF16)
    low_step = grad_step_proj.astype(BF16)
    own_state = low_state * (tensor_place == 0).astype(BF16)
    low_rest = jnp.concatenate([low_state, low_step], axis=1)
    low_rest_own = jnp.concatenate([own_state, low_step], axis=1)
    grad_rest = jnp.einsum("td,tc->dc", normed, low_rest, preferred_element_type=F32).astype(BF16)
    third = inner_dev // 3
    late_parts = scatter_rows(
        [grad_inner[:, turn * third : (turn + 1) * third] for turn in range(3)]
    )
    first_part = jnp.concatenate(late_parts + scatter_rows([grad_rest]), axis=1)
    grad_out_proj = out_part.T
    grad_in_gate_inner = jnp.stack([gate_part, first_part[:, :inner_dev]], axis=1)
    grad_in_state = first_part[:, inner_dev:state_end].reshape(in_state.shape)
    grad_in_step = first_part[:, state_end : state_end + heads_dev]
    head_grads = (
        dot_nt(low_gate, gate_weights)
        + dot_nt(low_inner, first_weights[:, :inner_dev])
        + dot_nt(low_rest_own, first_weights[:, inner_dev:])
    )
    normed_grad_own = scatter_pair(head_grads, tensor_place)
    grad_norm_part = jnp.sum(normed_grad_own * own_rows * row_scale, axis=0)
    scaled_rows = normed_grad_own * norm_gain[None, :]
    row_products = jnp.sum(scaled_rows * own_rows, axis=1, keepdims=True)
    grad_tokens = (
        cot_rows + row_scale * scaled_rows - own_rows * row_scale**3 * row_products / model_width
    )
    small_parts = (
        grad_norm_part + swap_pair(grad_norm_part),
        grad_conv_inner,
        grad_conv_inner_bias,
        grad_conv_state,
        grad_conv_state_bias,
        grad_step_bias,
        grad_decay_log,
        grad_skip_gain,
        grad_gate_gain,
    )
    summed = sum_small(jnp.concatenate([part.reshape(-1) for part in small_parts]))
    small, start = [], 0
    for part in small_parts:
        small.append(summed[start : start + part.size].reshape(part.shape))
        start += part.size
    return (
        block_out,
        grad_tokens,
        small[0],
        grad_in_gate_inner,
        grad_in_state,
        grad_in_step,
        *small[1:],
        grad_out_proj,
    )


def solution(mesh):
    in_specs = (
        P(("dp", "tensor"), None),
        P("dp"),
        P(),
        P("dp", None, "tensor"),
        P("dp", None, None),
        P("dp", "tensor"),
        P(None, "tensor"),
        P("tensor"),
        P(),
        P(),
        P("tensor"),
        P("tensor"),
        P("tensor"),
        P("tensor"),
        P("tensor", "dp"),
        P(("dp", "tensor"), None),
    )
    out_specs = (
        P(("dp", "tensor"), None),
        P(("dp", "tensor"), None),
        P(),
        P("dp", None, "tensor"),
        P("dp", None, None),
        P("dp", "tensor"),
        P(None, "tensor"),
        P("tensor"),
        P(),
        P(),
        P("tensor"),
        P("tensor"),
        P("tensor"),
        P("tensor"),
        P("tensor", "dp"),
    )

    return jax.shard_map(shards, mesh=mesh, in_specs=in_specs, out_specs=out_specs, check_vma=False)
```

```python
import jax
import jax.numpy as jnp
from jax import lax
from jax.experimental import pallas as pl
from jax.experimental.pallas import tpu as pltpu
from jax.sharding import PartitionSpec as P


EPSILON = 1e-05
HIGHEST = lax.Precision.HIGHEST
CHUNK = 128
HEADS_STEP = 8
F32 = jnp.float32
BF16 = jnp.bfloat16


def shift_down(values, steps_back, filler):
    leading = jnp.full((steps_back,) + values.shape[1:], filler, values.dtype)
    return jnp.concatenate([leading, values[: values.shape[0] - steps_back]], axis=0)


def causal_conv(values, conv_taps, conv_bias, segment):
    taps_count = conv_taps.shape[0]
    result = conv_bias[None, :] + conv_taps[taps_count - 1][None, :] * values
    for steps_back in range(1, taps_count):
        earlier = shift_down(values, steps_back, 0.0)
        same_seq = (shift_down(segment, steps_back, -2) == segment).astype(values.dtype)
        result = (
            result + conv_taps[taps_count - 1 - steps_back][None, :] * earlier * same_seq[:, None]
        )
    return result


def dot(a, b):
    return jnp.dot(a, b, preferred_element_type=F32)


def dot_nt(a, b):
    return lax.dot_general(a, b, (((1,), (1,)), ((), ())), preferred_element_type=F32)


def spread_heads(columns, pair, head_size):
    lane = lax.broadcasted_iota(jnp.int32, (columns.shape[0], 2 * head_size), 1)
    first = columns[:, 2 * pair : 2 * pair + 1]
    second = columns[:, 2 * pair + 1 : 2 * pair + 2]
    return jnp.where(lane < head_size, first, second)


def conv_pair(xr, taps, bias, masks, rows, before, lanes):
    current = xr[rows, lanes]
    joined = jnp.concatenate([xr[before, lanes], current], axis=0)
    count = taps.shape[0]
    value = bias[0:1, lanes] + taps[count - 1 : count, lanes] * current
    shifted = []
    for back in range(1, count):
        piece = pltpu.roll(joined, back, 0)[8:] * masks[back - 1, rows, :]
        shifted.append(piece)
        value = value + taps[count - 1 - back : count - back, lanes] * piece
    return current, shifted, value


def ssd_forward_kernel(
    xr, taps, bias, skip, masks, score, cs, bst, dt, cumc, reach, toend, cumr, kept,
    y_out, states_out, state,
):
    width = xr.shape[1]
    head_size = width // HEADS_STEP
    pair_width = 2 * head_size
    chunks = xr.shape[0] // CHUNK
    lane_count = dt.shape[1]
    to_front = lax.rem(lane_count - pl.program_id(0) * HEADS_STEP, lane_count)
    state[...] = jnp.zeros_like(state)

    def chunk_body(place, unused):
        start = pl.multiple_of(place * CHUNK, CHUNK)
        rows = pl.ds(start, CHUNK)
        before = pl.ds(pl.multiple_of(jnp.maximum(start - 8, 0), 8), 8)
        dt_cols, cum_cols, reach_cols, end_cols = (
            pltpu.roll(ref[rows, :], to_front, 1) for ref in (dt, cumc, reach, toend)
        )
        score_now, cs_now, bst_now = score[rows, :], cs[rows, :], bst[:, rows]
        lane = lax.broadcasted_iota(jnp.int32, (CHUNK, pair_width), 1)
        row_of = pl.ds(pl.multiple_of(place * 8, 8), 8)
        for pair in range(width // pair_width):
            lanes = slice(pair * pair_width, (pair + 1) * pair_width)
            _, _, value = conv_pair(
                xr, taps, bias, masks, rows, before, lanes
            )
            x = value * jax.nn.sigmoid(value)
            xdt = x * spread_heads(dt_cols, pair, head_size)
            xb = xdt.astype(BF16)
            held = state[:, lanes]
            held_low = held.astype(BF16)
            states_out[rows, lanes] = held_low
            halves = []
            for head in (2 * pair, 2 * pair + 1):
                spread = cum_cols[:, head : head + 1] - cumr[head : head + 1, rows]
                mixing = score_now * jnp.exp(jnp.minimum(spread, 0.0))
                halves.append(dot(mixing.astype(BF16), xb))
            y = jnp.where(lane < head_size, halves[0], halves[1])
            y = y + spread_heads(reach_cols, pair, head_size) * dot(cs_now, held_low)
            y_out[rows, lanes] = y + skip[0:1, lanes] * x
            fresh = dot(bst_now, (xdt * spread_heads(end_cols, pair, head_size)).astype(BF16))
            state[:, lanes] = fresh + kept[row_of, lanes][0:1] * held
        return unused

    lax.fori_loop(0, chunks, chunk_body, 0)


def ssd_backward_kernel(
    xr, taps, bias, skip, masks, score_t, cs, bs, cst, pick, dt, cumc, reach, toend, cumr, kept,
    states, dy,
    dxr_out, dscore_out, dbs_out, dcs_out, up_out, on_out, step_out, rows_out, span_out, sums_out,
    dstate, dvalue_next,
):
    width = xr.shape[1]
    head_size = width // HEADS_STEP
    pair_width = 2 * head_size
    length = xr.shape[0]
    chunks = length // CHUNK
    count = taps.shape[0]
    lane_count = dt.shape[1]
    first_head = pl.program_id(0) * HEADS_STEP
    to_front = lax.rem(lane_count - first_head, lane_count)
    dstate[...] = jnp.zeros_like(dstate)
    dvalue_next[...] = jnp.zeros_like(dvalue_next)
    sums_out[...] = jnp.zeros_like(sums_out)

    @pl.when(pl.program_id(0) == 0)
    def clear():
        dscore_out[...] = jnp.zeros_like(dscore_out)
        dbs_out[...] = jnp.zeros_like(dbs_out)
        dcs_out[...] = jnp.zeros_like(dcs_out)
        up_out[...] = jnp.zeros_like(up_out)
        on_out[...] = jnp.zeros_like(on_out)
        step_out[...] = jnp.zeros_like(step_out)

    def chunk_body(step, unused):
        place = chunks - 1 - step
        start = pl.multiple_of(place * CHUNK, CHUNK)
        rows = pl.ds(start, CHUNK)
        before = pl.ds(pl.multiple_of(jnp.maximum(start - 8, 0), 8), 8)
        after = pl.ds(pl.multiple_of(jnp.minimum(start + CHUNK, length - 8), 8), 8)
        dt_cols, cum_cols, reach_cols, end_cols = (
            pltpu.roll(ref[rows, :], to_front, 1) for ref in (dt, cumc, reach, toend)
        )
        score_now, cs_now, bs_now, cst_now = score_t[rows, :], cs[rows, :], bs[rows, :], cst[:, rows]
        lane = lax.broadcasted_iota(jnp.int32, (CHUNK, pair_width), 1)
        row_of = pl.ds(pl.multiple_of(place * 8, 8), 8)
        dscore = jnp.zeros((CHUNK, CHUNK), F32)
        dbs = jnp.zeros((CHUNK, bs_now.shape[1]), F32)
        dcs = jnp.zeros((CHUNK, bs_now.shape[1]), F32)
        columns = jnp.zeros((CHUNK, lane_count), F32)
        column_lane = lax.broadcasted_iota(jnp.int32, columns.shape, 1)
        for pair in range(width // pair_width):
            lanes = slice(pair * pair_width, (pair + 1) * pair_width)
            current, shifted, value = conv_pair(xr, taps, bias, masks, rows, before, lanes)
            gate = jax.nn.sigmoid(value)
            x = value * gate
            dt_now = spread_heads(dt_cols, pair, head_size)
            end_now = spread_heads(end_cols, pair, head_size)
            xdt = x * dt_now
            xb = xdt.astype(BF16)
            dy_now = dy[rows, lanes]
            dyb = dy_now.astype(BF16)
            held_low = states[rows, lanes]
            dheld = dstate[:, lanes]
            dheld_low = dheld.astype(BF16)
            dyr = dy_now * spread_heads(reach_cols, pair, head_size)
            dyr_low = dyr.astype(BF16)
            from_state = dyr * dot(cs_now, held_low)
            dcs = dcs + dot_nt(dyr_low, held_low)
            dxdt_end = end_now * dot(bs_now, dheld_low)
            dbs = dbs + dot_nt((xdt * end_now).astype(BF16), dheld_low)
            halves = []
            for side in (0, 1):
                head = 2 * pair + side
                spread = cumr[head : head + 1, rows] - cum_cols[:, head : head + 1]
                decay = jnp.exp(jnp.minimum(spread, 0.0))
                weight = score_now * decay
                own = (lane < head_size) if side == 0 else (lane >= head_size)
                pairs = dot_nt(jnp.where(own, xdt, 0.0).astype(BF16), dyb)
                dscore = dscore + pairs * decay
                share = pairs * weight
                columns = columns - jnp.where(
                    column_lane == head, jnp.sum(share, axis=1, keepdims=True), 0.0
                )
                rows_out[head : head + 1, rows] = jnp.sum(share, axis=0, keepdims=True)
                halves.append(dot(weight.astype(BF16), dyb))
            dxdt = jnp.where(lane < head_size, halves[0], halves[1]) + dxdt_end
            picked = jnp.concatenate(
                [
                    from_state.astype(BF16),
                    (xdt * dxdt_end).astype(BF16),
                    (x * dxdt).astype(BF16),
                ],
                axis=1,
            )
            columns = columns + dot(picked, pick[pair])
            dx = skip[0:1, lanes] * dy_now + dt_now * dxdt
            kept_row = kept[row_of, lanes][0:1]
            span_row = kept_row * jnp.sum(dheld * held_low.astype(F32), axis=0, keepdims=True)
            span_out[row_of, lanes] = jnp.broadcast_to(span_row, (8, pair_width))
            dstate[:, lanes] = kept_row * dheld + dot(cst_now, dyr_low)
            dvalue = dx * (gate * (1.0 + value * (1.0 - gate)))
            dxr = taps[count - 1 : count, lanes] * dvalue
            next_rows = dvalue_next[:, lanes]
            sums = [jnp.sum(dvalue * current, axis=0, keepdims=True)]
            for back in range(1, count):
                masked = dvalue * masks[back - 1, rows, :]
                joined = jnp.concatenate(
                    [masked, next_rows * masks[back - 1, after, :]], axis=0
                )
                lifted = pltpu.roll(joined, CHUNK + 8 - back, 0)[:CHUNK]
                dxr = dxr + taps[count - 1 - back : count - back, lanes] * lifted
                sums.append(jnp.sum(dvalue * shifted[back - 1], axis=0, keepdims=True))
            dvalue_next[:, lanes] = dvalue[:8]
            sums.append(jnp.sum(dvalue, axis=0, keepdims=True))
            sums.append(jnp.sum(dy_now * x, axis=0, keepdims=True))
            for slot, row in enumerate(sums):
                sums_out[slot : slot + 1, lanes] += row
            dxr_out[rows, lanes] = dxr.astype(dxr_out.dtype)
        dscore_out[rows, :] += dscore
        dbs_out[rows, :] += dbs
        dcs_out[rows, :] += dcs
        held_lane = (column_lane >= first_head) & (column_lane < first_head + HEADS_STEP)
        for slot, out in enumerate((up_out, on_out, step_out)):
            turn = lax.rem(first_head + lane_count - slot * HEADS_STEP, lane_count)
            out[rows, :] += jnp.where(held_lane, pltpu.roll(columns, turn, 1), 0.0)
        return unused

    lax.fori_loop(0, chunks, chunk_body, 0)


def chunk_terms(step_size, log_decay, segment, real_heads, head_size):
    length, heads = step_size.shape
    chunks = length // CHUNK
    parted = segment.reshape(chunks, CHUNK)
    places = jnp.arange(CHUNK)
    lower = (places[:, None] >= places[None, :]).astype(F32)
    allowed = (
        (parted[:, :, None] == parted[:, None, :]) & (places[:, None] >= places[None, :])[None]
    ).astype(F32)
    cumulative = jnp.einsum(
        "ts,csh->cth", lower, log_decay.reshape(chunks, CHUNK, heads), precision=HIGHEST
    )
    last = jnp.concatenate([jnp.full((1,), -2, segment.dtype), parted[:-1, CHUNK - 1]])
    carried = (parted == last[:, None]).astype(F32)
    final = parted[:, CHUNK - 1]
    at_end = (parted == final[:, None]).astype(F32)
    total = cumulative[:, CHUNK - 1]
    reach = jnp.exp(cumulative) * carried[:, :, None]
    to_end = jnp.exp(total[:, None, :] - cumulative) * at_end[:, :, None]
    kept = jnp.exp(total) * (final == last).astype(F32)[:, None]

    columns = (step_size, *(a.reshape(length, heads) for a in (cumulative, reach, to_end)))
    cum_rows = columns[1].T
    kept_rows = jnp.repeat(jnp.repeat(kept[:, :real_heads], head_size, axis=1), 8, axis=0)
    masks = jnp.stack(
        [
            jnp.broadcast_to(
                (shift_down(segment, back, -2) == segment).astype(F32)[:, None],
                (length, 2 * head_size),
            )
            for back in (1, 2, 3)
        ]
    )
    return allowed, columns, cum_rows, kept_rows, masks


def whole_spec(array):
    zeros = (0,) * array.ndim
    return pl.BlockSpec(array.shape, lambda g: zeros)


def lanes_spec(array, width):
    return pl.BlockSpec((array.shape[0], width), lambda g: (0, g))


def ssd_forward(xr, taps, bias, skip_row, terms, bs_low, cs_low, head_size):
    allowed, columns, cum_rows, kept_rows, masks = terms
    length, inner = xr.shape[0], taps.shape[1]
    width = HEADS_STEP * head_size
    groups = inner // width
    state_dim = bs_low.shape[1]
    chunks = length // CHUNK
    score = (
        jnp.einsum(
            "ctn,csn->cts",
            cs_low.reshape(chunks, CHUNK, state_dim),
            bs_low.reshape(chunks, CHUNK, state_dim),
            preferred_element_type=F32,
        )
        * allowed
    )
    shared = (masks, score.reshape(length, CHUNK), cs_low, bs_low.T, *columns)
    rows_spec = pl.BlockSpec((HEADS_STEP, length), lambda g: (g, 0))
    y, states = pl.pallas_call(
        ssd_forward_kernel,
        grid=(groups,),
        in_specs=[lanes_spec(a, width) for a in (xr, taps, bias, skip_row)]
        + [whole_spec(a) for a in shared]
        + [rows_spec, lanes_spec(kept_rows, width)],
        out_specs=[
            pl.BlockSpec((length, width), lambda g: (0, g)),
            pl.BlockSpec((chunks * state_dim, width), lambda g: (0, g)),
        ],
        out_shape=[
            jax.ShapeDtypeStruct((length, inner), F32),
            jax.ShapeDtypeStruct((chunks * state_dim, inner), BF16),
        ],
        scratch_shapes=[pltpu.VMEM((state_dim, width), F32)],
        cost_estimate=pl.CostEstimate(
            flops=130 * length * inner * CHUNK, bytes_accessed=12 * length * inner, transcendentals=0
        ),
        name="ssd_forward",
    )(xr, taps, bias, skip_row, *shared, cum_rows, kept_rows)
    return y, states, score


def ssd_backward(
    xr, taps, bias, skip_row, terms, score, bs_low, cs_low, states, dy, head_size
):
    allowed, columns, cum_rows, kept_rows, masks = terms
    length, inner = xr.shape[0], taps.shape[1]
    heads_step, heads = HEADS_STEP, columns[0].shape[1]
    width = heads_step * head_size
    groups = inner // width
    state_dim = bs_low.shape[1]
    chunks = length // CHUNK
    lane = jnp.arange(2 * head_size) // head_size
    pick = jnp.stack(
        [
            jnp.concatenate(
                [
                    (
                        (2 * pair + lane + slot * heads_step)[:, None] == jnp.arange(CHUNK)[None, :]
                    ).astype(BF16)
                    for slot in range(3)
                ]
            )
            for pair in range(heads_step // 2)
        ]
    )
    score_t = score.transpose(0, 2, 1).reshape(length, CHUNK)
    shared = (masks, score_t, cs_low, bs_low, cs_low.T, pick, *columns)
    rows_spec = pl.BlockSpec((heads_step, length), lambda g: (g, 0))
    fixed = pl.BlockSpec((length, CHUNK), lambda g: (0, 0))
    out = pl.pallas_call(
        ssd_backward_kernel,
        grid=(groups,),
        in_specs=[lanes_spec(a, width) for a in (xr, taps, bias, skip_row)]
        + [whole_spec(a) for a in shared]
        + [rows_spec, lanes_spec(kept_rows, width)]
        + [lanes_spec(a, width) for a in (states, dy)],
        out_specs=[
            pl.BlockSpec((length, width), lambda g: (0, g)),
            fixed,
            pl.BlockSpec((length, state_dim), lambda g: (0, 0)),
            pl.BlockSpec((length, state_dim), lambda g: (0, 0)),
            *[pl.BlockSpec((length, heads), lambda g: (0, 0))] * 3,
            rows_spec,
            pl.BlockSpec((8 * chunks, width), lambda g: (0, g)),
            pl.BlockSpec((8, width), lambda g: (0, g)),
        ],
        out_shape=[
            jax.ShapeDtypeStruct((length, inner), BF16),
            jax.ShapeDtypeStruct((length, CHUNK), F32),
            jax.ShapeDtypeStruct((length, state_dim), F32),
            jax.ShapeDtypeStruct((length, state_dim), F32),
            *[jax.ShapeDtypeStruct((length, heads), F32)] * 3,
            jax.ShapeDtypeStruct((groups * heads_step, length), F32),
            jax.ShapeDtypeStruct((8 * chunks, inner), F32),
            jax.ShapeDtypeStruct((8, inner), F32),
        ],
        scratch_shapes=[pltpu.VMEM((state_dim, width), F32), pltpu.VMEM((8, width), F32)],
        cost_estimate=pl.CostEstimate(
            flops=290 * length * inner * CHUNK, bytes_accessed=16 * length * inner, transcendentals=0
        ),
        name="ssd_backward",
    )(xr, taps, bias, skip_row, *shared, cum_rows, kept_rows, states, dy)
    dxr, dscore_t, dbs, dcs, upward, onward, dstep, rows, span, sums = out
    dscore_t = (dscore_t.reshape(chunks, CHUNK, CHUNK) * allowed.transpose(0, 2, 1)).astype(BF16)
    parted_c = cs_low.reshape(chunks, CHUNK, state_dim)
    parted_b = bs_low.reshape(chunks, CHUNK, state_dim)
    from_score_b = jnp.einsum("cst,ctn->csn", dscore_t, parted_c, preferred_element_type=F32)
    from_score_c = jnp.einsum("cst,csn->ctn", dscore_t, parted_b, preferred_element_type=F32)
    dbs = dbs + from_score_b.reshape(length, state_dim)
    dcs = dcs + from_score_c.reshape(length, state_dim)
    real_heads = groups * heads_step
    spare = heads - real_heads
    upward = upward + jnp.pad(rows.T, ((0, 0), (0, spare)))
    spans = jnp.sum(span[::8].reshape(chunks, real_heads, head_size), axis=2)
    spans = jnp.pad(spans, ((0, 0), (0, spare))).reshape(chunks, 1, heads)
    places = jnp.arange(CHUNK)
    at_or_after = (places[None, :] >= places[:, None]).astype(F32)
    ahead = (places[None, :] < places[:, None]).astype(F32)
    dlog = jnp.einsum(
        "rt,cth->crh", at_or_after, upward.reshape(chunks, CHUNK, heads), precision=HIGHEST
    )
    dlog = dlog + jnp.einsum(
        "rs,csh->crh", ahead, onward.reshape(chunks, CHUNK, heads), precision=HIGHEST
    )
    dlog = (dlog + spans).reshape(length, heads)
    return dxr, dbs, dcs, dstep, dlog, sums


def swap_pair(values):
    return lax.ppermute(values, "tensor", [(0, 1), (1, 0)])


def gather_pair(own, place):
    other = swap_pair(own)
    lower = jnp.where(place == 0, own, other)
    upper = jnp.where(place == 0, other, own)
    return jnp.concatenate([lower, upper], axis=0)


def scatter_pair(values, place):
    half = values.shape[0] // 2
    sent = lax.dynamic_slice_in_dim(values, (1 - place) * half, half)
    kept = lax.dynamic_slice_in_dim(values, place * half, half)
    return kept + swap_pair(sent)


def stage_orders(size):
    bits = size.bit_length() - 1
    if bits == 4:
        return ((0, 1, 2, 3), (1, 2, 3, 0), (2, 0, 1, 3))
    return tuple(tuple((bit + turn) % bits for bit in range(bits)) for turn in range(3))


def exchange(values, mask):
    size = lax.axis_size("dp")
    return lax.ppermute(values, "dp", [(i, i ^ mask) for i in range(size)])


def partner(values, bit):
    return exchange(values, 1 << bit)


def place_kernel(table, *refs):
    sources, (out, buffer, arrived, left) = refs[:-4], refs[-4:]
    turns, size = len(sources) // 4, out.shape[0]
    part = size // 4
    width = sources[0].shape[2]

    def arrival(turn, source, block, target):
        lanes = pl.ds(turn * width, width)
        return pltpu.make_async_copy(
            source.at[block], buffer.at[target, :, lanes], arrived.at[turn, target]
        )

    def start_in(target, unused):
        for turn in range(turns):
            block = table[turn, target]

            for place in range(4):

                @pl.when((block >= place * part) & (block < (place + 1) * part))
                def from_part():
                    source = sources[4 * turn + place]
                    arrival(turn, source, block - place * part, target).start()

        return unused

    def start_out(target, unused):
        for turn in range(turns):
            arrival(turn, sources[4 * turn], 0, target).wait()
        pltpu.make_async_copy(buffer.at[target], out.at[target], left.at[target]).start()
        return unused

    def finish(target, unused):
        pltpu.make_async_copy(buffer.at[target], out.at[target], left.at[target]).wait()
        return unused

    lax.fori_loop(0, size, start_in, 0)
    lax.fori_loop(0, size, start_out, 0)
    lax.fori_loop(0, size, finish, 0)


def gather_stages(pieces, first_stage, last_stage):
    size = lax.axis_size("dp")
    bits = size.bit_length() - 1
    for stage in range(first_stage, last_stage):
        joined = []
        for parts, order in zip(pieces, stage_orders(size)):
            others = [partner(part, order[::-1][stage]) for part in parts]
            if stage < bits - 2:
                joined.append([jnp.concatenate(parts + others, axis=0)])
            else:
                joined.append(parts + others)
        pieces = joined
    return pieces


def split_shard(shard):
    turns = len(stage_orders(lax.axis_size("dp")))
    width = shard.shape[1] // turns
    return [[shard[None, :, turn * width : (turn + 1) * width]] for turn in range(turns)]


def place_rows(pieces):
    size, index = lax.axis_size("dp"), lax.axis_index("dp")
    orders = stage_orders(size)
    targets = jnp.arange(size, dtype=jnp.int32) ^ index.astype(jnp.int32)
    tables = [
        sum(((targets >> bit) & 1) << stage for stage, bit in enumerate(order[::-1]))
        for order in orders
    ]
    _, rows, width = pieces[0][0].shape
    sources = [part for pair in pieces for part in pair]
    shape = (size, rows, width * len(orders))
    placed = pl.pallas_call(
        place_kernel,
        in_specs=[pl.BlockSpec(memory_space=pltpu.SMEM)]
        + [pl.BlockSpec(memory_space=pl.ANY)] * len(sources),
        out_specs=pl.BlockSpec(memory_space=pl.ANY),
        out_shape=jax.ShapeDtypeStruct(shape, BF16),
        scratch_shapes=[
            pltpu.VMEM(shape, BF16),
            pltpu.SemaphoreType.DMA((len(orders), size)),
            pltpu.SemaphoreType.DMA((size,)),
        ],
        cost_estimate=pl.CostEstimate(
            flops=0, bytes_accessed=4 * size * rows * shape[2], transcendentals=0
        ),
        name="place_rows",
    )(jnp.stack(tables), *sources)
    return placed.reshape(size * rows, shape[2])


def scatter_rows(pieces):
    size, index = lax.axis_size("dp"), lax.axis_index("dp")
    bits = size.bit_length() - 1
    orders = stage_orders(size)
    held, left = [], []
    for piece in pieces:
        held.append(piece.reshape((2,) * bits + (piece.shape[0] // size, piece.shape[1])))
        left.append(list(range(bits - 1, -1, -1)))
    for stage in range(bits):
        for turn, order in enumerate(orders[: len(pieces)]):
            bit = order[stage]
            axis = left[turn].index(bit)
            mine = (index >> bit) & 1
            sent = lax.dynamic_index_in_dim(held[turn], 1 - mine, axis, keepdims=False)
            kept = lax.dynamic_index_in_dim(held[turn], mine, axis, keepdims=False)
            got = partner(sent.astype(BF16), bit)
            held[turn] = kept.astype(F32) + got.astype(F32)
            left[turn].pop(axis)
    return held


def sum_small(values):
    bits = lax.axis_size("dp").bit_length() - 1
    for bit in range(0, bits, 2):
        if bit + 1 == bits:
            values = values + exchange(values, 1 << bit)
        else:
            near, far, cross = (exchange(values, turn << bit) for turn in (1, 2, 3))
            values = (values + near) + (far + cross)
    return values


def shards(
    tokens,
    segment_ids,
    norm_gain,
    in_gate_inner,
    in_state,
    in_step,
    conv_inner,
    conv_inner_bias,
    conv_state,
    conv_state_bias,
    step_bias,
    decay_log,
    skip_gain,
    gate_gain,
    out_proj,
    cotangent,
):
    width, _, inner_dev = in_gate_inner.shape
    state_dim = in_state.shape[2]
    heads_dev = in_step.shape[1]
    head_size = inner_dev // heads_dev
    step_pad = -heads_dev % 128
    first_shard = jnp.concatenate(
        [
            in_gate_inner[:, 1],
            in_state.reshape(width, -1),
            in_step,
            jnp.zeros((width, step_pad), BF16),
        ],
        axis=1,
    )
    bits = lax.axis_size("dp").bit_length() - 1
    first_pieces = gather_stages(split_shard(first_shard), 0, bits - 1)
    held_back = (
        in_gate_inner,
        out_proj,
        tokens,
        cotangent,
        segment_ids,
        norm_gain,
        conv_inner,
        conv_inner_bias,
        conv_state,
        conv_state_bias,
        step_bias,
        decay_log,
        skip_gain,
        gate_gain,
    )
    first_pieces, held_back = lax.optimization_barrier((first_pieces, held_back))
    (
        in_gate_inner,
        out_proj,
        tokens,
        cotangent,
        segment_ids,
        norm_gain,
        conv_inner,
        conv_inner_bias,
        conv_state,
        conv_state_bias,
        step_bias,
        decay_log,
        skip_gain,
        gate_gain,
    ) = held_back
    later_shard = jnp.concatenate([in_gate_inner[:, 0], out_proj.T], axis=1)
    later_pieces = split_shard(later_shard)
    first_pieces = gather_stages(first_pieces, bits - 1, bits)
    later_pieces = gather_stages(later_pieces, 0, bits)
    half_rows = tokens.shape[0]
    model_width = tokens.shape[1]
    tensor_place = lax.axis_index("tensor")
    own_segment = lax.dynamic_slice_in_dim(segment_ids, tensor_place * half_rows, half_rows)
    own_live = (own_segment >= 0).astype(F32)[:, None]
    own_rows = tokens.astype(F32)
    row_scale = lax.rsqrt(jnp.mean(own_rows * own_rows, axis=1, keepdims=True) + EPSILON)
    normed_own = (own_rows * row_scale * norm_gain[None, :]).astype(BF16)
    first_weights = place_rows(first_pieces)
    normed = gather_pair(normed_own, tensor_place)
    first_proj = dot(normed, first_weights)
    state_end = inner_dev + 2 * state_dim
    inner_proj = first_proj
    state_proj = first_proj[:, inner_dev:state_end]
    step_proj = first_proj[:, state_end:]
    step_bias_row = jnp.pad(step_bias, (0, step_pad))[None]

    def state_piece(state_values, conv_taps, conv_bias):
        return jax.nn.silu(
            causal_conv(
                state_values,
                conv_taps.reshape(conv_taps.shape[0], -1),
                conv_bias.reshape(-1),
                segment_ids,
            )
        )

    state_act, state_back = jax.vjp(state_piece, state_proj, conv_state, conv_state_bias)
    bs_low = state_act[:, :state_dim].astype(BF16)
    cs_low = state_act[:, state_dim:].astype(BF16)
    step_size = jax.nn.softplus(step_proj + step_bias_row)
    decay_rate = -jnp.exp(jnp.pad(decay_log, (0, step_pad)))
    log_decay = step_size * decay_rate[None, :]
    terms = chunk_terms(step_size, log_decay, segment_ids, heads_dev, head_size)
    skip_row = jnp.repeat(skip_gain, head_size)[None]
    bias_row = conv_inner_bias[None]
    mixed, states, score = ssd_forward(
        inner_proj, conv_inner, bias_row, skip_row, terms, bs_low, cs_low, head_size
    )
    later_weights = place_rows(later_pieces)
    gate_weights = later_weights[:, :inner_dev]
    out_weights_t = later_weights[:, inner_dev:]
    gate_proj = dot(normed, gate_weights)
    gate_sigmoid = jax.nn.sigmoid(gate_proj)
    gated_values = mixed * (gate_proj * gate_sigmoid)
    full_inner = inner_dev * lax.axis_size("tensor")
    squares = lax.psum(jnp.sum(gated_values * gated_values, axis=1), "tensor")
    gate_scale = lax.rsqrt(squares / full_inner + EPSILON)[:, None]
    normed_inner = (gated_values * gate_scale * gate_gain[None, :]).astype(BF16)
    partial_out = jnp.einsum(
        "tc,dc->td", normed_inner, out_weights_t, preferred_element_type=F32
    )
    branch_own = scatter_pair(partial_out, tensor_place)
    block_out = (own_rows + own_live * branch_own).astype(BF16)
    cot_rows = cotangent.astype(F32)
    branch_grad_own = (own_live * cot_rows).astype(BF16)
    branch_grad = gather_pair(branch_grad_own, tensor_place)
    grad_out_proj_t = jnp.einsum(
        "td,tc->dc", branch_grad, normed_inner, preferred_element_type=F32
    )
    grad_normed_inner = jnp.einsum(
        "td,dc->tc", branch_grad, out_weights_t, preferred_element_type=F32
    )
    grad_gate_gain = jnp.sum(grad_normed_inner * gated_values * gate_scale, axis=0)
    scaled_grad = grad_normed_inner * gate_gain[None, :]
    products = lax.psum(jnp.sum(scaled_grad * gated_values, axis=1), "tensor")
    grad_gated = (
        gate_scale * scaled_grad - gated_values * gate_scale**3 * (products / full_inner)[:, None]
    )
    low_gate = (
        grad_gated * mixed * (gate_sigmoid * (1.0 + gate_proj * (1.0 - gate_sigmoid)))
    ).astype(BF16)
    grad_mixed = grad_gated * (gate_proj * gate_sigmoid)
    grad_gate_half = jnp.einsum(
        "td,tc->dc", normed, low_gate, preferred_element_type=F32
    ).astype(BF16)
    grad_out_low = grad_out_proj_t.astype(BF16)
    grad_mixed, grad_gate_half, grad_out_low = lax.optimization_barrier(
        (grad_mixed, grad_gate_half, grad_out_low)
    )
    cut = 2 * inner_dev // 3
    early_parts = scatter_rows(
        [
            grad_gate_half[:, :cut],
            jnp.concatenate([grad_gate_half[:, cut:], grad_out_low[:, : 2 * cut - inner_dev]], axis=1),
            grad_out_low[:, 2 * cut - inner_dev :],
        ],
    )
    early_part = jnp.concatenate(early_parts, axis=1)
    gate_part, out_part = early_part[:, :inner_dev], early_part[:, inner_dev:]
    scan_back = ssd_backward(
        inner_proj,
        conv_inner,
        bias_row,
        skip_row,
        terms,
        score,
        bs_low,
        cs_low,
        states,
        grad_mixed,
        head_size,
    )
    low_inner, grad_bs, grad_cs, grad_step_size, grad_log, inner_sums = scan_back
    taps_count = conv_inner.shape[0]
    grad_conv_inner = inner_sums[:taps_count][::-1]
    grad_conv_inner_bias = inner_sums[taps_count]
    grad_skip_gain = jnp.sum(inner_sums[taps_count + 1].reshape(heads_dev, head_size), axis=1)
    grad_decay_log = jnp.sum(grad_log * log_decay, axis=0)[:heads_dev]
    grad_step_proj = (grad_step_size + grad_log * decay_rate[None, :]) * jax.nn.sigmoid(
        step_proj + step_bias_row
    )
    grad_step_bias = jnp.sum(grad_step_proj, axis=0)[:heads_dev]
    grad_inner = jnp.einsum("td,tc->dc", normed, low_inner, preferred_element_type=F32).astype(BF16)
    grad_state_part = jnp.concatenate([grad_bs, grad_cs], axis=1)
    grad_state_act = grad_state_part + swap_pair(grad_state_part)
    grad_state_proj, grad_conv_state, grad_conv_state_bias = state_back(grad_state_act)
    low_state = grad_state_proj.astype(BF16)
    low_step = grad_step_proj.astype(BF16)
    own_state = low_state * (tensor_place == 0).astype(BF16)
    low_rest = jnp.concatenate([low_state, low_step], axis=1)
    low_rest_own = jnp.concatenate([own_state, low_step], axis=1)
    grad_rest = jnp.einsum("td,tc->dc", normed, low_rest, preferred_element_type=F32).astype(BF16)
    third = inner_dev // 3
    late_parts = scatter_rows(
        [grad_inner[:, turn * third : (turn + 1) * third] for turn in range(3)]
    )
    first_part = jnp.concatenate(late_parts + scatter_rows([grad_rest]), axis=1)
    grad_out_proj = out_part.T
    grad_in_gate_inner = jnp.stack([gate_part, first_part[:, :inner_dev]], axis=1)
    grad_in_state = first_part[:, inner_dev:state_end].reshape(in_state.shape)
    grad_in_step = first_part[:, state_end : state_end + heads_dev]
    head_grads = (
        dot_nt(low_gate, gate_weights)
        + dot_nt(low_inner, first_weights[:, :inner_dev])
        + dot_nt(low_rest_own, first_weights[:, inner_dev:])
    )
    normed_grad_own = scatter_pair(head_grads, tensor_place)
    grad_norm_part = jnp.sum(normed_grad_own * own_rows * row_scale, axis=0)
    scaled_rows = normed_grad_own * norm_gain[None, :]
    row_products = jnp.sum(scaled_rows * own_rows, axis=1, keepdims=True)
    grad_tokens = (
        cot_rows + row_scale * scaled_rows - own_rows * row_scale**3 * row_products / model_width
    )
    small_parts = (
        grad_norm_part + swap_pair(grad_norm_part),
        grad_conv_inner,
        grad_conv_inner_bias,
        grad_conv_state,
        grad_conv_state_bias,
        grad_step_bias,
        grad_decay_log,
        grad_skip_gain,
        grad_gate_gain,
    )
    summed = sum_small(jnp.concatenate([part.reshape(-1) for part in small_parts]))
    small, start = [], 0
    for part in small_parts:
        small.append(summed[start : start + part.size].reshape(part.shape))
        start += part.size
    return (
        block_out,
        grad_tokens,
        small[0],
        grad_in_gate_inner,
        grad_in_state,
        grad_in_step,
        *small[1:],
        grad_out_proj,
    )


def solution(mesh):
    in_specs = (
        P(("dp", "tensor"), None),
        P("dp"),
        P(),
        P("dp", None, "tensor"),
        P("dp", None, None),
        P("dp", "tensor"),
        P(None, "tensor"),
        P("tensor"),
        P(),
        P(),
        P("tensor"),
        P("tensor"),
        P("tensor"),
        P("tensor"),
        P("tensor", "dp"),
        P(("dp", "tensor"), None),
    )
    out_specs = (
        P(("dp", "tensor"), None),
        P(("dp", "tensor"), None),
        P(),
        P("dp", None, "tensor"),
        P("dp", None, None),
        P("dp", "tensor"),
        P(None, "tensor"),
        P("tensor"),
        P(),
        P(),
        P("tensor"),
        P("tensor"),
        P("tensor"),
        P("tensor"),
        P("tensor", "dp"),
    )

    return jax.shard_map(shards, mesh=mesh, in_specs=in_specs, out_specs=out_specs, check_vma=False)
```
